32 devices in a mesh: rep: 8 (over y, x, core), shard: 4 (over z).
Axes of the slice: x: 2, y: 2, z: 4, core: 2. Of those that a mesh axis runs over, the one named last changes fastest.
Arguments:
- tokens: bfloat16 [64, 512, 768], P(('rep', 'shard')), may hold values from -6 to 6
- segment_ids: int32 [64, 512], P(('rep', 'shard')), may hold values from 0 to 63, never falling along the last dimension, each value on 1 to 256 neighbouring positions
- norm_gain: bfloat16 [768], P('shard'), may hold values from 0.5 to 1.5
- in_weight: bfloat16 [768, 3352], P('shard'), may hold values from -0.21875 to 0.21875
- conv_weight: bfloat16 [1792, 4], P('shard'), may hold values from -3 to 3
- conv_bias: bfloat16 [1792], P('shard'), may hold values from -3 to 3
- dt_bias: float32 [24], replicated, may hold values from -5 to -1
- a_log: float32 [24], replicated, may hold values from 0 to 2.77
- d_skip: float32 [24], replicated, may hold values from 0.5 to 1.5
- gate_gain: bfloat16 [1536], P('shard'), may hold values from 0.5 to 1.5
- out_weight: bfloat16 [1536, 768], P('shard'), may hold values from -0.15625 to 0.15625
- cotangent: bfloat16 [64, 512, 768], P(('rep', 'shard')), may hold values from -6 to 6
Outputs:
- mixed: bfloat16 [64, 512, 768], P(('rep', 'shard'))
- grad_tokens: float32 [64, 512, 768], P(('rep', 'shard'))
- grad_norm_gain: float32 [768], P('shard')
- grad_in_weight: float32 [768, 3352], P('shard')
- grad_conv_weight: float32 [1792, 4], P('shard')
- grad_conv_bias: float32 [1792], P('shard')
- grad_dt_bias: float32 [24], replicated
- grad_a_log: float32 [24], replicated
- grad_d_skip: float32 [24], replicated
- grad_gate_gain: float32 [1536], P('shard')
- grad_out_weight: float32 [1536, 768], P('shard')
The draws below stay inside these ranges and needn't reach their ends.
Inputs may be any that keep to these rules, and one draw needn't show every extreme that they name: `segment_ids`: along each sequence the segment numbers never fall, so every document is a run of consecutive tokens; the longest run in a sequence has at most 256 tokens.
All inputs are finite; a program needn't handle non-finite values.
Results may differ from the reference program's by a relative error of at most 0.0073.
Values may be sent and summed in bfloat16 or wider, within the bound.
A program may use at most 256 MiB of HBM per device.

```python
import math
from functools import partial
import jax
import jax.numpy as jnp
import numpy as np
from jax import lax

D = 768
HEADS = 24
HEADDIM = 64
STATE = 128
CONV = 4
BLOCK = 256
SEQ_LEN = 512
INNER = 1536
CONV_CH = 1792
PROJ = 3352
SEQS = 64


def block_scale(key, extent, pieces, smallest, largest):
    loudness, own = 1.0, jax.random.fold_in(key, 6)
    for axis_at, blocks in pieces:
        steps = jnp.exp(jax.random.uniform(jax.random.fold_in(own, axis_at), (blocks,), jnp.float32, smallest / len(pieces), largest / len(pieces)))
        loudness = loudness * jnp.repeat(steps, extent[axis_at] // blocks).reshape([-1 if axis == axis_at else 1 for axis in range(len(extent))])
    return loudness


def profile(count, total, reach, skew):
    weights = [(1 << 20) // math.isqrt(rank ** skew) + 1 for rank in range(2, count + 1)]
    rest, given = total - reach - (count - 1), [1] * (count - 1)
    while rest > 0:
        movable = [i for i in range(count - 1) if given[i] < reach]
        mass, budget = sum([weights[i] for i in movable]), rest
        for i in movable:
            addition = min(reach - given[i], max(1, budget * weights[i] // mass), rest)
            given[i] = given[i] + addition
            rest = rest - addition
    return np.array([reach] + given)


def ragged(key, count, total, most, skew):
    if count == 2:
        one = jax.random.randint(key, (), max(1, total - most), min(most, total - 1) + 1)
        return jnp.stack([one, total - one])
    sizes = jnp.asarray(profile(count, total, most, skew), jnp.int32)
    couples = (count - 1) // 2
    source_of, receiver = sizes[1:1 + 2 * couples:2], sizes[2:2 + 2 * couples:2]
    slack = jnp.minimum(source_of - 1, most - receiver)
    moved = jax.random.randint(jax.random.fold_in(key, 1), (couples,), 0, 1 << 20) % (slack + 1)
    sizes = sizes.at[1:1 + 2 * couples:2].set(source_of - moved).at[2:2 + 2 * couples:2].set(receiver + moved)
    return sizes[jax.random.permutation(jax.random.fold_in(key, 2), count)]


def bell_draw(own_key, dims, deviation, reach, cuts=(), held_as=jnp.bfloat16):
    entries = jax.random.normal(own_key, dims, jnp.float32) * deviation
    if len(cuts) > 0:
        entries = block_scale(own_key, dims, cuts, -0.22, 0.18) * entries
    return jnp.clip(entries, min=-reach, max=reach).astype(held_as)


def setup_inputs(seed: int = 0) -> dict:
    key_list = jax.random.split(jax.random.key(seed), 13)
    tokens = bell_draw(key_list[0], (SEQS, SEQ_LEN, D), 1.0, 6.0, ((0, 32),))
    segment_ids = jax.vmap(lambda own: jnp.searchsorted(jnp.cumsum(ragged(own, SEQ_LEN // 8, SEQ_LEN, SEQ_LEN // 2, 2)), jnp.arange(SEQ_LEN), side="right"))(jax.random.split(key_list[1], SEQS)).reshape((SEQS, SEQ_LEN)).astype(jnp.int32)
    norm_gain = jnp.clip(1.0 + 0.1 * jax.random.normal(key_list[2], (D,), jnp.float32), 0.5, 1.5).astype(jnp.bfloat16)
    in_weight = bell_draw(key_list[3], (D, PROJ), D ** -0.5, 0.21875, ((0, 4),))
    conv_weight = bell_draw(key_list[4], (CONV_CH, CONV), CONV ** -0.5, 3.0, ((0, 4),))
    conv_bias = bell_draw(key_list[5], (CONV_CH,), 0.5, 3.0, ((0, 4),))
    dt_bias = jnp.clip(jax.random.uniform(key_list[6], (HEADS,), jnp.float32, -5.0, -1.0), -5.0, -1.0)
    a_log = jnp.clip(jax.random.uniform(key_list[7], (HEADS,), jnp.float32, 0.0, 2.77), 0.0, 2.77)
    d_skip = jnp.clip(jax.random.uniform(key_list[8], (HEADS,), jnp.float32, 0.5, 1.5), 0.5, 1.5)
    gate_gain = jnp.clip(1.0 + 0.1 * jax.random.normal(key_list[9], (INNER,), jnp.float32), 0.5, 1.5).astype(jnp.bfloat16)
    out_weight = bell_draw(key_list[10], (INNER, D), INNER ** -0.5, 0.15625, ((0, 4),))
    cotangent = bell_draw(key_list[11], (SEQS, SEQ_LEN, D), 1.0, 6.0, ((0, 32),))
    return dict(tokens=tokens, segment_ids=segment_ids, norm_gain=norm_gain, in_weight=in_weight, conv_weight=conv_weight, conv_bias=conv_bias, dt_bias=dt_bias, a_log=a_log, d_skip=d_skip, gate_gain=gate_gain, out_weight=out_weight, cotangent=cotangent)


@jax.custom_vjp
def low(v):
    return lax.optimization_barrier(v.astype(jnp.bfloat16)).astype(jnp.float32)

@jax.custom_vjp
def low_back(v):
    return v

def low_keep(v):
    return (low(v), None)

def low_pass(kept, grad):
    return (grad,)

def back_keep(v):
    return (v, None)

def back_low(kept, grad):
    return (low(grad),)
low.defvjp(low_keep, low_pass)
low_back.defvjp(back_keep, back_low)
EPS = 1e-05
PRECISE = lax.Precision.HIGHEST

def product(left, right):
    return jnp.dot(left, right, precision=PRECISE, preferred_element_type=jnp.float32)

def rms_norm(values, gains):
    return values * lax.rsqrt(lax.optimization_barrier(jnp.mean(values * values, axis=-1, keepdims=True)) + EPS) * gains

def causal_conv(conv_in, segments, conv_taps, conv_shift):
    summed = conv_shift[None, :] + conv_taps[:, CONV - 1][None, :] * conv_in
    for offset in range(1, CONV):
        shifted = jnp.concatenate([jnp.zeros((offset, conv_in.shape[1]), jnp.float32), conv_in[:-offset]], axis=0)
        earlier = jnp.concatenate([jnp.full((offset,), -1, jnp.int32), segments[:-offset]])
        same_doc = (earlier == segments).astype(jnp.float32)[:, None]
        summed = summed + conv_taps[:, CONV - 1 - offset][None, :] * shifted * same_doc
    return summed

def block_weights(gram, cumulative, step_sizes, segments):
    places = jnp.arange(segments.shape[0])
    allowed = (places[:, None] >= places[None, :]) & (segments[:, None] == segments[None, :])
    spread = cumulative.T[:, :, None] - cumulative.T[:, None, :]
    decays = jnp.where(allowed[None], jnp.exp(jnp.minimum(spread, 0.0)), 0.0)
    return low(gram[None] * decays * step_sizes.T[:, None, :])

def block_step(carried, block, weigh):
    state, last_segment = carried
    values, b_part, c_part, rates, step_sizes, segments = block
    cumulative = jnp.cumsum(rates, axis=0)
    gram = low_back(product(c_part, b_part.T))
    weights = weigh(gram, cumulative, step_sizes, segments)
    y_inner = low_back(jnp.einsum('hts,shp->thp', weights, values, precision=PRECISE))
    carry_mask = (segments == last_segment).astype(jnp.float32)
    y_state = low_back(jnp.einsum('tn,hpn->thp', c_part, low(state), precision=PRECISE))
    y_block = y_inner + y_state * (jnp.exp(cumulative) * carry_mask[:, None])[:, :, None]
    tail_mask = (segments == segments[-1]).astype(jnp.float32)
    tail_scale = jnp.exp(cumulative[-1][None, :] - cumulative) * step_sizes * tail_mask[:, None]
    weighted = low(values * tail_scale[:, :, None])
    update = low_back(jnp.einsum('shp,sn->hpn', weighted, b_part, precision=PRECISE))
    keep_state = jnp.exp(cumulative[-1]) * (segments[-1] == last_segment).astype(jnp.float32)
    state = state * keep_state[:, None, None] + update
    return ((state, segments[-1]), y_block)

def layer_sequence(params, inputs, segments, stepper):
    norm_gains, in_proj, conv_taps, conv_shift, dt_shift, log_rates, skip_gain, gate_gains, out_proj = params
    length = inputs.shape[0]
    normed = low(rms_norm(inputs, norm_gains))
    projected = low_back(product(normed, in_proj))
    gate_part = projected[:, :INNER]
    conv_in = projected[:, INNER:INNER + CONV_CH]
    dt_raw = projected[:, INNER + CONV_CH:]
    conv_out = jax.nn.silu(causal_conv(conv_in, segments, conv_taps, conv_shift))
    x_heads = low(conv_out[:, :INNER]).reshape(length, HEADS, HEADDIM)
    b_all = low(conv_out[:, INNER:INNER + STATE])
    c_all = low(conv_out[:, INNER + STATE:])
    step_sizes = jax.nn.softplus(dt_raw + dt_shift[None, :])
    rates = -jnp.exp(log_rates)[None, :] * step_sizes
    count = length // BLOCK

    def blocked(values):
        return values.reshape((count, BLOCK) + values.shape[1:])
    initial = (jnp.zeros((HEADS, HEADDIM, STATE), jnp.float32), jnp.array(-1, jnp.int32))
    final_carry, y_blocks = lax.scan(stepper, initial, (blocked(x_heads), blocked(b_all), blocked(c_all), blocked(rates), blocked(step_sizes), blocked(segments)))
    y_heads = y_blocks.reshape(length, HEADS, HEADDIM) + skip_gain[None, :, None] * x_heads
    y_flat = y_heads.reshape(length, INNER)
    gated = low(rms_norm(y_flat * jax.nn.silu(gate_part), gate_gains))
    branch = low_back(product(gated, out_proj))
    return inputs + branch

def reference(tokens, segment_ids, norm_gain, in_weight, conv_weight, conv_bias, dt_bias, a_log, d_skip, gate_gain, out_weight, cotangent):
    params = (norm_gain.astype(jnp.float32), in_weight.astype(jnp.float32), conv_weight.astype(jnp.float32), conv_bias.astype(jnp.float32), dt_bias.astype(jnp.float32), a_log.astype(jnp.float32), d_skip.astype(jnp.float32), gate_gain.astype(jnp.float32), out_weight.astype(jnp.float32))
    inputs = tokens.astype(jnp.float32)
    stepper = jax.checkpoint(partial(block_step, weigh=block_weights))

    def forward(params_in, inputs_in):

        def one_sequence(item):
            return layer_sequence(params_in, item[0], item[1], stepper)
        return lax.map(jax.checkpoint(one_sequence), (inputs_in, segment_ids))
    outputs, pullback = jax.vjp(forward, params, inputs)
    grad_params, grad_inputs = pullback(cotangent.astype(jnp.float32))
    return (outputs.astype(jnp.bfloat16), grad_inputs, grad_params[0], grad_params[1], grad_params[2], grad_params[3], grad_params[4], grad_params[5], grad_params[6], grad_params[7], grad_params[8])
```

```python
from functools import partial

import jax
import jax.numpy as jnp
from jax import lax
from jax.experimental import pallas as pl
from jax.experimental.pallas import tpu as pltpu
from jax.sharding import PartitionSpec as P

HEADS = 24
HEADDIM = 64
STATE = 128
CONV = 4
INNER = 1536
CONV_CH = 1792
MODEL = 768
PROJ = 3352
PADDED = 3456
EPS = 1e-05

LEN = 512
CHUNK = 128
SEQ = 2
TOKENS = SEQ * LEN
QUADS = INNER // 256

f32 = jnp.float32
bf16 = jnp.bfloat16


def nn(a, b):
    return lax.dot_general(a, b, (((1,), (0,)), ((), ())), preferred_element_type=f32)


def nt(a, b):
    return lax.dot_general(a, b, (((1,), (1,)), ((), ())), preferred_element_type=f32)


def tn(a, b):
    return lax.dot_general(a, b, (((0,), (0,)), ((), ())), preferred_element_type=f32)


def exact(a, b):
    return lax.dot_general(
        a, b, (((1,), (0,)), ((), ())), preferred_element_type=f32, precision=lax.Precision.HIGHEST
    )


def sigmoid(v):
    return 0.5 * jnp.tanh(0.5 * v) + 0.5


def partial_sum(a):
    return a.reshape(a.shape[0] // 8, 8, a.shape[1]).sum(axis=0)


def lanes_of(shape):
    return lax.broadcasted_iota(jnp.int32, shape, 1)


def rows_of(shape):
    return lax.broadcasted_iota(jnp.int32, shape, 0)


def packed(a):
    a = jnp.where(lanes_of(a.shape) < HEADS, a, 0.0)
    high = a.astype(bf16).astype(f32)
    rest = a - high
    middle = rest.astype(bf16).astype(f32)
    low = rest - middle
    return (high + pltpu.roll(middle, 32, 1) + pltpu.roll(low, 64, 1)).astype(bf16)


def two_parts(a):
    high = a.astype(bf16)
    return high, (a - high.astype(f32)).astype(bf16)


def y_at(row, count, cols):
    right = cols.start >= MODEL
    base, shift = (LEN, MODEL) if right else (0, 0)
    return pl.ds(pl.multiple_of(base + row, 8), count), slice(cols.start - shift, cols.stop - shift)


def setup(seg_ref, win, s):
    r, c = rows_of((128, 256)), lanes_of((128, 256))
    for j in range(HEADS * 128 // 256):
        s["one128"][:, j * 256 : (j + 1) * 256] = (
            ((r & 31) == ((c + j * 256) >> 7)) & (r < 96)
        ).astype(f32).astype(bf16)
    for j in range(QUADS):
        s["one64"][:, j * 256 : (j + 1) * 256] = (
            ((r & 31) == ((c + j * 256) >> 6)) & (r < 96)
        ).astype(f32).astype(bf16)
    r, c = rows_of((256, 128)), lanes_of((256, 128))
    for j in range(QUADS):
        s["sum64"][j * 256 : (j + 1) * 256, :] = (((r + j * 256) >> 6) == c).astype(f32).astype(bf16)
    s["wdt"][...] = jnp.zeros((MODEL, 128), bf16)
    s["wdt"][:, :HEADS] = win[:, INNER + CONV_CH : PROJ]
    s["acc"][...] = jnp.zeros(s["acc"].shape, f32)
    s["pre"][TOKENS:, :] = jnp.zeros((16, CONV_CH), bf16)
    s["up"][:, 0:8, :] = jnp.zeros((2, 8, 256), f32)
    for q in range(SEQ):
        s["segc"][q, 0:8, :] = jnp.full((8, 128), -1.0, f32)
        for i in range(LEN // 128):
            seg = seg_ref[q : q + 1, i * 128 : (i + 1) * 128].astype(f32)
            s["segc"][q, 8 + i * 128 : 8 + (i + 1) * 128, :] = jnp.broadcast_to(seg, (128, 128)).T


def project(q, x_ref, seg_ref, win, sm, hd, s):
    row0 = pl.multiple_of(q * LEN, LEN)
    for i in range(LEN // 128):
        rows = pl.ds(row0 + i * 128, 128)
        x = x_ref[rows, :].astype(f32)
        r = lax.rsqrt(jnp.mean(x * x, axis=1, keepdims=True) + EPS)
        s["nrm"][rows, :] = (x * r * sm[6:7, :MODEL]).astype(bf16)
    seg = s["segc"][q, 8 : 8 + LEN, :]
    place = rows_of((LEN, 128))
    for o in range(1, CONV):
        s["back"][o - 1] = ((seg == pltpu.roll(seg, o, 0)) & (place >= o)).astype(f32)
    rows = pl.ds(row0, LEN)
    raw = nn(s["nrm"][rows, :], s["wdt"][...]) + hd[0:1, :]
    s["dtx"][rows, :] = raw
    for j in range(CONV_CH // 256):
        slot = j % 2
        s["up"][slot, 8:, :] = nn(s["nrm"][rows, :], win[:, INNER + j * 256 : INNER + (j + 1) * 256])
        for i in range(LEN // 128):
            for half in range(2):
                c0 = j * 256 + half * 128
                here = pl.ds(row0 + i * 128, 128)
                block = s["up"][slot, i * 128 : i * 128 + 136, half * 128 : (half + 1) * 128]
                u = block[8:]
                tap = lambda k: sm[k : k + 1, c0 : c0 + 128]
                pre = sm[4:5, c0 : c0 + 128] + tap(3) * u
                for o in range(1, CONV):
                    same = s["back"][o - 1, i * 128 : (i + 1) * 128, :]
                    pre = pre + tap(3 - o) * (pltpu.roll(block, o, 0)[8:] * same)
                s["u"][here, c0 : c0 + 128] = u.astype(bf16)
                s["pre"][here, c0 : c0 + 128] = pre.astype(bf16)
                s["xbc"][here, c0 : c0 + 128] = (pre * sigmoid(pre)).astype(bf16)


def chunk_terms(q, c, seg_ref, hd, s):
    row0 = pl.multiple_of(q * LEN + c * CHUNK, CHUNK)
    rows = pl.ds(row0, CHUNK)
    raw = s["dtx"][rows, :]
    dt = jnp.maximum(raw, 0.0) + jnp.log1p(jnp.exp(-jnp.abs(raw)))
    rate = -jnp.exp(hd[1:2, :]) * dt
    lower = (rows_of((CHUNK, CHUNK)) >= lanes_of((CHUNK, CHUNK))).astype(f32)
    cum = exact(lower, rate)
    source = cum - jnp.log(jnp.maximum(dt, 1e-37))
    start = 8 + c * CHUNK
    segc = s["segc"][q, pl.ds(pl.multiple_of(start, 8), CHUNK), :]
    segr = segc.T
    before = s["segc"][q, pl.ds(pl.multiple_of(start - 8, 8), 8), :][7:8]
    last = segc[CHUNK - 1 : CHUNK]
    carry = (segc == before).astype(f32)
    tail = (segc == last).astype(f32)
    end = cum[CHUNK - 1 : CHUNK, :]
    keep = jnp.exp(end) * (before == last).astype(f32)
    grow = jnp.exp(cum) * carry
    shrink = jnp.exp(end - source) * tail
    return rows, raw, dt, rate, cum, source, segc, segr, grow, shrink, keep


def scan_forward(q, c, seg_ref, sm, hd, s):
    rows, raw, dt, rate, cum, source, segc, segr, grow, shrink, keep = chunk_terms(q, c, seg_ref, hd, s)
    t, k = rows_of((CHUNK, CHUNK)), lanes_of((CHUNK, CHUNK))
    bound = jnp.where((segc == segr) & (t >= k), 3e38, -1e30)
    s["rowv"][...] = source.T
    target = packed(cum)
    grow_p, shrink_p = packed(grow), packed(shrink)
    keep_p = packed(jnp.broadcast_to(keep, (8, 128)))
    bv = s["xbc"][rows, INNER : INNER + STATE]
    cv = s["xbc"][rows, INNER + STATE :]
    gram = nt(cv, bv)
    bt = bv.T
    at = q * (LEN // CHUNK) + c
    left = lanes_of((CHUNK, 128)) < HEADDIM
    for j in range(QUADS):
        cols = slice(j * 256, (j + 1) * 256)
        grow_e = nn(grow_p, s["one64"][:, cols])
        shrink_e = nn(shrink_p, s["one64"][:, cols])
        keep_e = nn(keep_p, s["one64"][:, cols])[0:1, :]
        state = s["state"][:, cols]
        low_state = state.astype(bf16)
        s["states"][at, :, cols] = low_state
        y_state = nn(cv, low_state)
        xv = s["xbc"][rows, cols]
        xw = (xv.astype(f32) * shrink_e).astype(bf16)
        s["state"][:, cols] = state * keep_e + nn(bt, xw)
        parts = []
        for pair in range(2):
            spread = nn(target, s["one128"][:, j * 512 + pair * 256 : j * 512 + (pair + 1) * 256])
            weights = []
            for half in range(2):
                head = 4 * j + 2 * pair + half
                d = spread[:, half * 128 : (half + 1) * 128] - s["rowv"][head : head + 1, :]
                weights.append((gram * jnp.exp(jnp.minimum(d, bound))).astype(bf16))
            x2 = xv[:, pair * 128 : (pair + 1) * 128]
            zero = jnp.zeros_like(x2)
            stack = jnp.concatenate([jnp.where(left, x2, zero), jnp.where(left, zero, x2)], axis=0)
            parts.append(nn(jnp.concatenate(weights, axis=1), stack))
        s["y"][y_at(c * CHUNK, CHUNK, cols)] = (
            jnp.concatenate(parts, axis=1) + y_state * grow_e
        )


def gate(q, i, x_ref, cot_ref, win, wout, sm, mixed_ref, s):
    tall, block = 256, 64
    row0 = q * LEN + i * tall
    rows = pl.ds(pl.multiple_of(row0, tall), tall)
    for j in range(QUADS):
        cols = slice(j * 256, (j + 1) * 256)
        s["z"][:, cols] = nn(s["nrm"][rows, :], win[:, cols])
        s["dg"][:, cols] = nt(cot_ref[rows, :], wout[cols, :])

    @pl.loop(0, tall // block)
    def _(b):
        own = pl.ds(pl.multiple_of(b * block, block), block)
        here = i * tall + b * block
        where = pl.ds(pl.multiple_of(row0 + b * block, block), block)
        square = jnp.zeros((block, 128), f32)
        along = jnp.zeros((block, 128), f32)
        for j in range(INNER // 128):
            cols = slice(j * 128, (j + 1) * 128)
            z = s["z"][own, cols]
            y = s["y"][y_at(here, block, cols)] + sm[7:8, cols] * s["xbc"][where, cols].astype(f32)
            v = y * (z * sigmoid(z))
            square = square + v * v
            along = along + s["dg"][own, cols] * sm[5:6, cols] * v
        r = lax.rsqrt(jnp.sum(square, axis=1, keepdims=True) * (1.0 / INNER) + EPS)
        k = r * r * r * (jnp.sum(along, axis=1, keepdims=True) * (1.0 / INNER))
        for j in range(INNER // 128):
            cols = slice(j * 128, (j + 1) * 128)
            z = s["z"][own, cols]
            dg = s["dg"][own, cols]
            ys = s["y"][y_at(here, block, cols)]
            xv = s["xbc"][where, cols].astype(f32)
            y = ys + sm[7:8, cols] * xv
            sg = sigmoid(z)
            zs = z * sg
            v = y * zs
            vr = v * r
            gain = sm[5:6, cols]
            s["gated"][where, cols] = (vr * gain).astype(bf16)
            s["acc"][5, :, cols] += partial_sum(dg * vr)
            dv = r * (dg * gain) - v * k
            dy = dv * zs
            low_dy = dy.astype(bf16)
            s["dy"][where, cols] = low_dy
            s["dz"][where, cols] = (dv * y * (sg + zs * (1.0 - sg))).astype(bf16)
            s["acc"][7, :, cols] += partial_sum(dy * xv)
            s["dg"][own, cols] = low_dy.astype(f32) * ys

    high, low = two_parts(s["dg"][...])
    s["rowdot"][rows, :] = nn(high, s["sum64"][...]) + nn(low, s["sum64"][...])
    branch = nn(s["gated"][rows, :], wout[...])
    mixed_ref[rows, :] = (x_ref[rows, :].astype(f32) + branch).astype(bf16)


def scan_backward(q, c, seg_ref, sm, hd, s):
    rows, raw, dt, rate, cum, source, segc, segr, grow, shrink, keep = chunk_terms(q, c, seg_ref, hd, s)
    k, t = rows_of((CHUNK, CHUNK)), lanes_of((CHUNK, CHUNK))
    allowed = (segc == segr) & (t >= k)
    bound = jnp.where(allowed, 3e38, -1e30)
    s["rowv"][...] = cum.T
    origin = packed(source)
    grow_p, shrink_p = packed(grow), packed(shrink)
    keep_p = packed(jnp.broadcast_to(keep, (8, 128)))
    bv = s["xbc"][rows, INNER : INNER + STATE]
    cv = s["xbc"][rows, INNER + STATE :]
    gram = nt(bv, cv)
    ct = cv.T
    at = q * (LEN // CHUNK) + c
    left = lanes_of((CHUNK, 128)) < HEADDIM
    dgram = jnp.zeros((CHUNK, CHUNK), f32)
    for j in range(QUADS):
        cols = slice(j * 256, (j + 1) * 256)
        grow_e = nn(grow_p, s["one64"][:, cols])
        s["dys"][:, cols] = (s["dy"][rows, cols].astype(f32) * grow_e).astype(bf16)
        shrink_e = nn(shrink_p, s["one64"][:, cols])
        s["xw"][:, cols] = (s["xbc"][rows, cols].astype(f32) * shrink_e).astype(bf16)
        low_dstate = s["state"][:, cols].astype(bf16)
        s["lowd"][:, cols] = low_dstate
        part = nn(bv, low_dstate) * shrink_e
        s["part"][:, cols] = part
        keep_e = nn(keep_p, s["one64"][:, cols])[0:1, :]
        kept = s["state"][:, cols] * keep_e
        s["tail"][:, cols] = partial_sum(s["xbc"][rows, cols].astype(f32) * part) + partial_sum(
            kept * s["states"][at, :, cols].astype(f32)
        )
        s["state"][:, cols] = kept + nn(ct, s["dys"][:, cols])
    for j in range(INNER // 128):
        cols = slice(j * 128, (j + 1) * 128)
        xv = s["xbc"][rows, cols]
        dy = s["dy"][rows, cols]
        spread = nn(origin, s["one128"][:, j * 256 : (j + 1) * 256])
        zero = jnp.zeros_like(dy)
        stack = jnp.concatenate([jnp.where(left, dy, zero), jnp.where(left, zero, dy)], axis=0)
        dweights = nt(xv, stack)
        weights = []
        for half in range(2):
            head = 2 * j + half
            d = s["rowv"][head : head + 1, :] - spread[:, half * 128 : (half + 1) * 128]
            e = jnp.exp(jnp.minimum(d, bound))
            weights.append((gram * e).astype(bf16))
            dgram = dgram + dweights[:, half * 128 : (half + 1) * 128] * e
        dx = nn(jnp.concatenate(weights, axis=1), stack) + s["part"][:, cols]
        s["part"][:, cols] = xv.astype(f32) * dx
        dx = dx + sm[7:8, cols] * dy.astype(f32)
        pre = s["pre"][rows, cols].astype(f32)
        sg = sigmoid(pre)
        s["pre"][rows, cols] = (dx * (sg * (1.0 + pre * (1.0 - sg)))).astype(bf16)
    high, low = two_parts(s["part"][...])
    colsum = nn(high, s["sum64"][...]) + nn(low, s["sum64"][...])
    high, low = two_parts(s["tail"][...])
    dlast = jnp.sum(nn(high, s["sum64"][...]) + nn(low, s["sum64"][...]), axis=0, keepdims=True)
    dc = nt(s["dys"][...], s["states"][at])
    db = nt(s["xw"][...], s["lowd"][...])
    low_dgram = dgram.astype(bf16)
    db = db + nn(low_dgram, cv)
    dc = dc + tn(low_dgram, bv)
    for index, d in ((0, db), (1, dc)):
        cols = slice(INNER + index * STATE, INNER + (index + 1) * STATE)
        pre = s["pre"][rows, cols].astype(f32)
        sg = sigmoid(pre)
        s["pre"][rows, cols] = (d * (sg * (1.0 + pre * (1.0 - sg)))).astype(bf16)
    dcum = s["rowdot"][rows, :] - colsum
    drate = exact(allowed.astype(f32), dcum) + dlast * (segc == segc[CHUNK - 1 : CHUNK]).astype(f32)
    sg = sigmoid(raw)
    ratio = jnp.where(dt > 1e-30, sg / jnp.maximum(dt, 1e-30), 1.0)
    draw = colsum * ratio - drate * jnp.exp(hd[1:2, :]) * sg
    draw = jnp.where(lanes_of((CHUNK, 128)) < HEADS, draw, 0.0)
    s["ddt"][rows, :] = draw.astype(bf16)
    s["acc"][8, :, 0:128] += partial_sum(draw)
    s["acc"][9, :, 0:128] += partial_sum(drate * rate)


def conv_backward(q, sm, s):
    row0 = pl.multiple_of(q * LEN, LEN)
    rows = pl.ds(row0, LEN)
    seg = s["segc"][q, 8 : 8 + LEN, :]
    place = rows_of((LEN, 128))
    for o in range(1, CONV):
        s["back"][o - 1] = ((seg == pltpu.roll(seg, LEN - o, 0)) & (place < LEN - o)).astype(f32)
    for j in range(CONV_CH // 128):
        cols = slice(j * 128, (j + 1) * 128)
        sums = [jnp.zeros((8, 128), f32)] * 5
        for i in range(LEN // 128):
            here = pl.ds(row0 + i * 128, 128)
            block = s["pre"][pl.ds(row0 + i * 128, 144), cols].astype(f32)
            ds = block[:128]
            u = s["u"][here, cols].astype(f32)
            du = sm[3:4, cols] * ds
            sums[4] = sums[4] + partial_sum(ds)
            sums[3] = sums[3] + partial_sum(ds * u)
            for o in range(1, CONV):
                moved = pltpu.roll(block, 144 - o, 0)[:128] * s["back"][o - 1, i * 128 : (i + 1) * 128, :]
                du = du + sm[3 - o : 4 - o, cols] * moved
                sums[3 - o] = sums[3 - o] + partial_sum(moved * u)
            s["u"][here, cols] = du.astype(bf16)
        for k in range(5):
            s["acc"][k, :, cols] += sums[k]


def input_gradient(i, x_ref, cot_ref, sm, gtok_ref, s):
    rows = pl.ds(pl.multiple_of(i * 128, 128), 128)
    x = x_ref[rows, :].astype(f32)
    dn = gtok_ref[rows, :]
    r = lax.rsqrt(jnp.mean(x * x, axis=1, keepdims=True) + EPS)
    s["acc"][6, :, 0:MODEL] += partial_sum(dn * (x * r))
    h = dn * sm[6:7, :MODEL]
    k = r * r * r * jnp.mean(h * x, axis=1, keepdims=True)
    gtok_ref[rows, :] = r * h - k * x + cot_ref[rows, :].astype(f32)


SCRATCH = dict(
    nrm=((TOKENS, MODEL), bf16),
    u=((TOKENS, CONV_CH), bf16),
    pre=((TOKENS + 16, CONV_CH), bf16),
    xbc=((TOKENS, CONV_CH), bf16),
    dtx=((TOKENS, 128), f32),
    gated=((TOKENS, INNER), bf16),
    dy=((TOKENS, INNER), bf16),
    dz=((TOKENS, INNER), bf16),
    ddt=((TOKENS, 128), bf16),
    z=((256, INNER), f32),
    dg=((256, INNER), f32),
    rowdot=((TOKENS, 128), f32),
    dys=((CHUNK, INNER), bf16),
    xw=((CHUNK, INNER), bf16),
    lowd=((CHUNK, INNER), bf16),
    part=((CHUNK, INNER), f32),
    up=((2, 8 + LEN, 256), f32),
    state=((STATE, INNER), f32),
    states=((SEQ * LEN // CHUNK, STATE, INNER), bf16),
    rowv=((128, 128), f32),
    tail=((8, INNER), f32),
    segc=((SEQ, 8 + LEN, 128), f32),
    back=((CONV - 1, LEN, 128), f32),
    one128=((128, HEADS * 128), bf16),
    one64=((128, INNER), bf16),
    sum64=((INNER, 128), bf16),
    wdt=((MODEL, 128), bf16),
    acc=((10, 8, CONV_CH), f32),
)


def layer_kernel(x_ref, cot_ref, seg_ref, win, wout, sm, hd, mixed_ref, gtok_ref, dwin_ref, dwout_ref, gsm_ref, *refs):
    s = dict(zip(SCRATCH, refs))
    s["y"] = gtok_ref
    setup(seg_ref, win, s)
    chunks = LEN // CHUNK

    @pl.loop(0, SEQ)
    def _(q):
        project(q, x_ref, seg_ref, win, sm, hd, s)
        s["state"][...] = jnp.zeros((STATE, INNER), f32)

        @pl.loop(0, chunks)
        def _(c):
            scan_forward(q, c, seg_ref, sm, hd, s)

        @pl.loop(0, LEN // 256)
        def _(i):
            gate(q, i, x_ref, cot_ref, win, wout, sm, mixed_ref, s)

    for j in range(QUADS):
        cols = slice(j * 256, (j + 1) * 256)
        dwout_ref[cols, :] = tn(s["gated"][:, cols], cot_ref[...]).astype(bf16)

    @pl.loop(0, SEQ)
    def _(q):
        s["state"][...] = jnp.zeros((STATE, INNER), f32)

        @pl.loop(0, chunks)
        def _(c):
            scan_backward(q, chunks - 1 - c, seg_ref, sm, hd, s)

        conv_backward(q, sm, s)

    turned = s["gated"]
    for i in range(TOKENS // 128):
        for j in range(MODEL // 128):
            turned[j * 128 : (j + 1) * 128, i * 128 : (i + 1) * 128] = s["nrm"][
                i * 128 : (i + 1) * 128, j * 128 : (j + 1) * 128
            ].T
    for j in range(13):
        cols = slice(j * 256, (j + 1) * 256)
        of = s["dz"][:, cols] if j < QUADS else s["u"][:, j * 256 - INNER : (j + 1) * 256 - INNER]
        for i in range(3):
            rows = slice(i * 256, (i + 1) * 256)
            dwin_ref[rows, cols] = nn(turned[rows, :TOKENS], of).astype(bf16)
    dwin_ref[:, 3328:] = nn(turned[:MODEL, :TOKENS], s["ddt"][...]).astype(bf16)[:, :HEADS]

    @pl.loop(0, TOKENS // 256)
    def _(i):
        rows = pl.ds(pl.multiple_of(i * 256, 256), 256)
        for j in range(3):
            cols = slice(j * 256, (j + 1) * 256)
            gtok_ref[rows, cols] = (
                nt(s["dz"][rows, :], win[cols, :INNER])
                + nt(s["u"][rows, :], win[cols, INNER : INNER + CONV_CH])
                + nt(s["ddt"][rows, :], s["wdt"][cols, :])
            )

    @pl.loop(0, TOKENS // 128)
    def _(i):
        input_gradient(i, x_ref, cot_ref, sm, gtok_ref, s)

    for k in range(10):
        gsm_ref[k : k + 1, :] = jnp.sum(s["acc"][k], axis=0, keepdims=True)


def layer(x, cot, seg, win, wout, sm, hd):
    vmem = pl.BlockSpec(memory_space=pltpu.VMEM)
    return pl.pallas_call(
        layer_kernel,
        out_shape=(
            jax.ShapeDtypeStruct((TOKENS, MODEL), bf16),
            jax.ShapeDtypeStruct((TOKENS, MODEL), f32),
            jax.ShapeDtypeStruct((MODEL, PROJ), bf16),
            jax.ShapeDtypeStruct((INNER, MODEL), bf16),
            jax.ShapeDtypeStruct((10, CONV_CH), f32),
        ),
        in_specs=[vmem] * 7,
        out_specs=[vmem] * 5,
        scratch_shapes=[pltpu.VMEM(shape, kind) for shape, kind in SCRATCH.values()],
        compiler_params=pltpu.CompilerParams(vmem_limit_bytes=67043328),
        name="layer",
    )(x, cot, seg, win, wout, sm, hd)


def rows_to_lanes(v, width):
    return jnp.pad(v.astype(f32), (0, width - v.shape[0]))[None]


def on_device(tokens, segment_ids, norm_gain, in_weight, conv_weight, conv_bias, dt_bias, a_log, d_skip, gate_gain, out_weight, cotangent):
    win = lax.all_gather(in_weight, "shard", axis=0, tiled=True)
    wout = lax.all_gather(out_weight, "shard", axis=0, tiled=True)
    taps, bias, gain, first = lax.all_gather((conv_weight, conv_bias, gate_gain, norm_gain), "shard", axis=0, tiled=True)
    sm = jnp.concatenate(
        [
            taps.T.astype(f32),
            rows_to_lanes(bias, CONV_CH),
            rows_to_lanes(gain, CONV_CH),
            rows_to_lanes(first, CONV_CH),
            rows_to_lanes(jnp.repeat(d_skip, HEADDIM), CONV_CH),
        ],
        axis=0,
    )
    hd = jnp.concatenate([rows_to_lanes(dt_bias, 128), rows_to_lanes(a_log, 128), jnp.zeros((6, 128), f32)], axis=0)
    mixed, gtok, dwin, dwout, gsm = layer(
        tokens.reshape(TOKENS, MODEL), cotangent.reshape(TOKENS, MODEL), segment_ids, win, wout, sm, hd
    )
    dwin = lax.psum(lax.psum_scatter(dwin, "shard", scatter_dimension=0, tiled=True), "rep")
    dwout = lax.psum(lax.psum_scatter(dwout, "shard", scatter_dimension=0, tiled=True), "rep")
    gsm = lax.psum(gsm, ("rep", "shard"))
    me = lax.axis_index("shard")

    def owned(v, like):
        return lax.dynamic_slice_in_dim(v, me * like.shape[0], like.shape[0])

    return (
        mixed.reshape(SEQ, LEN, MODEL),
        gtok.reshape(SEQ, LEN, MODEL),
        owned(gsm[6, :MODEL], norm_gain),
        dwin.astype(f32),
        owned(gsm[:CONV].T, conv_weight),
        owned(gsm[4], conv_bias),
        gsm[8, :HEADS],
        gsm[9, :HEADS],
        gsm[7, :INNER].reshape(HEADS, HEADDIM).sum(axis=1),
        owned(gsm[5, :INNER], gate_gain),
        dwout.astype(f32),
    )


def solution(mesh):
    batch = P(("rep", "shard"), None, None)
    return jax.shard_map(
        on_device,
        mesh=mesh,
        in_specs=(
            batch,
            P(("rep", "shard"), None),
            P("shard"),
            P("shard", None),
            P("shard", None),
            P("shard"),
            P(),
            P(),
            P(),
            P("shard"),
            P("shard", None),
            batch,
        ),
        out_specs=(
            batch,
            batch,
            P("shard"),
            P("shard", None),
            P("shard", None),
            P("shard"),
            P(),
            P(),
            P(),
            P("shard"),
            P("shard", None),
        ),
        check_vma=False,
    )
```

```python
from functools import partial

import jax
import jax.numpy as jnp
from jax import lax
from jax.experimental import pallas as pl
from jax.experimental.pallas import tpu as pltpu
from jax.sharding import PartitionSpec as P

HEADS = 24
HEADDIM = 64
STATE = 128
CONV = 4
INNER = 1536
CONV_CH = 1792
MODEL = 768
PROJ = 3352
PADDED = 3584
DT = INNER + CONV_CH
EPS = 1e-05
MESH = pl.DeviceIdType.MESH

LEN = 512
CHUNK = 128
SEQ = 2
TOKENS = SEQ * LEN
QUADS = INNER // 256

f32 = jnp.float32
bf16 = jnp.bfloat16


def nn(a, b):
    return lax.dot_general(a, b, (((1,), (0,)), ((), ())), preferred_element_type=f32)


def nt(a, b):
    return lax.dot_general(a, b, (((1,), (1,)), ((), ())), preferred_element_type=f32)


def tn(a, b):
    return lax.dot_general(a, b, (((0,), (0,)), ((), ())), preferred_element_type=f32)


def exact(a, b):
    return lax.dot_general(
        a, b, (((1,), (0,)), ((), ())), preferred_element_type=f32, precision=lax.Precision.HIGHEST
    )


def sigmoid(v):
    return 0.5 * jnp.tanh(0.5 * v) + 0.5


def partial_sum(a):
    return a.reshape(a.shape[0] // 8, 8, a.shape[1]).sum(axis=0)


def lanes_of(shape):
    return lax.broadcasted_iota(jnp.int32, shape, 1)


def rows_of(shape):
    return lax.broadcasted_iota(jnp.int32, shape, 0)


def packed(a):
    a = jnp.where(lanes_of(a.shape) < HEADS, a, 0.0)
    high = a.astype(bf16).astype(f32)
    rest = a - high
    middle = rest.astype(bf16).astype(f32)
    low = rest - middle
    return (high + pltpu.roll(middle, 32, 1) + pltpu.roll(low, 64, 1)).astype(bf16)


def two_parts(a):
    high = a.astype(bf16)
    return high, (a - high.astype(f32)).astype(bf16)


def y_at(row, count, cols):
    right = cols.start >= MODEL
    base, shift = (LEN, MODEL) if right else (0, 0)
    return pl.ds(pl.multiple_of(base + row, 8), count), slice(cols.start - shift, cols.stop - shift)


def place():
    rep, shard = lax.axis_index("rep"), lax.axis_index("shard")
    core = rep % 2
    px, py = (rep // 2) % 2, rep // 4
    a = px * (1 - core) + py * core
    b = py * (1 - core) + px * core
    return dict(
        rep=rep,
        shard=shard,
        core=core,
        a=a,
        b=b,
        one=rep + (1 - 2 * a) * (2 + 2 * core),
        two=rep + (1 - 2 * b) * (4 - 2 * core),
        mate=rep + 1 - 2 * core,
    )


def greet(at, shards):
    barrier = pltpu.get_barrier_semaphore()
    for who in ("one", "two", "mate"):
        pl.semaphore_signal(barrier, inc=1, device_id=(at[who], at["shard"]), device_id_type=MESH)
    for d in range(1, shards):
        pl.semaphore_signal(
            barrier, inc=1, device_id=(at["rep"], (at["shard"] + d) % shards), device_id_type=MESH
        )
    pl.semaphore_wait(barrier, 2 + shards)


def remote(src, dst, send, recv, rep, shard):
    return pltpu.make_async_remote_copy(
        src_ref=src, dst_ref=dst, send_sem=send, recv_sem=recv, device_id=(rep, shard), device_id_type=MESH
    )


class Gather:
    def __init__(self, at, ref, shards, rows, start, half, sems, part):
        self.at, self.ref, self.shards, self.rows, self.start, self.half = at, ref, shards, rows, start, half
        self.send, self.recv = (lambda kind, d: sems[0].at[part, kind, d]), (lambda kind, d: sems[1].at[part, kind, d])

    def columns(self):
        return pl.ds(pl.multiple_of(self.start + self.at["core"] * self.half, 128), self.half)

    def piece(self, shard, a, b):
        tall = self.rows // 4
        return self.ref.at[pl.ds(pl.multiple_of(shard * self.rows + (2 * b + a) * tall, 16), tall), self.columns()]

    def strip(self, shard):
        return self.ref.at[pl.ds(pl.multiple_of(shard * self.rows, 16), self.rows), self.columns()]

    def source(self, d):
        return (self.at["shard"] + self.shards - d) % self.shards

    def copy(self, kind, d):
        at = self.at
        if kind == 0:
            own = self.piece(at["shard"], at["a"], at["b"])
            return remote(own, own, self.send(0, d), self.recv(0, d), at["rep"], (at["shard"] + d) % self.shards)
        if kind == 4:
            what, who = self.strip(self.source(d)), at["mate"]
        elif kind == 3:
            what, who = self.piece(self.source(d), at["a"], 1 - at["b"]), at["one"]
        else:
            what, who = self.piece(self.source(d), at["a"], at["b"]), at["one"] if kind == 1 else at["two"]
        return remote(what, what, self.send(kind, d), self.recv(kind, d), who, at["shard"])

    def each(self):
        return range(1, self.shards)

    def begin(self):
        for d in self.each():
            self.copy(0, d).start()

    def spread(self):
        for d in self.each():
            self.copy(0, d).wait_recv()
            self.copy(2, d).start()
            self.copy(1, d).start()

    def relay(self):
        for d in self.each():
            self.copy(2, d).wait_recv()
            self.copy(3, d).start()

    def share(self):
        for d in self.each():
            self.copy(1, d).wait_recv()
            self.copy(3, d).wait_recv()
            self.copy(4, d).start()

    def finish(self):
        for d in self.each():
            self.copy(4, d).wait_recv()
            for kind in range(5):
                self.copy(kind, d).wait_send()


def spread_lanes(block, width, offset):
    total = jnp.zeros((8, CONV_CH), f32)
    for z in range(4):
        part = jnp.where(lanes_of((8, 512)) < width, block[z], 0.0)
        part = jnp.concatenate([part, jnp.zeros((8, CONV_CH - 512), f32)], axis=1)
        total = total + (part if z == 0 else pltpu.roll(part, z * offset, 1))
    return total


def setup(seg_ref, s):
    r, c = rows_of((128, 256)), lanes_of((128, 256))
    for j in range(HEADS * 128 // 256):
        s["one128"][:, j * 256 : (j + 1) * 256] = (
            ((r & 31) == ((c + j * 256) >> 7)) & (r < 96)
        ).astype(f32).astype(bf16)
    for j in range(QUADS):
        s["one64"][:, j * 256 : (j + 1) * 256] = (
            ((r & 31) == ((c + j * 256) >> 6)) & (r < 96)
        ).astype(f32).astype(bf16)
    r, c = rows_of((256, 128)), lanes_of((256, 128))
    for j in range(QUADS):
        s["sum64"][j * 256 : (j + 1) * 256, :] = (((r + j * 256) >> 6) == c).astype(f32).astype(bf16)
    s["acc"][...] = jnp.zeros(s["acc"].shape, f32)
    s["pre"][TOKENS:, :] = jnp.zeros((16, CONV_CH), bf16)
    s["up"][:, 0:8, :] = jnp.zeros((2, 8, 256), f32)
    for q in range(SEQ):
        s["segc"][q, 0:8, :] = jnp.full((8, 128), -1.0, f32)
        for i in range(LEN // 128):
            seg = seg_ref[q : q + 1, i * 128 : (i + 1) * 128].astype(f32)
            s["segc"][q, 8 + i * 128 : 8 + (i + 1) * 128, :] = jnp.broadcast_to(seg, (128, 128)).T


def project(q, x_ref, seg_ref, win, sm, hd, s):
    row0 = pl.multiple_of(q * LEN, LEN)
    for i in range(LEN // 128):
        rows = pl.ds(row0 + i * 128, 128)
        x = x_ref[rows, :].astype(f32)
        r = lax.rsqrt(jnp.mean(x * x, axis=1, keepdims=True) + EPS)
        s["nrm"][rows, :] = (x * r * sm[6:7, :MODEL]).astype(bf16)
    seg = s["segc"][q, 8 : 8 + LEN, :]
    place = rows_of((LEN, 128))
    for o in range(1, CONV):
        s["back"][o - 1] = ((seg == pltpu.roll(seg, o, 0)) & (place >= o)).astype(f32)
    rows = pl.ds(row0, LEN)
    raw = nn(s["nrm"][rows, :], win[:, DT : DT + 128]) + hd[0:1, :128]
    s["dtx"][rows, :] = raw
    for j in range(CONV_CH // 256):
        slot = j % 2
        s["up"][slot, 8:, :] = nn(s["nrm"][rows, :], win[:, INNER + j * 256 : INNER + (j + 1) * 256])
        for i in range(LEN // 128):
            for half in range(2):
                c0 = j * 256 + half * 128
                here = pl.ds(row0 + i * 128, 128)
                block = s["up"][slot, i * 128 : i * 128 + 136, half * 128 : (half + 1) * 128]
                u = block[8:]
                tap = lambda k: sm[k : k + 1, c0 : c0 + 128]
                pre = sm[4:5, c0 : c0 + 128] + tap(3) * u
                for o in range(1, CONV):
                    same = s["back"][o - 1, i * 128 : (i + 1) * 128, :]
                    pre = pre + tap(3 - o) * (pltpu.roll(block, o, 0)[8:] * same)
                s["u"][here, c0 : c0 + 128] = u.astype(bf16)
                s["pre"][here, c0 : c0 + 128] = pre.astype(bf16)
                s["xbc"][here, c0 : c0 + 128] = (pre * sigmoid(pre)).astype(bf16)


def chunk_terms(q, c, seg_ref, hd, s):
    row0 = pl.multiple_of(q * LEN + c * CHUNK, CHUNK)
    rows = pl.ds(row0, CHUNK)
    raw = s["dtx"][rows, :]
    dt = jnp.maximum(raw, 0.0) + jnp.log1p(jnp.exp(-jnp.abs(raw)))
    rate = -jnp.exp(hd[1:2, :128]) * dt
    lower = (rows_of((CHUNK, CHUNK)) >= lanes_of((CHUNK, CHUNK))).astype(f32)
    cum = exact(lower, rate)
    source = cum - jnp.log(jnp.maximum(dt, 1e-37))
    start = 8 + c * CHUNK
    segc = s["segc"][q, pl.ds(pl.multiple_of(start, 8), CHUNK), :]
    segr = segc.T
    before = s["segc"][q, pl.ds(pl.multiple_of(start - 8, 8), 8), :][7:8]
    last = segc[CHUNK - 1 : CHUNK]
    carry = (segc == before).astype(f32)
    tail = (segc == last).astype(f32)
    end = cum[CHUNK - 1 : CHUNK, :]
    keep = jnp.exp(end) * (before == last).astype(f32)
    grow = jnp.exp(cum) * carry
    shrink = jnp.exp(end - source) * tail
    return rows, raw, dt, rate, cum, source, segc, segr, grow, shrink, keep


def scan_forward(q, c, seg_ref, sm, hd, s):
    rows, raw, dt, rate, cum, source, segc, segr, grow, shrink, keep = chunk_terms(q, c, seg_ref, hd, s)
    t, k = rows_of((CHUNK, CHUNK)), lanes_of((CHUNK, CHUNK))
    bound = jnp.where((segc == segr) & (t >= k), 3e38, -1e30)
    s["rowv"][...] = source.T
    target = packed(cum)
    grow_p, shrink_p = packed(grow), packed(shrink)
    keep_p = packed(jnp.broadcast_to(keep, (8, 128)))
    bv = s["xbc"][rows, INNER : INNER + STATE]
    cv = s["xbc"][rows, INNER + STATE :]
    gram = nt(cv, bv)
    bt = bv.T
    at = q * (LEN // CHUNK) + c
    left = lanes_of((CHUNK, 128)) < HEADDIM
    for j in range(QUADS):
        cols = slice(j * 256, (j + 1) * 256)
        grow_e = nn(grow_p, s["one64"][:, cols])
        shrink_e = nn(shrink_p, s["one64"][:, cols])
        keep_e = nn(keep_p, s["one64"][:, cols])[0:1, :]
        state = s["state"][:, cols]
        low_state = state.astype(bf16)
        s["states"][at, :, cols] = low_state
        y_state = nn(cv, low_state)
        xv = s["xbc"][rows, cols]
        xw = (xv.astype(f32) * shrink_e).astype(bf16)
        s["state"][:, cols] = state * keep_e + nn(bt, xw)
        parts = []
        for pair in range(2):
            spread = nn(target, s["one128"][:, j * 512 + pair * 256 : j * 512 + (pair + 1) * 256])
            weights = []
            for half in range(2):
                head = 4 * j + 2 * pair + half
                d = spread[:, half * 128 : (half + 1) * 128] - s["rowv"][head : head + 1, :]
                weights.append((gram * jnp.exp(jnp.minimum(d, bound))).astype(bf16))
            x2 = xv[:, pair * 128 : (pair + 1) * 128]
            zero = jnp.zeros_like(x2)
            stack = jnp.concatenate([jnp.where(left, x2, zero), jnp.where(left, zero, x2)], axis=0)
            parts.append(nn(jnp.concatenate(weights, axis=1), stack))
        s["y"][y_at(c * CHUNK, CHUNK, cols)] = (
            jnp.concatenate(parts, axis=1) + y_state * grow_e
        )


def gate(q, i, x_ref, cot_ref, win, wout, sm, mixed_ref, s):
    tall, block = 256, 64
    row0 = q * LEN + i * tall
    rows = pl.ds(pl.multiple_of(row0, tall), tall)
    for j in range(QUADS):
        cols = slice(j * 256, (j + 1) * 256)
        s["z"][:, cols] = nn(s["nrm"][rows, :], win[:, cols])
        s["dg"][:, cols] = nt(cot_ref[rows, :], wout[cols, :])

    @pl.loop(0, tall // block)
    def _(b):
        own = pl.ds(pl.multiple_of(b * block, block), block)
        here = i * tall + b * block
        where = pl.ds(pl.multiple_of(row0 + b * block, block), block)
        square = jnp.zeros((block, 128), f32)
        along = jnp.zeros((block, 128), f32)
        for j in range(INNER // 128):
            cols = slice(j * 128, (j + 1) * 128)
            z = s["z"][own, cols]
            y = s["y"][y_at(here, block, cols)] + sm[7:8, cols] * s["xbc"][where, cols].astype(f32)
            v = y * (z * sigmoid(z))
            square = square + v * v
            along = along + s["dg"][own, cols] * sm[5:6, cols] * v
        r = lax.rsqrt(jnp.sum(square, axis=1, keepdims=True) * (1.0 / INNER) + EPS)
        k = r * r * r * (jnp.sum(along, axis=1, keepdims=True) * (1.0 / INNER))
        for j in range(INNER // 128):
            cols = slice(j * 128, (j + 1) * 128)
            z = s["z"][own, cols]
            dg = s["dg"][own, cols]
            ys = s["y"][y_at(here, block, cols)]
            xv = s["xbc"][where, cols].astype(f32)
            y = ys + sm[7:8, cols] * xv
            sg = sigmoid(z)
            zs = z * sg
            v = y * zs
            vr = v * r
            gain = sm[5:6, cols]
            s["gated"][where, cols] = (vr * gain).astype(bf16)
            s["acc"][5, :, cols] += partial_sum(dg * vr)
            dv = r * (dg * gain) - v * k
            dy = dv * zs
            low_dy = dy.astype(bf16)
            s["dy"][where, cols] = low_dy
            s["dz"][where, cols] = (dv * y * (sg + zs * (1.0 - sg))).astype(bf16)
            s["acc"][7, :, cols] += partial_sum(dy * xv)
            s["dg"][own, cols] = low_dy.astype(f32) * ys

    high, low = two_parts(s["dg"][...])
    s["rowdot"][rows, :] = nn(high, s["sum64"][...]) + nn(low, s["sum64"][...])
    branch = nn(s["gated"][rows, :], wout[...])
    s["mixed"][...] = (x_ref[rows, :].astype(f32) + branch).astype(bf16)
    out = pltpu.make_async_copy(s["mixed"], mixed_ref.at[rows, :], s["mixed_sem"])
    out.start()
    out.wait()


def scan_backward(q, c, seg_ref, sm, hd, s):
    rows, raw, dt, rate, cum, source, segc, segr, grow, shrink, keep = chunk_terms(q, c, seg_ref, hd, s)
    k, t = rows_of((CHUNK, CHUNK)), lanes_of((CHUNK, CHUNK))
    allowed = (segc == segr) & (t >= k)
    bound = jnp.where(allowed, 3e38, -1e30)
    s["rowv"][...] = cum.T
    origin = packed(source)
    grow_p, shrink_p = packed(grow), packed(shrink)
    keep_p = packed(jnp.broadcast_to(keep, (8, 128)))
    bv = s["xbc"][rows, INNER : INNER + STATE]
    cv = s["xbc"][rows, INNER + STATE :]
    gram = nt(bv, cv)
    ct = cv.T
    at = q * (LEN // CHUNK) + c
    left = lanes_of((CHUNK, 128)) < HEADDIM
    dgram = jnp.zeros((CHUNK, CHUNK), f32)
    for j in range(QUADS):
        cols = slice(j * 256, (j + 1) * 256)
        grow_e = nn(grow_p, s["one64"][:, cols])
        s["dys"][:, cols] = (s["dy"][rows, cols].astype(f32) * grow_e).astype(bf16)
        shrink_e = nn(shrink_p, s["one64"][:, cols])
        s["xw"][:, cols] = (s["xbc"][rows, cols].astype(f32) * shrink_e).astype(bf16)
        low_dstate = s["state"][:, cols].astype(bf16)
        s["lowd"][:, cols] = low_dstate
        part = nn(bv, low_dstate) * shrink_e
        s["part"][:, cols] = part
        keep_e = nn(keep_p, s["one64"][:, cols])[0:1, :]
        kept = s["state"][:, cols] * keep_e
        s["tail"][:, cols] = partial_sum(s["xbc"][rows, cols].astype(f32) * part) + partial_sum(
            kept * s["states"][at, :, cols].astype(f32)
        )
        s["state"][:, cols] = kept + nn(ct, s["dys"][:, cols])
    for j in range(INNER // 128):
        cols = slice(j * 128, (j + 1) * 128)
        xv = s["xbc"][rows, cols]
        dy = s["dy"][rows, cols]
        spread = nn(origin, s["one128"][:, j * 256 : (j + 1) * 256])
        zero = jnp.zeros_like(dy)
        stack = jnp.concatenate([jnp.where(left, dy, zero), jnp.where(left, zero, dy)], axis=0)
        dweights = nt(xv, stack)
        weights = []
        for half in range(2):
            head = 2 * j + half
            d = s["rowv"][head : head + 1, :] - spread[:, half * 128 : (half + 1) * 128]
            e = jnp.exp(jnp.minimum(d, bound))
            weights.append((gram * e).astype(bf16))
            dgram = dgram + dweights[:, half * 128 : (half + 1) * 128] * e
        dx = nn(jnp.concatenate(weights, axis=1), stack) + s["part"][:, cols]
        s["part"][:, cols] = xv.astype(f32) * dx
        dx = dx + sm[7:8, cols] * dy.astype(f32)
        pre = s["pre"][rows, cols].astype(f32)
        sg = sigmoid(pre)
        s["pre"][rows, cols] = (dx * (sg * (1.0 + pre * (1.0 - sg)))).astype(bf16)
    high, low = two_parts(s["part"][...])
    colsum = nn(high, s["sum64"][...]) + nn(low, s["sum64"][...])
    high, low = two_parts(s["tail"][...])
    dlast = jnp.sum(nn(high, s["sum64"][...]) + nn(low, s["sum64"][...]), axis=0, keepdims=True)
    dc = nt(s["dys"][...], s["states"][at])
    db = nt(s["xw"][...], s["lowd"][...])
    low_dgram = dgram.astype(bf16)
    db = db + nn(low_dgram, cv)
    dc = dc + tn(low_dgram, bv)
    for index, d in ((0, db), (1, dc)):
        cols = slice(INNER + index * STATE, INNER + (index + 1) * STATE)
        pre = s["pre"][rows, cols].astype(f32)
        sg = sigmoid(pre)
        s["pre"][rows, cols] = (d * (sg * (1.0 + pre * (1.0 - sg)))).astype(bf16)
    dcum = s["rowdot"][rows, :] - colsum
    drate = exact(allowed.astype(f32), dcum) + dlast * (segc == segc[CHUNK - 1 : CHUNK]).astype(f32)
    sg = sigmoid(raw)
    ratio = jnp.where(dt > 1e-30, sg / jnp.maximum(dt, 1e-30), 1.0)
    draw = colsum * ratio - drate * jnp.exp(hd[1:2, :128]) * sg
    draw = jnp.where(lanes_of((CHUNK, 128)) < HEADS, draw, 0.0)
    s["ddt"][rows, :] = draw.astype(bf16)
    s["acc"][8, :, 0:128] += partial_sum(draw)
    s["acc"][9, :, 0:128] += partial_sum(drate * rate)


def conv_backward(q, sm, s):
    row0 = pl.multiple_of(q * LEN, LEN)
    rows = pl.ds(row0, LEN)
    seg = s["segc"][q, 8 : 8 + LEN, :]
    place = rows_of((LEN, 128))
    for o in range(1, CONV):
        s["back"][o - 1] = ((seg == pltpu.roll(seg, LEN - o, 0)) & (place < LEN - o)).astype(f32)
    for j in range(CONV_CH // 128):
        cols = slice(j * 128, (j + 1) * 128)
        sums = [jnp.zeros((8, 128), f32)] * 5
        for i in range(LEN // 128):
            here = pl.ds(row0 + i * 128, 128)
            block = s["pre"][pl.ds(row0 + i * 128, 144), cols].astype(f32)
            ds = block[:128]
            u = s["u"][here, cols].astype(f32)
            du = sm[3:4, cols] * ds
            sums[4] = sums[4] + partial_sum(ds)
            sums[3] = sums[3] + partial_sum(ds * u)
            for o in range(1, CONV):
                moved = pltpu.roll(block, 144 - o, 0)[:128] * s["back"][o - 1, i * 128 : (i + 1) * 128, :]
                du = du + sm[3 - o : 4 - o, cols] * moved
                sums[3 - o] = sums[3 - o] + partial_sum(moved * u)
            s["u"][here, cols] = du.astype(bf16)
        for k in range(5):
            s["acc"][k, :, cols] += sums[k]


def input_gradient(i, x_ref, cot_ref, sm, gtok_ref, s):
    rows = pl.ds(pl.multiple_of(i * 128, 128), 128)
    x = x_ref[rows, :].astype(f32)
    dn = gtok_ref[rows, :]
    r = lax.rsqrt(jnp.mean(x * x, axis=1, keepdims=True) + EPS)
    s["acc"][6, :, 0:MODEL] += partial_sum(dn * (x * r))
    h = dn * sm[6:7, :MODEL]
    k = r * r * r * jnp.mean(h * x, axis=1, keepdims=True)
    gtok_ref[rows, :] = r * h - k * x + cot_ref[rows, :].astype(f32)


SCRATCH = dict(
    win=((MODEL, PADDED), bf16),
    wout=((INNER, MODEL), bf16),
    parts=((4, 8, 512), f32),
    sm=((8, CONV_CH), f32),
    mixed=((256, MODEL), bf16),
    nrm=((TOKENS, MODEL), bf16),
    u=((TOKENS, CONV_CH), bf16),
    pre=((TOKENS + 16, CONV_CH), bf16),
    xbc=((TOKENS, CONV_CH), bf16),
    dtx=((TOKENS, 128), f32),
    gated=((TOKENS, INNER), bf16),
    dy=((TOKENS, INNER), bf16),
    dz=((TOKENS, INNER), bf16),
    ddt=((TOKENS, 128), bf16),
    z=((256, INNER), f32),
    dg=((256, INNER), f32),
    rowdot=((TOKENS, 128), f32),
    dys=((CHUNK, INNER), bf16),
    xw=((CHUNK, INNER), bf16),
    lowd=((CHUNK, INNER), bf16),
    part=((CHUNK, INNER), f32),
    up=((2, 8 + LEN, 256), f32),
    state=((STATE, INNER), f32),
    states=((SEQ * LEN // CHUNK, STATE, INNER), bf16),
    rowv=((128, 128), f32),
    tail=((8, INNER), f32),
    segc=((SEQ, 8 + LEN, 128), f32),
    back=((CONV - 1, LEN, 128), f32),
    one128=((128, HEADS * 128), bf16),
    one64=((128, INNER), bf16),
    sum64=((INNER, 128), bf16),
    acc=((10, 8, CONV_CH), f32),
)


def gather_weights(shards, seg_ref, win_own, wout_own, sm_own, hd, s, send_sems, recv_sems, small_send, small_recv):
    win, wout, sm = s["win"], s["wout"], s["sm"]
    at = place()
    shard = at["shard"]
    rows = pl.ds(pl.multiple_of(shard * (MODEL // shards), 16), MODEL // shards)
    win[rows, DT:] = jnp.zeros((MODEL // shards, PADDED - DT), bf16)
    win[rows, :PROJ] = win_own[...]
    wout[pl.ds(pl.multiple_of(shard * (INNER // shards), 16), INNER // shards), :] = wout_own[...]
    s["parts"][shard] = sm_own[...]
    greet(at, shards)
    sems = (send_sems, recv_sems)
    conv_part = Gather(at, win, shards, MODEL // shards, INNER, (PADDED - INNER) // 2, sems, 0)
    gate_part = Gather(at, win, shards, MODEL // shards, 0, INNER // 2, sems, 1)
    out_part = Gather(at, wout, shards, INNER // shards, 0, MODEL // 2, sems, 2)

    def small(d):
        return remote(
            s["parts"].at[shard],
            s["parts"].at[shard],
            small_send.at[d],
            small_recv.at[d],
            at["rep"],
            (shard + d) % shards,
        )

    for d in range(1, shards):
        small(d).start()
    conv_part.begin()
    setup(seg_ref, s)
    conv_part.spread()
    gate_part.begin()
    out_part.begin()
    conv_part.relay()
    conv_part.share()
    for d in range(1, shards):
        small(d).wait_recv()
        small(d).wait_send()
    row = rows_of((8, CONV_CH))
    taps = spread_lanes(s["parts"], 448, 448)
    gain = spread_lanes(s["parts"], 384, 384)
    first = spread_lanes(s["parts"], 192, 192)
    sm[...] = jnp.where(row < 5, taps, jnp.where(row == 5, gain, first))
    sm[7:8, :] = hd[2:3, :]
    conv_part.finish()
    for part in (gate_part, out_part):
        part.spread()
        part.relay()
        part.share()
    for part in (gate_part, out_part):
        part.finish()


def copy_weights(seg_ref, win_all, wout_all, sm_all, hd, s, sems):
    copies = [
        pltpu.make_async_copy(src, s[name], sems.at[i])
        for i, (src, name) in enumerate(((win_all, "win"), (wout_all, "wout"), (sm_all, "sm")))
    ]
    for copy in copies:
        copy.start()
    setup(seg_ref, s)
    for copy in copies:
        copy.wait()
    s["sm"][7:8, :] = hd[2:3, :]


def layer_kernel(
    direct,
    shards,
    x_ref,
    cot_ref,
    seg_ref,
    win_own,
    wout_own,
    sm_own,
    hd,
    mixed_ref,
    gtok_ref,
    dwin_ref,
    dwout_ref,
    gsm_ref,
    *refs,
):
    s = dict(zip(SCRATCH, refs))
    s["mixed_sem"], *sems = refs[len(SCRATCH) :]
    s["y"] = gtok_ref
    win, wout, sm = s["win"], s["wout"], s["sm"]
    if direct:
        gather_weights(shards, seg_ref, win_own, wout_own, sm_own, hd, s, *sems)
    else:
        copy_weights(seg_ref, win_own, wout_own, sm_own, hd, s, *sems)
    chunks = LEN // CHUNK

    @pl.loop(0, SEQ)
    def _(q):
        project(q, x_ref, seg_ref, win, sm, hd, s)
        s["state"][...] = jnp.zeros((STATE, INNER), f32)

        @pl.loop(0, chunks)
        def _(c):
            scan_forward(q, c, seg_ref, sm, hd, s)

        @pl.loop(0, LEN // 256)
        def _(i):
            gate(q, i, x_ref, cot_ref, win, wout, sm, mixed_ref, s)

    for j in range(QUADS):
        cols = slice(j * 256, (j + 1) * 256)
        dwout_ref[cols, :] = tn(s["gated"][:, cols], cot_ref[...]).astype(bf16)

    @pl.loop(0, SEQ)
    def _(q):
        s["state"][...] = jnp.zeros((STATE, INNER), f32)

        @pl.loop(0, chunks)
        def _(c):
            scan_backward(q, chunks - 1 - c, seg_ref, sm, hd, s)

        conv_backward(q, sm, s)

    turned = s["gated"]
    for i in range(TOKENS // 128):
        for j in range(MODEL // 128):
            turned[j * 128 : (j + 1) * 128, i * 128 : (i + 1) * 128] = s["nrm"][
                i * 128 : (i + 1) * 128, j * 128 : (j + 1) * 128
            ].T
    for j in range(13):
        cols = slice(j * 256, (j + 1) * 256)
        of = s["dz"][:, cols] if j < QUADS else s["u"][:, j * 256 - INNER : (j + 1) * 256 - INNER]
        for i in range(3):
            rows = slice(i * 256, (i + 1) * 256)
            dwin_ref[rows, cols] = nn(turned[rows, :TOKENS], of).astype(bf16)
    dwin_ref[:, 3328:] = nn(turned[:MODEL, :TOKENS], s["ddt"][...]).astype(bf16)[:, :HEADS]

    @pl.loop(0, TOKENS // 256)
    def _(i):
        rows = pl.ds(pl.multiple_of(i * 256, 256), 256)
        for j in range(3):
            cols = slice(j * 256, (j + 1) * 256)
            gtok_ref[rows, cols] = (
                nt(s["dz"][rows, :], win[cols, :INNER])
                + nt(s["u"][rows, :], win[cols, INNER : INNER + CONV_CH])
                + nt(s["ddt"][rows, :], win[cols, DT : DT + 128])
            )

    @pl.loop(0, TOKENS // 128)
    def _(i):
        input_gradient(i, x_ref, cot_ref, sm, gtok_ref, s)

    for k in range(10):
        gsm_ref[k : k + 1, :] = jnp.sum(s["acc"][k], axis=0, keepdims=True)


def reaches(mesh):
    return mesh.shape["rep"] == 8 and mesh.shape["shard"] == 4


def layer(mesh, x, cot, seg, win, wout, sm, hd):
    direct, shards = reaches(mesh), mesh.shape["shard"]
    vmem = pl.BlockSpec(memory_space=pltpu.VMEM)
    hbm = pl.BlockSpec(memory_space=pl.ANY)
    dma = pltpu.SemaphoreType.DMA
    if direct:
        sems = [dma((3, 5, shards)), dma((3, 5, shards)), dma((shards,)), dma((shards,))]
        options = dict(collective_id=0, has_side_effects=True)
        weights = vmem
    else:
        sems, options, weights = [dma((3,))], {}, hbm
    return pl.pallas_call(
        partial(layer_kernel, direct, shards),
        out_shape=(
            jax.ShapeDtypeStruct((TOKENS, MODEL), bf16),
            jax.ShapeDtypeStruct((TOKENS, MODEL), f32),
            jax.ShapeDtypeStruct((MODEL, PROJ), bf16),
            jax.ShapeDtypeStruct((INNER, MODEL), bf16),
            jax.ShapeDtypeStruct((10, CONV_CH), f32),
        ),
        in_specs=[vmem] * 3 + [weights] * 3 + [vmem],
        out_specs=[hbm] + [vmem] * 4,
        scratch_shapes=[pltpu.VMEM(shape, kind) for shape, kind in SCRATCH.values()] + [dma] + sems,
        compiler_params=pltpu.CompilerParams(vmem_limit_bytes=67043328, **options),
        name="layer",
    )(x, cot, seg, win, wout, sm, hd)


def rows_to_lanes(v, width):
    return jnp.pad(v.astype(f32), (0, width - v.shape[0]))[None]


def on_device(mesh, tokens, segment_ids, norm_gain, in_weight, conv_weight, conv_bias, dt_bias, a_log, d_skip, gate_gain, out_weight, cotangent):
    small = (conv_bias, gate_gain, norm_gain)
    if reaches(mesh):
        win, wout = in_weight, out_weight
        sm = jnp.concatenate([conv_weight.T.astype(f32)] + [rows_to_lanes(v, 512 - 64) for v in small + (norm_gain,)])
        sm = jnp.pad(sm, ((0, 0), (0, 64)))
    else:
        win, wout, taps, *small = lax.all_gather(
            (in_weight, out_weight, conv_weight) + small, "shard", axis=0, tiled=True
        )
        win = jnp.pad(win, ((0, 0), (0, PADDED - PROJ)))
        sm = jnp.concatenate([taps.T.astype(f32)] + [rows_to_lanes(v, CONV_CH) for v in (*small, small[-1])])
    hd = jnp.concatenate(
        [rows_to_lanes(v, CONV_CH) for v in (dt_bias, a_log, jnp.repeat(d_skip, HEADDIM))] + [jnp.zeros((5, CONV_CH), f32)],
        axis=0,
    )
    mixed, gtok, dwin, dwout, gsm = layer(
        mesh,
        tokens.reshape(TOKENS, MODEL), cotangent.reshape(TOKENS, MODEL), segment_ids, win, wout, sm, hd
    )
    dwin = lax.psum(lax.psum_scatter(dwin, "shard", scatter_dimension=0, tiled=True), "rep")
    dwout = lax.psum(lax.psum_scatter(dwout, "shard", scatter_dimension=0, tiled=True), "rep")
    gsm = lax.psum(gsm, ("rep", "shard"))
    me = lax.axis_index("shard")

    def owned(v, like):
        return lax.dynamic_slice_in_dim(v, me * like.shape[0], like.shape[0])

    return (
        mixed.reshape(SEQ, LEN, MODEL),
        gtok.reshape(SEQ, LEN, MODEL),
        owned(gsm[6, :MODEL], norm_gain),
        dwin.astype(f32),
        owned(gsm[:CONV].T, conv_weight),
        owned(gsm[4], conv_bias),
        gsm[8, :HEADS],
        gsm[9, :HEADS],
        gsm[7, :INNER].reshape(HEADS, HEADDIM).sum(axis=1),
        owned(gsm[5, :INNER], gate_gain),
        dwout.astype(f32),
    )


def solution(mesh):
    batch = P(("rep", "shard"), None, None)
    return jax.shard_map(
        partial(on_device, mesh),
        mesh=mesh,
        in_specs=(
            batch,
            P(("rep", "shard"), None),
            P("shard"),
            P("shard", None),
            P("shard", None),
            P("shard"),
            P(),
            P(),
            P(),
            P("shard"),
            P("shard", None),
            batch,
        ),
        out_specs=(
            batch,
            batch,
            P("shard"),
            P("shard", None),
            P("shard", None),
            P("shard"),
            P(),
            P(),
            P(),
            P("shard"),
            P("shard", None),
        ),
        check_vma=False,
    )
```

```python
from functools import partial

import jax
import jax.numpy as jnp
from jax import lax
from jax.experimental import pallas as pl
from jax.experimental.pallas import tpu as pltpu
from jax.sharding import PartitionSpec as P

HEADS = 24
HEADDIM = 64
STATE = 128
CONV = 4
INNER = 1536
CONV_CH = 1792
MODEL = 768
PROJ = 3352
PADDED = 3584
DT = INNER + CONV_CH
EPS = 1e-05
MESH = pl.DeviceIdType.MESH

LEN = 512
CHUNK = 128
SEQ = 2
TOKENS = SEQ * LEN
QUADS = INNER // 256

f32 = jnp.float32
bf16 = jnp.bfloat16


def nn(a, b):
    return lax.dot_general(a, b, (((1,), (0,)), ((), ())), preferred_element_type=f32)


def nt(a, b):
    return lax.dot_general(a, b, (((1,), (1,)), ((), ())), preferred_element_type=f32)


def tn(a, b):
    return lax.dot_general(a, b, (((0,), (0,)), ((), ())), preferred_element_type=f32)


def exact(a, b):
    return lax.dot_general(
        a, b, (((1,), (0,)), ((), ())), preferred_element_type=f32, precision=lax.Precision.HIGHEST
    )


def sigmoid(v):
    return 0.5 * jnp.tanh(0.5 * v) + 0.5


def partial_sum(a):
    return a.reshape(a.shape[0] // 8, 8, a.shape[1]).sum(axis=0)


def lanes_of(shape):
    return lax.broadcasted_iota(jnp.int32, shape, 1)


def rows_of(shape):
    return lax.broadcasted_iota(jnp.int32, shape, 0)


def packed(a):
    a = jnp.where(lanes_of(a.shape) < HEADS, a, 0.0)
    high = a.astype(bf16).astype(f32)
    rest = a - high
    middle = rest.astype(bf16).astype(f32)
    low = rest - middle
    return (high + pltpu.roll(middle, 32, 1) + pltpu.roll(low, 64, 1)).astype(bf16)


def two_parts(a):
    high = a.astype(bf16)
    return high, (a - high.astype(f32)).astype(bf16)


def y_at(row, count, cols):
    right = cols.start >= MODEL
    base, shift = (LEN, MODEL) if right else (0, 0)
    return pl.ds(pl.multiple_of(base + row, 8), count), slice(cols.start - shift, cols.stop - shift)


def place():
    rep, shard = lax.axis_index("rep"), lax.axis_index("shard")
    core = rep % 2
    px, py = (rep // 2) % 2, rep // 4
    a = px * (1 - core) + py * core
    b = py * (1 - core) + px * core
    return dict(
        rep=rep,
        shard=shard,
        core=core,
        a=a,
        b=b,
        one=rep + (1 - 2 * a) * (2 + 2 * core),
        two=rep + (1 - 2 * b) * (4 - 2 * core),
        mate=rep + 1 - 2 * core,
    )


def greet(at, shards):
    barrier = pltpu.get_barrier_semaphore()
    for who in ("one", "two", "mate"):
        pl.semaphore_signal(barrier, inc=1, device_id=(at[who], at["shard"]), device_id_type=MESH)
    for d in range(1, shards):
        pl.semaphore_signal(
            barrier, inc=1, device_id=(at["rep"], (at["shard"] + d) % shards), device_id_type=MESH
        )
    pl.semaphore_wait(barrier, 2 + shards)


def remote(src, dst, send, recv, rep, shard):
    return pltpu.make_async_remote_copy(
        src_ref=src, dst_ref=dst, send_sem=send, recv_sem=recv, device_id=(rep, shard), device_id_type=MESH
    )


class Gather:
    def __init__(self, at, ref, shards, rows, start, half, sems, part):
        self.at, self.ref, self.shards, self.rows, self.start, self.half = at, ref, shards, rows, start, half
        self.send, self.recv = (lambda kind, d: sems[0].at[part, kind, d]), (lambda kind, d: sems[1].at[part, kind, d])

    def columns(self):
        return pl.ds(pl.multiple_of(self.start + self.at["core"] * self.half, 128), self.half)

    def piece(self, shard, a, b):
        tall = self.rows // 4
        return self.ref.at[pl.ds(pl.multiple_of(shard * self.rows + (2 * b + a) * tall, 16), tall), self.columns()]

    def strip(self, shard):
        return self.ref.at[pl.ds(pl.multiple_of(shard * self.rows, 16), self.rows), self.columns()]

    def source(self, d):
        return (self.at["shard"] + self.shards - d) % self.shards

    def copy(self, kind, d):
        at = self.at
        if kind == 0:
            own = self.piece(at["shard"], at["a"], at["b"])
            return remote(own, own, self.send(0, d), self.recv(0, d), at["rep"], (at["shard"] + d) % self.shards)
        if kind == 4:
            what, who = self.strip(self.source(d)), at["mate"]
        elif kind == 3:
            what, who = self.piece(self.source(d), at["a"], 1 - at["b"]), at["one"]
        else:
            what, who = self.piece(self.source(d), at["a"], at["b"]), at["one"] if kind == 1 else at["two"]
        return remote(what, what, self.send(kind, d), self.recv(kind, d), who, at["shard"])

    def each(self):
        return range(1, self.shards)

    def begin(self):
        for d in self.each():
            self.copy(0, d).start()

    def spread(self):
        for d in self.each():
            self.copy(0, d).wait_recv()
            self.copy(2, d).start()
            self.copy(1, d).start()

    def relay(self):
        for d in self.each():
            self.copy(2, d).wait_recv()
            self.copy(3, d).start()

    def share(self):
        for d in self.each():
            self.copy(1, d).wait_recv()
            self.copy(3, d).wait_recv()
            self.copy(4, d).start()

    def finish(self):
        for d in self.each():
            self.copy(4, d).wait_recv()
            for kind in range(5):
                self.copy(kind, d).wait_send()


def meet(at, shards, sem):
    for who in ("one", "two", "mate"):
        pl.semaphore_signal(sem, inc=1, device_id=(at[who], at["shard"]), device_id_type=MESH)
    for d in range(1, shards):
        pl.semaphore_signal(sem, inc=1, device_id=(at["rep"], (at["shard"] + d) % shards), device_id_type=MESH)


def met(shards, sem):
    pl.semaphore_wait(sem, 2 + shards)


class Reduce:
    def __init__(self, at, grad, rows, half, slots, out, column, sems, part, local):
        self.at, self.grad, self.rows, self.half, self.slots = at, grad, rows, half, slots
        self.out, self.column = out, column
        self.tall, self.own_rows = rows // 16, rows // 4
        self.send, self.recv = (lambda i: sems[0].at[part, i]), (lambda i: sems[1].at[part, i])
        self.local = local
        self.keep = pl.ds(pl.multiple_of(at["core"] * half, 128), half)
        self.give = pl.ds(pl.multiple_of((1 - at["core"]) * half, 128), half)

    def slot(self, level, start, count):
        ref, row, column = self.slots[level]
        return ref.at[pl.ds(row + start, count), pl.ds(column, self.half)]

    def at_block(self, shard, a, b):
        return pl.multiple_of(shard * self.own_rows + (2 * b + a) * self.tall, 16)

    def block(self, shard, a, b):
        return self.grad.at[pl.ds(self.at_block(shard, a, b), self.tall), self.keep]

    def to(self, src, dst, index, who):
        rep, shard = who
        return remote(src, dst, self.send(index), self.recv(index), rep, shard)

    def partner(self, name):
        return self.at[name], self.at["shard"]

    def add(self, start, level, place_in_slot):
        rows = pl.ds(start, self.tall)
        got = self.slot(level, place_in_slot, self.tall)[...]
        self.grad[rows, self.keep] = (self.grad[rows, self.keep].astype(f32) + got.astype(f32)).astype(bf16)

    def halves(self):
        whole = self.slot(0, 0, self.rows)
        return self.to(self.grad.at[:, self.give], whole, 0, self.partner("mate"))

    def begin(self):
        self.halves().start()

    def first(self):
        at = self.at
        self.halves().wait_recv()

        @pl.loop(0, 16)
        def _(i):
            start = pl.multiple_of(i * self.tall, 16)
            self.add(start, 0, start)

        for shard in range(4):
            for b in range(2):
                self.to(
                    self.block(shard, 1 - at["a"], b),
                    self.slot(1, (2 * shard + b) * self.tall, self.tall),
                    1,
                    self.partner("one"),
                ).start()

    def all_of(self, level, index, name):
        whole = self.slot(level, 0, self.rows >> level)
        return self.to(whole, whole, index, self.partner(name))

    def second(self):
        at = self.at
        self.all_of(1, 1, "one").wait_recv()
        for shard in range(4):
            for b in range(2):
                self.add(self.at_block(shard, at["a"], b), 1, (2 * shard + b) * self.tall)
        for shard in range(4):
            self.to(
                self.block(shard, at["a"], 1 - at["b"]),
                self.slot(2, shard * self.tall, self.tall),
                2,
                self.partner("two"),
            ).start()

    def across(self, d):
        at = self.at
        shard = (at["shard"] + d) % 4
        return self.to(
            self.block(shard, at["a"], at["b"]), self.slot(3, (d - 1) * self.tall, self.tall), 2 + d, (at["rep"], shard)
        )

    def third(self):
        at = self.at
        self.all_of(2, 2, "two").wait_recv()
        for shard in range(4):
            self.add(self.at_block(shard, at["a"], at["b"]), 2, shard * self.tall)
        for d in range(1, 4):
            self.across(d).start()

    def landed(self, a, b):
        rows = pl.ds(pl.multiple_of((2 * b + a) * self.tall, 16), self.tall)
        return self.out.at[rows, pl.ds(pl.multiple_of(self.column + self.at["core"] * self.half, 128), self.half)]

    def spread(self, index):
        at = self.at
        own = self.block(at["shard"], at["a"], at["b"])
        return self.to(own, self.landed(at["a"], at["b"]), index, self.partner("one" if index == 6 else "two"))

    def home(self):
        at = self.at
        own = self.block(at["shard"], at["a"], at["b"])
        return pltpu.make_async_copy(own, self.landed(at["a"], at["b"]), self.local)

    def fourth(self):
        at = self.at
        for d in range(1, 4):
            self.across(d).wait_recv()
        rows = pl.ds(self.at_block(at["shard"], at["a"], at["b"]), self.tall)
        total = self.grad[rows, self.keep].astype(f32)
        for d in range(1, 4):
            total = total + self.slot(3, (d - 1) * self.tall, self.tall)[...].astype(f32)
        self.grad[rows, self.keep] = total.astype(bf16)
        self.spread(7).start()
        self.spread(6).start()
        self.home().start()

    def relay(self):
        at = self.at
        far = self.landed(at["a"], 1 - at["b"])
        return self.to(far, far, 8, self.partner("one"))

    def fifth(self):
        self.spread(7).wait_recv()
        self.relay().start()

    def strip(self):
        columns = pl.ds(pl.multiple_of(self.column + self.at["core"] * self.half, 128), self.half)
        return self.to(self.out.at[:, columns], self.out.at[:, columns], 9, self.partner("mate"))

    def sixth(self):
        self.home().wait()
        self.spread(6).wait_recv()
        self.relay().wait_recv()
        self.strip().start()

    def seventh(self):
        self.strip().wait_recv()
        self.halves().wait_send()
        self.all_of(1, 1, "one").wait_send()
        self.all_of(2, 2, "two").wait_send()
        for d in range(1, 4):
            self.across(d).wait_send()
        self.spread(6).wait_send()
        self.spread(7).wait_send()
        self.relay().wait_send()
        self.strip().wait_send()


class Total:
    def __init__(self, at, mine, slots, sems):
        self.at, self.mine, self.slots, self.sems = at, mine, slots, sems

    def copy(self, index):
        at = self.at
        if index < 3:
            who = at[("mate", "one", "two")[index]], at["shard"]
        else:
            who = at["rep"], (at["shard"] + index - 2) % 4
        return remote(self.mine.at[min(index, 3)], self.slot(index), self.sems[0].at[index], self.sems[1].at[index], *who)

    def slot(self, index):
        return self.slots.at[index // 3, pl.ds(8 + (index % 3) * 112, 112), :]

    def begin(self):
        self.copy(0).start()

    def step(self, index):
        self.copy(index).wait_recv()
        self.mine[index + 1] = self.mine[index] + self.slot(index)[...]
        for following in (index + 1,) if index < 2 else (3, 4, 5):
            self.copy(following).start()

    def finish(self, out):
        total = self.mine[3]
        for index in (3, 4, 5):
            self.copy(index).wait_recv()
            total = total + self.slot(index)[...]
        for index in range(6):
            self.copy(index).wait_send()
        out[...] = total


def spread_lanes(block, width, offset):
    total = jnp.zeros((8, CONV_CH), f32)
    for z in range(4):
        part = jnp.where(lanes_of((8, 512)) < width, block[z], 0.0)
        part = jnp.concatenate([part, jnp.zeros((8, CONV_CH - 512), f32)], axis=1)
        total = total + (part if z == 0 else pltpu.roll(part, z * offset, 1))
    return total


def setup(seg_ref, s):
    r, c = rows_of((128, 256)), lanes_of((128, 256))
    for j in range(HEADS * 128 // 256):
        s["one128"][:, j * 256 : (j + 1) * 256] = (
            ((r & 31) == ((c + j * 256) >> 7)) & (r < 96)
        ).astype(f32).astype(bf16)
    for j in range(QUADS):
        s["one64"][:, j * 256 : (j + 1) * 256] = (
            ((r & 31) == ((c + j * 256) >> 6)) & (r < 96)
        ).astype(f32).astype(bf16)
    r, c = rows_of((256, 128)), lanes_of((256, 128))
    for j in range(QUADS):
        s["sum64"][j * 256 : (j + 1) * 256, :] = (((r + j * 256) >> 6) == c).astype(f32).astype(bf16)
    s["acc"][...] = jnp.zeros(s["acc"].shape, f32)
    s["pre"][TOKENS:, :] = jnp.zeros((16, CONV_CH), bf16)
    s["up"][:, 0:8, :] = jnp.zeros((2, 8, 256), f32)
    for q in range(SEQ):
        s["segc"][q, 0:8, :] = jnp.full((8, 128), -1.0, f32)
        for i in range(LEN // 128):
            seg = seg_ref[q : q + 1, i * 128 : (i + 1) * 128].astype(f32)
            s["segc"][q, 8 + i * 128 : 8 + (i + 1) * 128, :] = jnp.broadcast_to(seg, (128, 128)).T


def project(q, x_ref, seg_ref, win, sm, hd, s):
    row0 = pl.multiple_of(q * LEN, LEN)
    for i in range(LEN // 128):
        rows = pl.ds(row0 + i * 128, 128)
        x = x_ref[rows, :].astype(f32)
        r = lax.rsqrt(jnp.mean(x * x, axis=1, keepdims=True) + EPS)
        s["nrm"][rows, :] = (x * r * sm[6:7, :MODEL]).astype(bf16)
    seg = s["segc"][q, 8 : 8 + LEN, :]
    place = rows_of((LEN, 128))
    for o in range(1, CONV):
        s["back"][o - 1] = ((seg == pltpu.roll(seg, o, 0)) & (place >= o)).astype(f32)
    rows = pl.ds(row0, LEN)
    raw = nn(s["nrm"][rows, :], win[:, DT : DT + 128]) + hd[0:1, :128]
    s["dtx"][rows, :] = raw
    for j in range(CONV_CH // 256):
        slot = j % 2
        s["up"][slot, 8:, :] = nn(s["nrm"][rows, :], win[:, INNER + j * 256 : INNER + (j + 1) * 256])
        for i in range(LEN // 128):
            for half in range(2):
                c0 = j * 256 + half * 128
                here = pl.ds(row0 + i * 128, 128)
                block = s["up"][slot, i * 128 : i * 128 + 136, half * 128 : (half + 1) * 128]
                u = block[8:]
                tap = lambda k: sm[k : k + 1, c0 : c0 + 128]
                pre = sm[4:5, c0 : c0 + 128] + tap(3) * u
                for o in range(1, CONV):
                    same = s["back"][o - 1, i * 128 : (i + 1) * 128, :]
                    pre = pre + tap(3 - o) * (pltpu.roll(block, o, 0)[8:] * same)
                s["u"][here, c0 : c0 + 128] = u.astype(bf16)
                s["pre"][here, c0 : c0 + 128] = pre.astype(bf16)
                s["xbc"][here, c0 : c0 + 128] = (pre * sigmoid(pre)).astype(bf16)


def chunk_terms(q, c, seg_ref, hd, s):
    row0 = pl.multiple_of(q * LEN + c * CHUNK, CHUNK)
    rows = pl.ds(row0, CHUNK)
    raw = s["dtx"][rows, :]
    dt = jnp.maximum(raw, 0.0) + jnp.log1p(jnp.exp(-jnp.abs(raw)))
    rate = -jnp.exp(hd[1:2, :128]) * dt
    lower = (rows_of((CHUNK, CHUNK)) >= lanes_of((CHUNK, CHUNK))).astype(f32)
    cum = exact(lower, rate)
    source = cum - jnp.log(jnp.maximum(dt, 1e-37))
    start = 8 + c * CHUNK
    segc = s["segc"][q, pl.ds(pl.multiple_of(start, 8), CHUNK), :]
    segr = segc.T
    before = s["segc"][q, pl.ds(pl.multiple_of(start - 8, 8), 8), :][7:8]
    last = segc[CHUNK - 1 : CHUNK]
    carry = (segc == before).astype(f32)
    tail = (segc == last).astype(f32)
    end = cum[CHUNK - 1 : CHUNK, :]
    keep = jnp.exp(end) * (before == last).astype(f32)
    grow = jnp.exp(cum) * carry
    shrink = jnp.exp(end - source) * tail
    return rows, raw, dt, rate, cum, source, segc, segr, grow, shrink, keep


def scan_forward(q, c, seg_ref, sm, hd, s):
    rows, raw, dt, rate, cum, source, segc, segr, grow, shrink, keep = chunk_terms(q, c, seg_ref, hd, s)
    t, k = rows_of((CHUNK, CHUNK)), lanes_of((CHUNK, CHUNK))
    bound = jnp.where((segc == segr) & (t >= k), 3e38, -1e30)
    s["rowv"][...] = source.T
    target = packed(cum)
    grow_p, shrink_p = packed(grow), packed(shrink)
    keep_p = packed(jnp.broadcast_to(keep, (8, 128)))
    bv = s["xbc"][rows, INNER : INNER + STATE]
    cv = s["xbc"][rows, INNER + STATE :]
    gram = nt(cv, bv)
    bt = bv.T
    at = q * (LEN // CHUNK) + c
    left = lanes_of((CHUNK, 128)) < HEADDIM
    for j in range(QUADS):
        cols = slice(j * 256, (j + 1) * 256)
        grow_e = nn(grow_p, s["one64"][:, cols])
        shrink_e = nn(shrink_p, s["one64"][:, cols])
        keep_e = nn(keep_p, s["one64"][:, cols])[0:1, :]
        state = s["state"][:, cols]
        low_state = state.astype(bf16)
        s["states"][at, :, cols] = low_state
        y_state = nn(cv, low_state)
        xv = s["xbc"][rows, cols]
        xw = (xv.astype(f32) * shrink_e).astype(bf16)
        s["state"][:, cols] = state * keep_e + nn(bt, xw)
        parts = []
        for pair in range(2):
            spread = nn(target, s["one128"][:, j * 512 + pair * 256 : j * 512 + (pair + 1) * 256])
            weights = []
            for half in range(2):
                head = 4 * j + 2 * pair + half
                d = spread[:, half * 128 : (half + 1) * 128] - s["rowv"][head : head + 1, :]
                weights.append((gram * jnp.exp(jnp.minimum(d, bound))).astype(bf16))
            x2 = xv[:, pair * 128 : (pair + 1) * 128]
            zero = jnp.zeros_like(x2)
            stack = jnp.concatenate([jnp.where(left, x2, zero), jnp.where(left, zero, x2)], axis=0)
            parts.append(nn(jnp.concatenate(weights, axis=1), stack))
        s["y"][y_at(c * CHUNK, CHUNK, cols)] = (
            jnp.concatenate(parts, axis=1) + y_state * grow_e
        )


def gate(q, i, x_ref, cot_ref, win, wout, sm, mixed_ref, s):
    tall, block = 256, 64
    row0 = q * LEN + i * tall
    rows = pl.ds(pl.multiple_of(row0, tall), tall)
    for j in range(QUADS):
        cols = slice(j * 256, (j + 1) * 256)
        s["z"][:, cols] = nn(s["nrm"][rows, :], win[:, cols])
        s["dg"][:, cols] = nt(cot_ref[rows, :], wout[cols, :])

    @pl.loop(0, tall // block)
    def _(b):
        own = pl.ds(pl.multiple_of(b * block, block), block)
        here = i * tall + b * block
        where = pl.ds(pl.multiple_of(row0 + b * block, block), block)
        square = jnp.zeros((block, 128), f32)
        along = jnp.zeros((block, 128), f32)
        for j in range(INNER // 128):
            cols = slice(j * 128, (j + 1) * 128)
            z = s["z"][own, cols]
            y = s["y"][y_at(here, block, cols)] + sm[7:8, cols] * s["xbc"][where, cols].astype(f32)
            v = y * (z * sigmoid(z))
            square = square + v * v
            along = along + s["dg"][own, cols] * sm[5:6, cols] * v
        r = lax.rsqrt(jnp.sum(square, axis=1, keepdims=True) * (1.0 / INNER) + EPS)
        k = r * r * r * (jnp.sum(along, axis=1, keepdims=True) * (1.0 / INNER))
        for j in range(INNER // 128):
            cols = slice(j * 128, (j + 1) * 128)
            z = s["z"][own, cols]
            dg = s["dg"][own, cols]
            ys = s["y"][y_at(here, block, cols)]
            xv = s["xbc"][where, cols].astype(f32)
            y = ys + sm[7:8, cols] * xv
            sg = sigmoid(z)
            zs = z * sg
            v = y * zs
            vr = v * r
            gain = sm[5:6, cols]
            s["gated"][where, cols] = (vr * gain).astype(bf16)
            s["acc"][5, :, cols] += partial_sum(dg * vr)
            dv = r * (dg * gain) - v * k
            dy = dv * zs
            low_dy = dy.astype(bf16)
            s["dy"][where, cols] = low_dy
            s["dz"][where, cols] = (dv * y * (sg + zs * (1.0 - sg))).astype(bf16)
            s["acc"][7, :, cols] += partial_sum(dy * xv)
            s["dg"][own, cols] = low_dy.astype(f32) * ys

    high, low = two_parts(s["dg"][...])
    s["rowdot"][rows, :] = nn(high, s["sum64"][...]) + nn(low, s["sum64"][...])
    branch = nn(s["gated"][rows, :], wout[...])
    s["mixed"][...] = (x_ref[rows, :].astype(f32) + branch).astype(bf16)
    out = pltpu.make_async_copy(s["mixed"], mixed_ref.at[rows, :], s["mixed_sem"])
    out.start()
    out.wait()


def scan_backward(q, c, seg_ref, sm, hd, s):
    rows, raw, dt, rate, cum, source, segc, segr, grow, shrink, keep = chunk_terms(q, c, seg_ref, hd, s)
    k, t = rows_of((CHUNK, CHUNK)), lanes_of((CHUNK, CHUNK))
    allowed = (segc == segr) & (t >= k)
    bound = jnp.where(allowed, 3e38, -1e30)
    s["rowv"][...] = cum.T
    origin = packed(source)
    grow_p, shrink_p = packed(grow), packed(shrink)
    keep_p = packed(jnp.broadcast_to(keep, (8, 128)))
    bv = s["xbc"][rows, INNER : INNER + STATE]
    cv = s["xbc"][rows, INNER + STATE :]
    gram = nt(bv, cv)
    ct = cv.T
    at = q * (LEN // CHUNK) + c
    left = lanes_of((CHUNK, 128)) < HEADDIM
    dgram = jnp.zeros((CHUNK, CHUNK), f32)
    for j in range(QUADS):
        cols = slice(j * 256, (j + 1) * 256)
        grow_e = nn(grow_p, s["one64"][:, cols])
        s["dys"][:, cols] = (s["dy"][rows, cols].astype(f32) * grow_e).astype(bf16)
        shrink_e = nn(shrink_p, s["one64"][:, cols])
        s["xw"][:, cols] = (s["xbc"][rows, cols].astype(f32) * shrink_e).astype(bf16)
        low_dstate = s["state"][:, cols].astype(bf16)
        s["lowd"][:, cols] = low_dstate
        part = nn(bv, low_dstate) * shrink_e
        s["part"][:CHUNK, cols] = part
        keep_e = nn(keep_p, s["one64"][:, cols])[0:1, :]
        kept = s["state"][:, cols] * keep_e
        s["tail"][:, cols] = partial_sum(s["xbc"][rows, cols].astype(f32) * part) + partial_sum(
            kept * s["states"][at, :, cols].astype(f32)
        )
        s["state"][:, cols] = kept + nn(ct, s["dys"][:, cols])
    for j in range(INNER // 128):
        cols = slice(j * 128, (j + 1) * 128)
        xv = s["xbc"][rows, cols]
        dy = s["dy"][rows, cols]
        spread = nn(origin, s["one128"][:, j * 256 : (j + 1) * 256])
        zero = jnp.zeros_like(dy)
        stack = jnp.concatenate([jnp.where(left, dy, zero), jnp.where(left, zero, dy)], axis=0)
        dweights = nt(xv, stack)
        weights = []
        for half in range(2):
            head = 2 * j + half
            d = s["rowv"][head : head + 1, :] - spread[:, half * 128 : (half + 1) * 128]
            e = jnp.exp(jnp.minimum(d, bound))
            weights.append((gram * e).astype(bf16))
            dgram = dgram + dweights[:, half * 128 : (half + 1) * 128] * e
        dx = nn(jnp.concatenate(weights, axis=1), stack) + s["part"][:CHUNK, cols]
        s["part"][:CHUNK, cols] = xv.astype(f32) * dx
        dx = dx + sm[7:8, cols] * dy.astype(f32)
        pre = s["pre"][rows, cols].astype(f32)
        sg = sigmoid(pre)
        s["pre"][rows, cols] = (dx * (sg * (1.0 + pre * (1.0 - sg)))).astype(bf16)
    high, low = two_parts(s["part"][:CHUNK, :])
    colsum = nn(high, s["sum64"][...]) + nn(low, s["sum64"][...])
    high, low = two_parts(s["tail"][...])
    dlast = jnp.sum(nn(high, s["sum64"][...]) + nn(low, s["sum64"][...]), axis=0, keepdims=True)
    dc = nt(s["dys"][...], s["states"][at])
    db = nt(s["xw"][...], s["lowd"][...])
    low_dgram = dgram.astype(bf16)
    db = db + nn(low_dgram, cv)
    dc = dc + tn(low_dgram, bv)
    for index, d in ((0, db), (1, dc)):
        cols = slice(INNER + index * STATE, INNER + (index + 1) * STATE)
        pre = s["pre"][rows, cols].astype(f32)
        sg = sigmoid(pre)
        s["pre"][rows, cols] = (d * (sg * (1.0 + pre * (1.0 - sg)))).astype(bf16)
    dcum = s["rowdot"][rows, :] - colsum
    drate = exact(allowed.astype(f32), dcum) + dlast * (segc == segc[CHUNK - 1 : CHUNK]).astype(f32)
    sg = sigmoid(raw)
    ratio = jnp.where(dt > 1e-30, sg / jnp.maximum(dt, 1e-30), 1.0)
    draw = colsum * ratio - drate * jnp.exp(hd[1:2, :128]) * sg
    draw = jnp.where(lanes_of((CHUNK, 128)) < HEADS, draw, 0.0)
    s["ddt"][rows, :] = draw.astype(bf16)
    s["acc"][8, :, 0:128] += partial_sum(draw)
    s["acc"][9, :, 0:128] += partial_sum(drate * rate)


def conv_backward(q, sm, s):
    row0 = pl.multiple_of(q * LEN, LEN)
    rows = pl.ds(row0, LEN)
    seg = s["segc"][q, 8 : 8 + LEN, :]
    place = rows_of((LEN, 128))
    for o in range(1, CONV):
        s["back"][o - 1] = ((seg == pltpu.roll(seg, LEN - o, 0)) & (place < LEN - o)).astype(f32)
    for j in range(CONV_CH // 128):
        cols = slice(j * 128, (j + 1) * 128)
        sums = [jnp.zeros((8, 128), f32)] * 5
        for i in range(LEN // 128):
            here = pl.ds(row0 + i * 128, 128)
            block = s["pre"][pl.ds(row0 + i * 128, 144), cols].astype(f32)
            ds = block[:128]
            u = s["u"][here, cols].astype(f32)
            du = sm[3:4, cols] * ds
            sums[4] = sums[4] + partial_sum(ds)
            sums[3] = sums[3] + partial_sum(ds * u)
            for o in range(1, CONV):
                moved = pltpu.roll(block, 144 - o, 0)[:128] * s["back"][o - 1, i * 128 : (i + 1) * 128, :]
                du = du + sm[3 - o : 4 - o, cols] * moved
                sums[3 - o] = sums[3 - o] + partial_sum(moved * u)
            s["u"][here, cols] = du.astype(bf16)
        for k in range(5):
            s["acc"][k, :, cols] += sums[k]


def input_gradient(i, x_ref, cot_ref, sm, gtok_ref, s):
    rows = pl.ds(pl.multiple_of(i * 128, 128), 128)
    x = x_ref[rows, :].astype(f32)
    dn = gtok_ref[rows, :]
    r = lax.rsqrt(jnp.mean(x * x, axis=1, keepdims=True) + EPS)
    s["acc"][6, :, 0:MODEL] += partial_sum(dn * (x * r))
    h = dn * sm[6:7, :MODEL]
    k = r * r * r * jnp.mean(h * x, axis=1, keepdims=True)
    gtok_ref[rows, :] = r * h - k * x + cot_ref[rows, :].astype(f32)


SCRATCH = dict(
    win=((MODEL, PADDED), bf16),
    wout=((INNER, MODEL), bf16),
    parts=((4, 8, 512), f32),
    sm=((8, CONV_CH), f32),
    mixed=((256, MODEL), bf16),
    nrm=((TOKENS, MODEL), bf16),
    u=((TOKENS, CONV_CH), bf16),
    pre=((TOKENS + 16, CONV_CH), bf16),
    xbc=((TOKENS, CONV_CH), bf16),
    dtx=((TOKENS, 128), f32),
    gated=((TOKENS, INNER), bf16),
    dy=((TOKENS, INNER), bf16),
    dz=((TOKENS, INNER), bf16),
    ddt=((TOKENS, 128), bf16),
    z=((256, INNER), f32),
    dg=((256, INNER), f32),
    rowdot=((TOKENS, 128), f32),
    dys=((CHUNK, INNER), bf16),
    xw=((CHUNK, INNER), bf16),
    lowd=((CHUNK, INNER), bf16),
    dwz=((MODEL, INNER), bf16),
    dwu=((MODEL, 2048), bf16),
    dwo=((INNER, MODEL), bf16),
    zr=((1488, MODEL), bf16),
    mine=((4, 112, 256), f32),
    up=((2, 8 + LEN, 256), f32),
    state=((STATE, INNER), f32),
    states=((SEQ * LEN // CHUNK, STATE, INNER), bf16),
    rowv=((128, 128), f32),
    tail=((8, INNER), f32),
    segc=((SEQ, 8 + LEN, 128), f32),
    back=((CONV - 1, LEN, 128), f32),
    one128=((128, HEADS * 128), bf16),
    one64=((128, INNER), bf16),
    sum64=((INNER, 128), bf16),
    acc=((10, 8, CONV_CH), f32),
)


def gather_weights(shards, seg_ref, win_own, wout_own, sm_own, hd, s, send_sems, recv_sems, small_send, small_recv):
    win, wout, sm = s["win"], s["wout"], s["sm"]
    at = place()
    shard = at["shard"]
    rows = pl.ds(pl.multiple_of(shard * (MODEL // shards), 16), MODEL // shards)
    win[rows, DT:] = jnp.zeros((MODEL // shards, PADDED - DT), bf16)
    win[rows, :PROJ] = win_own[...]
    wout[pl.ds(pl.multiple_of(shard * (INNER // shards), 16), INNER // shards), :] = wout_own[...]
    s["parts"][shard] = sm_own[...]
    greet(at, shards)
    sems = (send_sems, recv_sems)
    conv_part = Gather(at, win, shards, MODEL // shards, INNER, (PADDED - INNER) // 2, sems, 0)
    gate_part = Gather(at, win, shards, MODEL // shards, 0, INNER // 2, sems, 1)
    out_part = Gather(at, wout, shards, INNER // shards, 0, MODEL // 2, sems, 2)

    def small(d):
        return remote(
            s["parts"].at[shard],
            s["parts"].at[shard],
            small_send.at[d],
            small_recv.at[d],
            at["rep"],
            (shard + d) % shards,
        )

    for d in range(1, shards):
        small(d).start()
    conv_part.begin()
    setup(seg_ref, s)
    conv_part.spread()
    gate_part.begin()
    out_part.begin()
    conv_part.relay()
    conv_part.share()
    for d in range(1, shards):
        small(d).wait_recv()
        small(d).wait_send()
    row = rows_of((8, CONV_CH))
    taps = spread_lanes(s["parts"], 448, 448)
    gain = spread_lanes(s["parts"], 384, 384)
    first = spread_lanes(s["parts"], 192, 192)
    sm[...] = jnp.where(row < 5, taps, jnp.where(row == 5, gain, first))
    sm[7:8, :] = hd[2:3, :]
    conv_part.finish()
    for part in (gate_part, out_part):
        part.spread()
        part.relay()
        part.share()
    for part in (gate_part, out_part):
        part.finish()
    return at


def copy_weights(seg_ref, win_all, wout_all, sm_all, hd, s, sems):
    copies = [
        pltpu.make_async_copy(src, s[name], sems.at[i])
        for i, (src, name) in enumerate(((win_all, "win"), (wout_all, "wout"), (sm_all, "sm")))
    ]
    for copy in copies:
        copy.start()
    setup(seg_ref, s)
    for copy in copies:
        copy.wait()
    s["sm"][7:8, :] = hd[2:3, :]


def transposed(src, dst):
    for i in range(TOKENS // 128):
        for j in range(MODEL // 128):
            dst[j * 128 : (j + 1) * 128, i * 128 : (i + 1) * 128] = src[
                i * 128 : (i + 1) * 128, j * 128 : (j + 1) * 128
            ].T


def out_weight_gradient(cot_ref, s):
    for j in range(QUADS):
        cols = slice(j * 256, (j + 1) * 256)
        s["dwo"][cols, :] = tn(s["gated"][:, cols], cot_ref[...]).astype(bf16)


def in_weight_gradient(ref, column, tile):
    def fill(turned):
        for i in range(3):
            rows = slice(i * 256, (i + 1) * 256)
            ref[rows, column : column + tile.shape[1]] = nn(turned[rows, :TOKENS], tile[...]).astype(bf16)

    return fill


def token_gradient(i, win, gtok_ref, s):
    rows = pl.ds(pl.multiple_of(i * 256, 256), 256)
    for j in range(3):
        cols = slice(j * 256, (j + 1) * 256)
        gtok_ref[rows, cols] = (
            nt(s["dz"][rows, :], win[cols, :INNER])
            + nt(s["u"][rows, :], win[cols, INNER:DT])
            + nt(s["ddt"][rows, :], win[cols, DT : DT + 128])
        )


def pack_small(mine, s):
    for j in range(CONV_CH // 256):
        sums = [jnp.sum(s["acc"][k, :, j * 256 : (j + 1) * 256], axis=0, keepdims=True) for k in range(10)]
        mine[0, j * 16 : (j + 1) * 16, :] = jnp.concatenate(sums + [jnp.zeros((6, 256), f32)], axis=0)


def layer_kernel(
    direct, shards, x_ref, cot_ref, seg_ref, win_own, wout_own, sm_own, hd, mixed_ref, gtok_ref, gin_ref, gout_ref, gsm_ref, *refs
):
    s = dict(zip(SCRATCH, refs))
    s["mixed_sem"], *sems = refs[len(SCRATCH) :]
    s["y"] = gtok_ref
    s["part"] = s["z"]
    win, wout, sm = s["win"], s["wout"], s["sm"]
    if direct:
        *sems, sends, recvs, locals_, total_send, total_recv, forward_done, scan_done = sems
        at = gather_weights(shards, seg_ref, win_own, wout_own, sm_own, hd, s, *sems)
        pair = (sends, recvs)
        zr, xbc, dy = s["zr"], s["xbc"], s["dy"]
        gate_sum = Reduce(
            at, s["dwz"], MODEL, INNER // 2, [(zr, 0, 0), (zr, 768, 0), (zr, 1152, 0), (zr, 1344, 0)], gin_ref, 0, pair, 0, locals_.at[0]
        )
        out_sum = Reduce(
            at, s["dwo"], INNER, MODEL // 2, [(wout, 0, 0), (wout, 0, 384), (wout, 768, 384), (wout, 1152, 384)], gout_ref, 0, pair, 1, locals_.at[1]
        )
        conv_sum = Reduce(
            at, s["dwu"], MODEL, 1024, [(xbc, 0, 0), (dy, 0, 0), (dy, 384, 0), (dy, 576, 0)], gin_ref, INNER, pair, 2, locals_.at[2]
        )
        small_sum = Total(at, s["mine"], s["up"], (total_send, total_recv))
    else:
        copy_weights(seg_ref, win_own, wout_own, sm_own, hd, s, *sems)
    chunks = LEN // CHUNK

    @pl.loop(0, SEQ)
    def _(q):
        project(q, x_ref, seg_ref, win, sm, hd, s)
        s["state"][...] = jnp.zeros((STATE, INNER), f32)

        @pl.loop(0, chunks)
        def _(c):
            scan_forward(q, c, seg_ref, sm, hd, s)

        @pl.loop(0, LEN // 256)
        def _(i):
            gate(q, i, x_ref, cot_ref, win, wout, sm, mixed_ref, s)

    if direct:
        meet(at, shards, forward_done)
    out_weight_gradient(cot_ref, s)
    if direct:
        met(shards, forward_done)
        out_sum.begin()
    turned = s["gated"]
    transposed(s["nrm"], turned)
    for j in range(QUADS):
        in_weight_gradient(s["dwz"], j * 256, s["dz"].at[:, j * 256 : (j + 1) * 256])(turned)
    if direct:
        gate_sum.begin()

    @pl.loop(0, SEQ * chunks)
    def _(n):
        @pl.when(n % chunks == 0)
        def _():
            s["state"][...] = jnp.zeros((STATE, INNER), f32)

        scan_backward(n // chunks, chunks - 1 - n % chunks, seg_ref, sm, hd, s)
        if direct:
            stages = ((0, "first"), (2, "second"), (4, "third"), (6, "fourth"), (7, "fifth"))
            for index, name in stages:

                @pl.when(n == index)
                def _():
                    getattr(out_sum, name)()
                    getattr(gate_sum, name)()

    if direct:
        meet(at, shards, scan_done)
        out_sum.sixth()
        gate_sum.sixth()

    @pl.loop(0, SEQ)
    def _(q):
        conv_backward(q, sm, s)

    for j in range(CONV_CH // 256):
        in_weight_gradient(s["dwu"], j * 256, s["u"].at[:, j * 256 : (j + 1) * 256])(turned)
    in_weight_gradient(s["dwu"], CONV_CH, s["ddt"])(turned)
    s["dwu"][:, CONV_CH + 128 :] = jnp.zeros((MODEL, 128), bf16)
    if direct:
        met(shards, scan_done)
        conv_sum.begin()
        token_gradient(0, win, gtok_ref, s)
        conv_sum.first()

        @pl.loop(1, TOKENS // 256)
        def _(i):
            token_gradient(i, win, gtok_ref, s)

        conv_sum.second()
    else:

        @pl.loop(0, TOKENS // 256)
        def _(i):
            token_gradient(i, win, gtok_ref, s)

    @pl.loop(0, TOKENS // 128)
    def _(i):
        input_gradient(i, x_ref, cot_ref, sm, gtok_ref, s)

    pack_small(s["mine"], s)
    if direct:
        small_sum.begin()
        conv_sum.third()
        small_sum.step(0)
        out_sum.seventh()
        gate_sum.seventh()
        small_sum.step(1)
        conv_sum.fourth()
        small_sum.step(2)
        conv_sum.fifth()
        conv_sum.sixth()
        small_sum.finish(gsm_ref)
        conv_sum.seventh()
    else:
        gsm_ref[...] = s["mine"][0]
        copies = [
            pltpu.make_async_copy(s["dwz"], gin_ref.at[:, :INNER], sems[0].at[0]),
            pltpu.make_async_copy(s["dwu"], gin_ref.at[:, INNER:], sems[0].at[1]),
            pltpu.make_async_copy(s["dwo"], gout_ref, sems[0].at[2]),
        ]
        for copy in copies:
            copy.start()
        for copy in copies:
            copy.wait()


def reaches(mesh):
    return mesh.shape["rep"] == 8 and mesh.shape["shard"] == 4


def layer(mesh, x, cot, seg, win, wout, sm, hd):
    direct, shards = reaches(mesh), mesh.shape["shard"]
    vmem = pl.BlockSpec(memory_space=pltpu.VMEM)
    hbm = pl.BlockSpec(memory_space=pl.ANY)
    dma = pltpu.SemaphoreType.DMA
    if direct:
        sems = [dma((3, 5, shards)), dma((3, 5, shards)), dma((shards,)), dma((shards,))]
        sems += [dma((3, 10)), dma((3, 10)), dma((3,)), dma((6,)), dma((6,))]
        sems += [pltpu.SemaphoreType.REGULAR] * 2
        options = dict(collective_id=0, has_side_effects=True)
        weights = vmem
    else:
        sems, options, weights = [dma((3,))], {}, hbm
    return pl.pallas_call(
        partial(layer_kernel, direct, shards),
        out_shape=(
            jax.ShapeDtypeStruct((TOKENS, MODEL), bf16),
            jax.ShapeDtypeStruct((TOKENS, MODEL), f32),
            jax.ShapeDtypeStruct((MODEL // shards if direct else MODEL, PADDED), bf16),
            jax.ShapeDtypeStruct((INNER // shards if direct else INNER, MODEL), bf16),
            jax.ShapeDtypeStruct((112, 256), f32),
        ),
        in_specs=[vmem] * 3 + [weights] * 3 + [vmem],
        out_specs=[hbm, vmem, hbm, hbm, vmem],
        scratch_shapes=[pltpu.VMEM(shape, kind) for shape, kind in SCRATCH.values()] + [dma] + sems,
        compiler_params=pltpu.CompilerParams(vmem_limit_bytes=67043328, **options),
        name="layer",
    )(x, cot, seg, win, wout, sm, hd)


def rows_to_lanes(v, width):
    return jnp.pad(v.astype(f32), (0, width - v.shape[0]))[None]


def on_device(mesh, tokens, segment_ids, norm_gain, in_weight, conv_weight, conv_bias, dt_bias, a_log, d_skip, gate_gain, out_weight, cotangent):
    small = (conv_bias, gate_gain, norm_gain)
    if reaches(mesh):
        win, wout = in_weight, out_weight
        sm = jnp.concatenate([conv_weight.T.astype(f32)] + [rows_to_lanes(v, 512 - 64) for v in small + (norm_gain,)])
        sm = jnp.pad(sm, ((0, 0), (0, 64)))
    else:
        win, wout, taps, *small = lax.all_gather(
            (in_weight, out_weight, conv_weight) + small, "shard", axis=0, tiled=True
        )
        win = jnp.pad(win, ((0, 0), (0, PADDED - PROJ)))
        sm = jnp.concatenate([taps.T.astype(f32)] + [rows_to_lanes(v, CONV_CH) for v in (*small, small[-1])])
    hd = jnp.concatenate(
        [rows_to_lanes(v, CONV_CH) for v in (dt_bias, a_log, jnp.repeat(d_skip, HEADDIM))] + [jnp.zeros((5, CONV_CH), f32)],
        axis=0,
    )
    mixed, gtok, gin, gout, gsm = layer(
        mesh,
        tokens.reshape(TOKENS, MODEL), cotangent.reshape(TOKENS, MODEL), segment_ids, win, wout, sm, hd
    )
    if not reaches(mesh):
        gin = lax.psum(lax.psum_scatter(gin, "shard", scatter_dimension=0, tiled=True), "rep")
        gout = lax.psum(lax.psum_scatter(gout, "shard", scatter_dimension=0, tiled=True), "rep")
        gsm = lax.psum(gsm, ("rep", "shard"))
    gsm = gsm.reshape(CONV_CH // 256, 16, 256).transpose(1, 0, 2).reshape(16, CONV_CH)
    me = lax.axis_index("shard")

    def owned(v, like):
        return lax.dynamic_slice_in_dim(v, me * like.shape[0], like.shape[0])

    return (
        mixed.reshape(SEQ, LEN, MODEL),
        gtok.reshape(SEQ, LEN, MODEL),
        owned(gsm[6, :MODEL], norm_gain),
        gin[:, :PROJ].astype(f32),
        owned(gsm[:CONV].T, conv_weight),
        owned(gsm[4], conv_bias),
        gsm[8, :HEADS],
        gsm[9, :HEADS],
        gsm[7, :INNER].reshape(HEADS, HEADDIM).sum(axis=1),
        owned(gsm[5, :INNER], gate_gain),
        gout.astype(f32),
    )


def solution(mesh):
    batch = P(("rep", "shard"), None, None)
    return jax.shard_map(
        partial(on_device, mesh),
        mesh=mesh,
        in_specs=(
            batch,
            P(("rep", "shard"), None),
            P("shard"),
            P("shard", None),
            P("shard", None),
            P("shard"),
            P(),
            P(),
            P(),
            P("shard"),
            P("shard", None),
            batch,
        ),
        out_specs=(
            batch,
            batch,
            P("shard"),
            P("shard", None),
            P("shard", None),
            P("shard"),
            P(),
            P(),
            P(),
            P("shard"),
            P("shard", None),
        ),
        check_vma=False,
    )
```

```python
from functools import partial

import jax
import jax.numpy as jnp
from jax import lax
from jax.experimental import pallas as pl
from jax.experimental.pallas import tpu as pltpu
from jax.sharding import PartitionSpec as P

HEADS = 24
HEADDIM = 64
STATE = 128
CONV = 4
INNER = 1536
CONV_CH = 1792
MODEL = 768
PROJ = 3352
PADDED = 3584
DT = INNER + CONV_CH
EPS = 1e-05
MESH = pl.DeviceIdType.MESH

LEN = 512
CHUNK = 128
SEQ = 2
TOKENS = SEQ * LEN
QUADS = INNER // 256

f32 = jnp.float32
bf16 = jnp.bfloat16


def nn(a, b):
    return lax.dot_general(a, b, (((1,), (0,)), ((), ())), preferred_element_type=f32)


def nt(a, b):
    return lax.dot_general(a, b, (((1,), (1,)), ((), ())), preferred_element_type=f32)


def tn(a, b):
    return lax.dot_general(a, b, (((0,), (0,)), ((), ())), preferred_element_type=f32)


def exact(a, b):
    return lax.dot_general(
        a, b, (((1,), (0,)), ((), ())), preferred_element_type=f32, precision=lax.Precision.HIGHEST
    )


def sigmoid(v):
    return 0.5 * jnp.tanh(0.5 * v) + 0.5


def partial_sum(a):
    return a.reshape(a.shape[0] // 8, 8, a.shape[1]).sum(axis=0)


def lanes_of(shape):
    return lax.broadcasted_iota(jnp.int32, shape, 1)


def rows_of(shape):
    return lax.broadcasted_iota(jnp.int32, shape, 0)


def packed(a):
    a = jnp.where(lanes_of(a.shape) < HEADS, a, 0.0)
    high = a.astype(bf16).astype(f32)
    rest = a - high
    middle = rest.astype(bf16).astype(f32)
    low = rest - middle
    return (high + pltpu.roll(middle, 32, 1) + pltpu.roll(low, 64, 1)).astype(bf16)


def two_parts(a):
    high = a.astype(bf16)
    return high, (a - high.astype(f32)).astype(bf16)


def scanned(s, rows, cols):
    return s["dy"][rows, cols].astype(f32) + s["dz"][rows, cols].astype(f32)


def place():
    rep, shard = lax.axis_index("rep"), lax.axis_index("shard")
    core = rep % 2
    px, py = (rep // 2) % 2, rep // 4
    a = px * (1 - core) + py * core
    b = py * (1 - core) + px * core
    return dict(
        rep=rep,
        shard=shard,
        core=core,
        a=a,
        b=b,
        one=rep + (1 - 2 * a) * (2 + 2 * core),
        far=rep + (1 - 2 * a) * (2 + 2 * core) + (1 - 2 * b) * (4 - 2 * core),
        two=rep + (1 - 2 * b) * (4 - 2 * core),
        mate=rep + 1 - 2 * core,
    )


def greet(at, shards):
    barrier = pltpu.get_barrier_semaphore()
    for who in ("one", "two", "far", "mate"):
        pl.semaphore_signal(barrier, inc=1, device_id=(at[who], at["shard"]), device_id_type=MESH)
    for d in range(1, shards):
        pl.semaphore_signal(
            barrier, inc=1, device_id=(at["rep"], (at["shard"] + d) % shards), device_id_type=MESH
        )
    pl.semaphore_wait(barrier, 3 + shards)


def remote(src, dst, send, recv, rep, shard):
    return pltpu.make_async_remote_copy(
        src_ref=src, dst_ref=dst, send_sem=send, recv_sem=recv, device_id=(rep, shard), device_id_type=MESH
    )


class Gather:
    def __init__(self, at, ref, shards, rows, start, half, sems, part):
        self.at, self.ref, self.shards, self.rows, self.start, self.half = at, ref, shards, rows, start, half
        self.send, self.recv = (lambda kind, d: sems[0].at[part, kind, d]), (lambda kind, d: sems[1].at[part, kind, d])

    def columns(self):
        return pl.ds(pl.multiple_of(self.start + self.at["core"] * self.half, 128), self.half)

    def piece(self, shard, a, b):
        tall = self.rows // 4
        return self.ref.at[pl.ds(pl.multiple_of(shard * self.rows + (2 * b + a) * tall, 16), tall), self.columns()]

    def strip(self, shard):
        return self.ref.at[pl.ds(pl.multiple_of(shard * self.rows, 16), self.rows), self.columns()]

    def source(self, d):
        return (self.at["shard"] + self.shards - d) % self.shards

    def copy(self, kind, d):
        at = self.at
        if kind == 0:
            own = self.piece(at["shard"], at["a"], at["b"])
            return remote(own, own, self.send(0, d), self.recv(0, d), at["rep"], (at["shard"] + d) % self.shards)
        if kind == 4:
            what, who = self.strip(self.source(d)), at["mate"]
        elif kind == 3:
            what, who = self.piece(self.source(d), at["a"], 1 - at["b"]), at["one"]
        else:
            what, who = self.piece(self.source(d), at["a"], at["b"]), at["one"] if kind == 1 else at["two"]
        return remote(what, what, self.send(kind, d), self.recv(kind, d), who, at["shard"])

    def each(self):
        return range(1, self.shards)

    def begin(self):
        for d in self.each():
            self.copy(0, d).start()

    def spread(self):
        for d in self.each():
            self.copy(0, d).wait_recv()
            self.copy(2, d).start()
            self.copy(1, d).start()

    def relay(self):
        for d in self.each():
            self.copy(2, d).wait_recv()
            self.copy(3, d).start()

    def share(self):
        for d in self.each():
            self.copy(1, d).wait_recv()
            self.copy(3, d).wait_recv()
            self.copy(4, d).start()

    def finish(self):
        for d in self.each():
            self.copy(4, d).wait_recv()
            for kind in range(5):
                self.copy(kind, d).wait_send()


def meet(at, shards, sem):
    for who in ("one", "two", "far", "mate"):
        pl.semaphore_signal(sem, inc=1, device_id=(at[who], at["shard"]), device_id_type=MESH)
    for d in range(1, shards):
        pl.semaphore_signal(sem, inc=1, device_id=(at["rep"], (at["shard"] + d) % shards), device_id_type=MESH)


def met(shards, sem):
    pl.semaphore_wait(sem, 3 + shards)


class Reduce:
    def __init__(self, at, grad, rows, half, slots, out, column, sems, part, local):
        self.at, self.grad, self.rows, self.half, self.slots = at, grad, rows, half, slots
        self.out, self.column = out, column
        self.tall, self.own_rows = rows // 16, rows // 4
        self.send, self.recv = (lambda i: sems[0].at[part, i]), (lambda i: sems[1].at[part, i])
        self.local = local
        self.keep = pl.ds(pl.multiple_of(at["core"] * half, 128), half)
        self.give = pl.ds(pl.multiple_of((1 - at["core"]) * half, 128), half)

    def slot(self, level, start, count):
        ref, row, column = self.slots[level]
        return ref.at[pl.ds(row + start, count), pl.ds(column, self.half)]

    def at_block(self, shard, a, b):
        return pl.multiple_of(shard * self.own_rows + (2 * b + a) * self.tall, 16)

    def block(self, shard, a, b):
        return self.grad.at[pl.ds(self.at_block(shard, a, b), self.tall), self.keep]

    def to(self, src, dst, index, who):
        rep, shard = who
        return remote(src, dst, self.send(index), self.recv(index), rep, shard)

    def partner(self, name):
        return self.at[name], self.at["shard"]

    def add(self, start, level, place_in_slot):
        rows = pl.ds(start, self.tall)
        got = self.slot(level, place_in_slot, self.tall)[...]
        self.grad[rows, self.keep] = (self.grad[rows, self.keep].astype(f32) + got.astype(f32)).astype(bf16)

    def halves(self):
        whole = self.slot(0, 0, self.rows)
        return self.to(self.grad.at[:, self.give], whole, 0, self.partner("mate"))

    def begin(self):
        self.halves().start()

    def first(self):
        at = self.at
        self.halves().wait_recv()

        @pl.loop(0, 16)
        def _(i):
            start = pl.multiple_of(i * self.tall, 16)
            self.add(start, 0, start)

        for shard in range(4):
            for b in range(2):
                self.to(
                    self.block(shard, 1 - at["a"], b),
                    self.slot(1, (2 * shard + b) * self.tall, self.tall),
                    1,
                    self.partner("one"),
                ).start()

    def all_of(self, level, index, name):
        whole = self.slot(level, 0, self.rows >> level)
        return self.to(whole, whole, index, self.partner(name))

    def second(self):
        at = self.at
        self.all_of(1, 1, "one").wait_recv()
        for shard in range(4):
            for b in range(2):
                self.add(self.at_block(shard, at["a"], b), 1, (2 * shard + b) * self.tall)
        for shard in range(4):
            self.to(
                self.block(shard, at["a"], 1 - at["b"]),
                self.slot(2, shard * self.tall, self.tall),
                2,
                self.partner("two"),
            ).start()

    def across(self, d):
        at = self.at
        shard = (at["shard"] + d) % 4
        return self.to(
            self.block(shard, at["a"], at["b"]), self.slot(3, (d - 1) * self.tall, self.tall), 2 + d, (at["rep"], shard)
        )

    def third(self):
        at = self.at
        self.all_of(2, 2, "two").wait_recv()
        for shard in range(4):
            self.add(self.at_block(shard, at["a"], at["b"]), 2, shard * self.tall)
        for d in range(1, 4):
            self.across(d).start()

    def landed(self, a, b):
        rows = pl.ds(pl.multiple_of((2 * b + a) * self.tall, 16), self.tall)
        return self.out.at[rows, pl.ds(pl.multiple_of(self.column + self.at["core"] * self.half, 128), self.half)]

    def spread(self, index):
        at = self.at
        own = self.block(at["shard"], at["a"], at["b"])
        return self.to(own, self.landed(at["a"], at["b"]), index, self.partner(("one", "two", "far")[index - 6]))

    def home(self):
        at = self.at
        own = self.block(at["shard"], at["a"], at["b"])
        return pltpu.make_async_copy(own, self.landed(at["a"], at["b"]), self.local)

    def fourth(self):
        at = self.at
        for d in range(1, 4):
            self.across(d).wait_recv()
        rows = pl.ds(self.at_block(at["shard"], at["a"], at["b"]), self.tall)
        total = self.grad[rows, self.keep].astype(f32)
        for d in range(1, 4):
            total = total + self.slot(3, (d - 1) * self.tall, self.tall)[...].astype(f32)
        self.grad[rows, self.keep] = total.astype(bf16)
        for index in (8, 7, 6):
            self.spread(index).start()
        self.home().start()

    def strip(self):
        columns = pl.ds(pl.multiple_of(self.column + self.at["core"] * self.half, 128), self.half)
        return self.to(self.out.at[:, columns], self.out.at[:, columns], 9, self.partner("mate"))

    def sixth(self):
        self.home().wait()
        for index in (6, 7, 8):
            self.spread(index).wait_recv()
        self.strip().start()

    def seventh(self):
        self.strip().wait_recv()
        self.halves().wait_send()
        self.all_of(1, 1, "one").wait_send()
        self.all_of(2, 2, "two").wait_send()
        for d in range(1, 4):
            self.across(d).wait_send()
        for index in (6, 7, 8):
            self.spread(index).wait_send()
        self.strip().wait_send()


def unpack_small(total, gain, out):
    for j in range(CONV_CH // 256):
        out[0:8, j * 256 : (j + 1) * 256] = total[j * 8 : (j + 1) * 8, :]
    for j in range(MODEL // 128):
        out[6:7, j * 128 : (j + 1) * 128] = gain[j : j + 1, :]
    for k in range(3):
        out[7 + k : 8 + k, 0:128] = total[8 * (k // 2) + 6 : 8 * (k // 2) + 7, (k % 2) * 128 : (k % 2 + 1) * 128]


class Total:
    def __init__(self, at, mine, slot, sems, part):
        self.at, self.mine, self.slot = at, mine, slot
        self.send, self.recv = (lambda i: sems[0].at[part, i]), (lambda i: sems[1].at[part, i])

    def copy(self, index):
        at = self.at
        if index < 3:
            who = at[("mate", "one", "two")[index]], at["shard"]
        else:
            who = at["rep"], (at["shard"] + index - 2) % 4
        return remote(self.mine.at[min(index, 3)], self.slot(index), self.send(index), self.recv(index), *who)

    def begin(self):
        self.copy(0).start()

    def step(self, index):
        self.copy(index).wait_recv()
        self.mine[index + 1] = self.mine[index] + self.slot(index)[...]
        for following in (index + 1,) if index < 2 else (3, 4, 5):
            self.copy(following).start()

    def finish(self):
        total = self.mine[3]
        for index in (3, 4, 5):
            self.copy(index).wait_recv()
            total = total + self.slot(index)[...]
        for index in range(6):
            self.copy(index).wait_send()
        return total


def spread_lanes(block, width, offset):
    total = jnp.zeros((8, CONV_CH), f32)
    for z in range(4):
        part = jnp.where(lanes_of((8, 512)) < width, block[z], 0.0)
        part = jnp.concatenate([part, jnp.zeros((8, CONV_CH - 512), f32)], axis=1)
        total = total + (part if z == 0 else pltpu.roll(part, z * offset, 1))
    return total


def setup(seg_ref, s):
    r, c = rows_of((128, 256)), lanes_of((128, 256))
    for j in range(HEADS * 128 // 256):
        s["one128"][:, j * 256 : (j + 1) * 256] = (
            ((r & 31) == ((c + j * 256) >> 7)) & (r < 96)
        ).astype(f32).astype(bf16)
    for j in range(QUADS):
        s["one64"][:, j * 256 : (j + 1) * 256] = (
            ((r & 31) == ((c + j * 256) >> 6)) & (r < 96)
        ).astype(f32).astype(bf16)
    r, c = rows_of((256, 128)), lanes_of((256, 128))
    for j in range(QUADS):
        s["sum64"][j * 256 : (j + 1) * 256, :] = (((r + j * 256) >> 6) == c).astype(f32).astype(bf16)
    s["acc"][...] = jnp.zeros(s["acc"].shape, f32)
    s["pre"][TOKENS:, :] = jnp.zeros((16, CONV_CH), bf16)
    s["up"][:, 0:8, :] = jnp.zeros((2, 8, 256), f32)
    for q in range(SEQ):
        s["segc"][q, 0:8, :] = jnp.full((8, 128), -1.0, f32)
        for i in range(LEN // 128):
            seg = seg_ref[q : q + 1, i * 128 : (i + 1) * 128].astype(f32)
            s["segc"][q, 8 + i * 128 : 8 + (i + 1) * 128, :] = jnp.broadcast_to(seg, (128, 128)).T


def norm_input(q, x_ref, sm, s):
    @pl.loop(0, LEN // 64)
    def _(i):
        rows = pl.ds(pl.multiple_of(q * LEN + i * 64, 64), 64)
        x = x_ref[rows, :].astype(f32)
        r = lax.rsqrt(jnp.mean(x * x, axis=1, keepdims=True) + EPS)
        s["nrm"][rows, :] = (x * r * sm[6:7, :MODEL]).astype(bf16)


def project(q, win, sm, hd, s):
    row0 = pl.multiple_of(q * LEN, LEN)
    seg = s["segc"][q, 8 : 8 + LEN, :]
    place = rows_of((LEN, 128))
    for o in range(1, CONV):
        s["back"][o - 1] = ((seg == pltpu.roll(seg, o, 0)) & (place >= o)).astype(f32)
    rows = pl.ds(row0, LEN)
    raw = nn(s["nrm"][rows, :], win[:, DT : DT + 128]) + hd[0:1, :]
    s["dtx"][rows, :] = raw
    for j in range(CONV_CH // 256):
        slot = j % 2
        s["up"][slot, 8:, :] = nn(s["nrm"][rows, :], win[:, INNER + j * 256 : INNER + (j + 1) * 256])
        for i in range(LEN // 128):
            for half in range(2):
                c0 = j * 256 + half * 128
                here = pl.ds(row0 + i * 128, 128)
                block = s["up"][slot, i * 128 : i * 128 + 136, half * 128 : (half + 1) * 128]
                u = block[8:]
                tap = lambda k: sm[k : k + 1, c0 : c0 + 128]
                pre = sm[4:5, c0 : c0 + 128] + tap(3) * u
                for o in range(1, CONV):
                    same = s["back"][o - 1, i * 128 : (i + 1) * 128, :]
                    pre = pre + tap(3 - o) * (pltpu.roll(block, o, 0)[8:] * same)
                s["u"][here, c0 : c0 + 128] = u.astype(bf16)
                s["pre"][here, c0 : c0 + 128] = pre.astype(bf16)
                s["xbc"][here, c0 : c0 + 128] = (pre * sigmoid(pre)).astype(bf16)


def chunk_terms(q, c, seg_ref, hd, s):
    row0 = pl.multiple_of(q * LEN + c * CHUNK, CHUNK)
    rows = pl.ds(row0, CHUNK)
    raw = s["dtx"][rows, :]
    dt = jnp.maximum(raw, 0.0) + jnp.log1p(jnp.exp(-jnp.abs(raw)))
    rate = -jnp.exp(hd[1:2, :]) * dt
    lower = (rows_of((CHUNK, CHUNK)) >= lanes_of((CHUNK, CHUNK))).astype(f32)
    cum = exact(lower, rate)
    source = cum - jnp.log(jnp.maximum(dt, 1e-37))
    start = 8 + c * CHUNK
    segc = s["segc"][q, pl.ds(pl.multiple_of(start, 8), CHUNK), :]
    segr = segc.T
    before = s["segc"][q, pl.ds(pl.multiple_of(start - 8, 8), 8), :][7:8]
    last = segc[CHUNK - 1 : CHUNK]
    carry = (segc == before).astype(f32)
    tail = (segc == last).astype(f32)
    end = cum[CHUNK - 1 : CHUNK, :]
    keep = jnp.exp(end) * (before == last).astype(f32)
    grow = jnp.exp(cum) * carry
    shrink = jnp.exp(end - source) * tail
    return rows, raw, dt, rate, cum, source, segc, segr, grow, shrink, keep


def scan_forward(q, c, seg_ref, sm, hd, s):
    rows, raw, dt, rate, cum, source, segc, segr, grow, shrink, keep = chunk_terms(q, c, seg_ref, hd, s)
    t, k = rows_of((CHUNK, CHUNK)), lanes_of((CHUNK, CHUNK))
    bound = jnp.where((segc == segr) & (t >= k), 3e38, -1e30)
    s["rowv"][...] = source.T
    target = packed(cum)
    grow_p, shrink_p = packed(grow), packed(shrink)
    keep_p = packed(jnp.broadcast_to(keep, (8, 128)))
    bv = s["xbc"][rows, INNER : INNER + STATE]
    cv = s["xbc"][rows, INNER + STATE :]
    gram = nt(cv, bv)
    bt = bv.T
    at = q * (LEN // CHUNK) + c
    left = lanes_of((CHUNK, 128)) < HEADDIM
    for j in range(QUADS):
        cols = slice(j * 256, (j + 1) * 256)
        grow_e = nn(grow_p, s["one64"][:, cols])
        shrink_e = nn(shrink_p, s["one64"][:, cols])
        keep_e = nn(keep_p, s["one64"][:, cols])[0:1, :]
        state = s["state"][:, cols]
        low_state = state.astype(bf16)
        s["states"][at, :, cols] = low_state
        y_state = nn(cv, low_state)
        xv = s["xbc"][rows, cols]
        xw = (xv.astype(f32) * shrink_e).astype(bf16)
        s["state"][:, cols] = state * keep_e + nn(bt, xw)
        parts = []
        for pair in range(2):
            spread = nn(target, s["one128"][:, j * 512 + pair * 256 : j * 512 + (pair + 1) * 256])
            weights = []
            for half in range(2):
                head = 4 * j + 2 * pair + half
                d = spread[:, half * 128 : (half + 1) * 128] - s["rowv"][head : head + 1, :]
                weights.append((gram * jnp.exp(jnp.minimum(d, bound))).astype(bf16))
            x2 = xv[:, pair * 128 : (pair + 1) * 128]
            zero = jnp.zeros_like(x2)
            stack = jnp.concatenate([jnp.where(left, x2, zero), jnp.where(left, zero, x2)], axis=0)
            parts.append(nn(jnp.concatenate(weights, axis=1), stack))
        s["dy"][rows, cols], s["dz"][rows, cols] = two_parts(jnp.concatenate(parts, axis=1) + y_state * grow_e)


def gate(i, x_ref, cot_ref, win, wout, sm, mixed_ref, s):
    tall, block = 256, 64
    row0 = i * tall
    rows = pl.ds(pl.multiple_of(row0, tall), tall)
    for j in range(QUADS):
        cols = slice(j * 256, (j + 1) * 256)
        s["z"][:, cols] = nn(s["nrm"][rows, :], win[:, cols])
        s["dg"][:, cols] = nt(cot_ref[rows, :], wout[cols, :])

    @pl.loop(0, tall // block)
    def _(b):
        own = pl.ds(pl.multiple_of(b * block, block), block)
        where = pl.ds(pl.multiple_of(row0 + b * block, block), block)
        square = jnp.zeros((block, 128), f32)
        along = jnp.zeros((block, 128), f32)
        for j in range(INNER // 128):
            cols = slice(j * 128, (j + 1) * 128)
            z = s["z"][own, cols]
            y = scanned(s, where, cols) + sm[7:8, cols] * s["xbc"][where, cols].astype(f32)
            v = y * (z * sigmoid(z))
            square = square + v * v
            along = along + s["dg"][own, cols] * sm[5:6, cols] * v
        r = lax.rsqrt(jnp.sum(square, axis=1, keepdims=True) * (1.0 / INNER) + EPS)
        k = r * r * r * (jnp.sum(along, axis=1, keepdims=True) * (1.0 / INNER))
        for j in range(INNER // 128):
            cols = slice(j * 128, (j + 1) * 128)
            z = s["z"][own, cols]
            dg = s["dg"][own, cols]
            ys = scanned(s, where, cols)
            xv = s["xbc"][where, cols].astype(f32)
            y = ys + sm[7:8, cols] * xv
            sg = sigmoid(z)
            zs = z * sg
            v = y * zs
            vr = v * r
            gain = sm[5:6, cols]
            s["gated"][where, cols] = (vr * gain).astype(bf16)
            s["acc"][5, :, cols] += partial_sum(dg * vr)
            dv = r * (dg * gain) - v * k
            dy = dv * zs
            low_dy = dy.astype(bf16)
            s["dy"][where, cols] = low_dy
            s["dz"][where, cols] = (dv * y * (sg + zs * (1.0 - sg))).astype(bf16)
            s["acc"][7, :, cols] += partial_sum(dy * xv)
            s["dg"][own, cols] = low_dy.astype(f32) * ys

    high, low = two_parts(s["dg"][...])
    s["rowdot"][rows, :] = nn(high, s["sum64"][...]) + nn(low, s["sum64"][...])
    branch = nn(s["gated"][rows, :], wout[...])
    s["mixed"][...] = (x_ref[rows, :].astype(f32) + branch).astype(bf16)
    out = pltpu.make_async_copy(s["mixed"], mixed_ref.at[rows, :], s["mixed_sem"])
    out.start()
    out.wait()


def set_aside(s, at, kind):
    row, column = (at // 4) * 128, ((at % 4) * 3 + kind) * 128
    return s["dg"].at[pl.ds(pl.multiple_of(row, 128), 128), pl.ds(pl.multiple_of(column, 128), 128)]


def sums_aside(s, at):
    return s["z"].at[128:256, pl.ds(pl.multiple_of(at * 128, 128), 128)]


def scan_backward(q, c, quads, first, seg_ref, sm, hd, s):
    rows, raw, dt, rate, cum, source, segc, segr, grow, shrink, keep = chunk_terms(q, c, seg_ref, hd, s)
    k, t = rows_of((CHUNK, CHUNK)), lanes_of((CHUNK, CHUNK))
    allowed = (segc == segr) & (t >= k)
    bound = jnp.where(allowed, 3e38, -1e30)
    s["rowv"][...] = cum.T
    origin = packed(source)
    grow_p, shrink_p = packed(grow), packed(shrink)
    keep_p = packed(jnp.broadcast_to(keep, (8, 128)))
    bv = s["xbc"][rows, INNER : INNER + STATE]
    cv = s["xbc"][rows, INNER + STATE :]
    gram = nt(bv, cv)
    ct = cv.T
    at = q * (LEN // CHUNK) + c
    left = lanes_of((CHUNK, 128)) < HEADDIM
    dgram = jnp.zeros((CHUNK, CHUNK), f32) if first else set_aside(s, at, 0)[...]
    for j in quads:
        cols = slice(j * 256, (j + 1) * 256)
        grow_e = nn(grow_p, s["one64"][:, cols])
        s["dys"][:, cols] = (s["dy"][rows, cols].astype(f32) * grow_e).astype(bf16)
        shrink_e = nn(shrink_p, s["one64"][:, cols])
        s["xw"][:, cols] = (s["xbc"][rows, cols].astype(f32) * shrink_e).astype(bf16)
        low_dstate = s["state"][:, cols].astype(bf16)
        s["lowd"][:, cols] = low_dstate
        part = nn(bv, low_dstate) * shrink_e
        s["part"][:CHUNK, cols] = part
        keep_e = nn(keep_p, s["one64"][:, cols])[0:1, :]
        kept = s["state"][:, cols] * keep_e
        s["tail"][:, cols] = partial_sum(s["xbc"][rows, cols].astype(f32) * part) + partial_sum(
            kept * s["states"][at, :, cols].astype(f32)
        )
        s["state"][:, cols] = kept + nn(ct, s["dys"][:, cols])
    for j in range(2 * quads[0], 2 * quads[-1] + 2):
        cols = slice(j * 128, (j + 1) * 128)
        xv = s["xbc"][rows, cols]
        dy = s["dy"][rows, cols]
        spread = nn(origin, s["one128"][:, j * 256 : (j + 1) * 256])
        zero = jnp.zeros_like(dy)
        stack = jnp.concatenate([jnp.where(left, dy, zero), jnp.where(left, zero, dy)], axis=0)
        dweights = nt(xv, stack)
        weights = []
        for half in range(2):
            head = 2 * j + half
            d = s["rowv"][head : head + 1, :] - spread[:, half * 128 : (half + 1) * 128]
            e = jnp.exp(jnp.minimum(d, bound))
            weights.append((gram * e).astype(bf16))
            dgram = dgram + dweights[:, half * 128 : (half + 1) * 128] * e
        dx = nn(jnp.concatenate(weights, axis=1), stack) + s["part"][:CHUNK, cols]
        s["part"][:CHUNK, cols] = xv.astype(f32) * dx
        dx = dx + sm[7:8, cols] * dy.astype(f32)
        pre = s["pre"][rows, cols].astype(f32)
        sg = sigmoid(pre)
        s["pre"][rows, cols] = (dx * (sg * (1.0 + pre * (1.0 - sg)))).astype(bf16)
    some = slice(quads[0] * 256, (quads[-1] + 1) * 256)
    high, low = two_parts(s["part"][:CHUNK, some])
    colsum = nn(high, s["sum64"][some, :]) + nn(low, s["sum64"][some, :])
    high, low = two_parts(s["tail"][:, some])
    dlast = nn(high, s["sum64"][some, :]) + nn(low, s["sum64"][some, :])
    dc = nt(s["dys"][:, some], s["states"][at, :, some])
    db = nt(s["xw"][:, some], s["lowd"][:, some])
    if first:
        for index, value in enumerate((dgram, db, dc)):
            set_aside(s, at, index)[...] = value
        sums_aside(s, at)[...] = colsum
        s["kept_last"][at] = dlast
        return
    db, dc, colsum = db + set_aside(s, at, 1)[...], dc + set_aside(s, at, 2)[...], colsum + sums_aside(s, at)[...]
    dlast = jnp.sum(dlast + s["kept_last"][at], axis=0, keepdims=True)
    low_dgram = dgram.astype(bf16)
    db = db + nn(low_dgram, cv)
    dc = dc + tn(low_dgram, bv)
    for index, d in ((0, db), (1, dc)):
        cols = slice(INNER + index * STATE, INNER + (index + 1) * STATE)
        pre = s["pre"][rows, cols].astype(f32)
        sg = sigmoid(pre)
        s["pre"][rows, cols] = (d * (sg * (1.0 + pre * (1.0 - sg)))).astype(bf16)
    dcum = s["rowdot"][rows, :] - colsum
    drate = exact(allowed.astype(f32), dcum) + dlast * (segc == segc[CHUNK - 1 : CHUNK]).astype(f32)
    sg = sigmoid(raw)
    ratio = jnp.where(dt > 1e-30, sg / jnp.maximum(dt, 1e-30), 1.0)
    draw = colsum * ratio - drate * jnp.exp(hd[1:2, :]) * sg
    draw = jnp.where(lanes_of((CHUNK, 128)) < HEADS, draw, 0.0)
    s["ddt"][rows, :] = draw.astype(bf16)
    s["acc"][8, :, 0:128] += partial_sum(draw)
    s["acc"][9, :, 0:128] += partial_sum(drate * rate)


def conv_backward(q, tiles, sm, s):
    row0 = pl.multiple_of(q * LEN, LEN)
    rows = pl.ds(row0, LEN)
    seg = s["segc"][q, 8 : 8 + LEN, :]
    place = rows_of((LEN, 128))
    for o in range(1, CONV):
        s["back"][o - 1] = ((seg == pltpu.roll(seg, LEN - o, 0)) & (place < LEN - o)).astype(f32)
    for j in tiles:
        cols = slice(j * 128, (j + 1) * 128)
        sums = [jnp.zeros((8, 128), f32)] * 5
        for i in range(LEN // 128):
            here = pl.ds(row0 + i * 128, 128)
            block = s["pre"][pl.ds(row0 + i * 128, 144), cols].astype(f32)
            ds = block[:128]
            u = s["u"][here, cols].astype(f32)
            du = sm[3:4, cols] * ds
            sums[4] = sums[4] + partial_sum(ds)
            sums[3] = sums[3] + partial_sum(ds * u)
            for o in range(1, CONV):
                moved = pltpu.roll(block, 144 - o, 0)[:128] * s["back"][o - 1, i * 128 : (i + 1) * 128, :]
                du = du + sm[3 - o : 4 - o, cols] * moved
                sums[3 - o] = sums[3 - o] + partial_sum(moved * u)
            s["u"][here, cols] = du.astype(bf16)
        for k in range(5):
            s["acc"][k, :, cols] += sums[k]


def input_gradient(i, x_ref, cot_ref, sm, gtok_ref, s):
    rows = pl.ds(pl.multiple_of(i * 64, 64), 64)
    x = x_ref[rows, :].astype(f32)
    dn = gtok_ref[rows, :]
    r = lax.rsqrt(jnp.mean(x * x, axis=1, keepdims=True) + EPS)
    s["acc"][6, :, 0:MODEL] += partial_sum(dn * (x * r))
    h = dn * sm[6:7, :MODEL]
    k = r * r * r * jnp.mean(h * x, axis=1, keepdims=True)
    gtok_ref[rows, :] = r * h - k * x + cot_ref[rows, :].astype(f32)


SCRATCH = dict(
    win=((MODEL, PADDED), bf16),
    wout=((INNER, MODEL), bf16),
    parts=((4, 8, 512), f32),
    sm=((16, CONV_CH), f32),
    hd=((8, 128), f32),
    mixed=((256, MODEL), bf16),
    nrm=((TOKENS, MODEL), bf16),
    u=((TOKENS, CONV_CH), bf16),
    pre=((TOKENS + 16, CONV_CH), bf16),
    xbc=((TOKENS, CONV_CH), bf16),
    dtx=((TOKENS, 128), f32),
    gated=((TOKENS, INNER), bf16),
    dy=((TOKENS, INNER), bf16),
    dz=((TOKENS, INNER), bf16),
    ddt=((TOKENS, 128), bf16),
    z=((256, INNER), f32),
    dg=((256, INNER), f32),
    rowdot=((TOKENS, 128), f32),
    dys=((CHUNK, INNER), bf16),
    xw=((CHUNK, INNER), bf16),
    lowd=((CHUNK, INNER), bf16),
    dwz=((MODEL, INNER), bf16),
    dwu=((MODEL, 2048), bf16),
    dwo=((INNER, MODEL), bf16),
    zr=((1488, MODEL), bf16),
    mine=((4, 56, 256), f32),
    gain=((4, 8, 128), f32),
    gain_slots=((6, 8, 128), f32),
    up=((2, 8 + LEN, 256), f32),
    state=((STATE, INNER), f32),
    states=((SEQ * LEN // CHUNK, STATE, INNER), bf16),
    rowv=((128, 128), f32),
    tail=((8, INNER), f32),
    kept_last=((SEQ * LEN // CHUNK, 8, 128), f32),
    segc=((SEQ, 8 + LEN, 128), f32),
    back=((CONV - 1, LEN, 128), f32),
    one128=((128, HEADS * 128), bf16),
    one64=((128, INNER), bf16),
    sum64=((INNER, 128), bf16),
    acc=((10, 8, CONV_CH), f32),
)


def gather_weights(shards, x_ref, seg_ref, win_own, wout_own, sm_own, hd, s, send_sems, recv_sems, small_send, small_recv):
    win, wout, sm = s["win"], s["wout"], s["sm"]
    at = place()
    shard = at["shard"]
    rows = pl.ds(pl.multiple_of(shard * (MODEL // shards), 16), MODEL // shards)
    win[rows, DT:] = jnp.zeros((MODEL // shards, PADDED - DT), bf16)
    win[rows, :PROJ] = win_own[...]
    own = wout.at[pl.ds(pl.multiple_of(shard * (INNER // shards), 16), INNER // shards), :]
    fetch = pltpu.make_async_copy(wout_own, own, s["mixed_sem"])
    fetch.start()
    s["parts"][shard] = sm_own[0:8, :]
    fetch.wait()
    hd[0:2, :] = sm_own[8:10, :128]
    greet(at, shards)
    sems = (send_sems, recv_sems)
    conv_part = Gather(at, win, shards, MODEL // shards, INNER, (PADDED - INNER) // 2, sems, 0)
    gate_part = Gather(at, win, shards, MODEL // shards, 0, INNER // 2, sems, 1)
    out_part = Gather(at, wout, shards, INNER // shards, 0, MODEL // 2, sems, 2)

    def small(d):
        return remote(
            s["parts"].at[shard],
            s["parts"].at[shard],
            small_send.at[d],
            small_recv.at[d],
            at["rep"],
            (shard + d) % shards,
        )

    for d in range(1, shards):
        small(d).start()
    conv_part.begin()
    setup(seg_ref, s)
    for d in range(1, shards):
        small(d).wait_recv()
        small(d).wait_send()
    row = rows_of((8, CONV_CH))
    taps = spread_lanes(s["parts"], 448, 448)
    gain = spread_lanes(s["parts"], 384, 384)
    first = spread_lanes(s["parts"], 192, 192)
    sm[0:8, :] = jnp.where(row < 5, taps, jnp.where(row == 5, gain, first))
    skip = packed(jnp.broadcast_to(sm_own[10:11, :128], (8, 128)))
    sm[7:8, :INNER] = nn(skip, s["one64"][...])[0:1, :]
    conv_part.spread()
    norm_input(0, x_ref, sm, s)
    conv_part.relay()
    norm_input(1, x_ref, sm, s)
    conv_part.share()
    gate_part.begin()
    out_part.begin()
    conv_part.finish()
    return at, gate_part, out_part


def copy_weights(seg_ref, win_all, wout_all, sm_all, hd, s, sems):
    copies = [
        pltpu.make_async_copy(src, s[name], sems.at[i])
        for i, (src, name) in enumerate(((win_all, "win"), (wout_all, "wout"), (sm_all, "sm")))
    ]
    for copy in copies:
        copy.start()
    setup(seg_ref, s)
    for copy in copies:
        copy.wait()
    hd[0:2, :] = s["sm"][8:10, :128]
    skip = packed(jnp.broadcast_to(s["sm"][10:11, :128], (8, 128)))
    s["sm"][7:8, :INNER] = nn(skip, s["one64"][...])[0:1, :]


def transposed(src, dst):
    for i in range(TOKENS // 128):
        for j in range(MODEL // 128):
            dst[j * 128 : (j + 1) * 128, i * 128 : (i + 1) * 128] = src[
                i * 128 : (i + 1) * 128, j * 128 : (j + 1) * 128
            ].T


def out_weight_gradient(cot_ref, s):
    for j in range(QUADS):
        cols = slice(j * 256, (j + 1) * 256)
        s["dwo"][cols, :] = tn(s["gated"][:, cols], cot_ref[...]).astype(bf16)


def in_weight_gradient(ref, column, tile):
    def fill(turned):
        for i in range(3):
            rows = slice(i * 256, (i + 1) * 256)
            ref[rows, column : column + tile.shape[1]] = nn(turned[rows, :TOKENS], tile[...]).astype(bf16)

    return fill


def token_gradient(i, win, gtok_ref, s):
    rows = pl.ds(pl.multiple_of(i * 256, 256), 256)
    for j in range(3):
        cols = slice(j * 256, (j + 1) * 256)
        gtok_ref[rows, cols] = (
            nt(s["dz"][rows, :], win[cols, :INNER])
            + nt(s["u"][rows, :], win[cols, INNER:DT])
            + nt(s["ddt"][rows, :], win[cols, DT : DT + 128])
        )


def pack_small(mine, s):
    high, low = two_parts(s["acc"][7, :, :INNER])
    skip = nn(high, s["sum64"][...]) + nn(low, s["sum64"][...])
    s["acc"][7, :, 0:128] = skip
    heads = [jnp.sum(s["acc"][k, :, 0:128], axis=0, keepdims=True) for k in (7, 8, 9)] + [jnp.zeros((1, 128), f32)]
    for j in range(CONV_CH // 256):
        sums = [jnp.sum(s["acc"][k, :, j * 256 : (j + 1) * 256], axis=0, keepdims=True) for k in range(6)]
        tail = jnp.concatenate(heads[2 * j : 2 * j + 2], axis=1) if j < 2 else jnp.zeros((1, 256), f32)
        mine[0, j * 8 : (j + 1) * 8, :] = jnp.concatenate(sums + [tail, jnp.zeros((1, 256), f32)], axis=0)


def pack_gain(mine, s):
    sums = [jnp.sum(s["acc"][6, :, j * 128 : (j + 1) * 128], axis=0, keepdims=True) for j in range(MODEL // 128)]
    mine[0] = jnp.concatenate(sums + [jnp.zeros((2, 128), f32)], axis=0)


def layer_kernel(
    direct, shards, x_ref, cot_ref, seg_ref, win_own, wout_own, sm_own, mixed_ref, gtok_ref, gin_ref, gout_ref, gsm_ref, *refs
):
    s = dict(zip(SCRATCH, refs))
    s["mixed_sem"], *sems = refs[len(SCRATCH) :]
    s["part"] = s["z"]
    win, wout, sm, hd = s["win"], s["wout"], s["sm"], s["hd"]
    if direct:
        *sems, sends, recvs, locals_, total_send, total_recv, forward_done, scan_done = sems
        at, gate_part, out_part = gather_weights(shards, x_ref, seg_ref, win_own, wout_own, sm_own, hd, s, *sems)
        pair = (sends, recvs)
        zr, xbc, dy = s["zr"], s["xbc"], s["dy"]
        gate_sum = Reduce(
            at, s["dwz"], MODEL, INNER // 2, [(zr, 0, 0), (zr, 768, 0), (zr, 1152, 0), (zr, 1344, 0)], gin_ref, 0, pair, 0, locals_.at[0]
        )
        out_sum = Reduce(
            at, s["dwo"], INNER, MODEL // 2, [(wout, 0, 0), (wout, 0, 384), (wout, 768, 384), (wout, 1152, 384)], gout_ref, 0, pair, 1, locals_.at[1]
        )
        early_sum, late_sum = (
            Reduce(
                at,
                s["dwu"].at[:, i * 1024 : (i + 1) * 1024],
                MODEL,
                512,
                [(xbc, 0, i * 512), (dy, 0, i * 512), (dy, 384, i * 512), (dy, 576, i * 512)],
                gin_ref,
                INNER + i * 1024,
                pair,
                2 + i,
                locals_.at[2 + i],
            )
            for i in range(2)
        )
        totals = (total_send, total_recv)
        small_sum = Total(
            at, s["mine"], lambda i: s["up"].at[i // 3, pl.ds(8 + (i % 3) * 56, 56), :], totals, 0
        )
        gain_sum = Total(at, s["gain"], lambda i: s["gain_slots"].at[i], totals, 1)
    else:
        copy_weights(seg_ref, win_own, wout_own, sm_own, hd, s, *sems)
        for q in range(SEQ):
            norm_input(q, x_ref, sm, s)
    chunks = LEN // CHUNK

    @pl.loop(0, SEQ)
    def _(q):
        project(q, win, sm, hd, s)
        s["state"][...] = jnp.zeros((STATE, INNER), f32)
        if direct:

            @pl.when(q == 0)
            def _():
                gate_part.spread()
                out_part.spread()

        @pl.loop(0, chunks)
        def _(c):
            scan_forward(q, c, seg_ref, sm, hd, s)
            if direct:
                polls = ((2, gate_part.relay), (3, out_part.relay))
                for index, poll in polls:

                    @pl.when((q == 0) & (c == index))
                    def _():
                        poll()

                @pl.when((q == 1) & (c == 0))
                def _():
                    gate_part.share()

                @pl.when((q == 1) & (c == 1))
                def _():
                    out_part.share()

    if direct:
        gate_part.finish()
        out_part.finish()

    @pl.loop(0, TOKENS // 256)
    def _(i):
        gate(i, x_ref, cot_ref, win, wout, sm, mixed_ref, s)

    if direct:
        meet(at, shards, forward_done)
    out_weight_gradient(cot_ref, s)
    if direct:
        met(shards, forward_done)
        out_sum.begin()
    turned = s["gated"]
    transposed(s["nrm"], turned)
    for j in range(QUADS):
        in_weight_gradient(s["dwz"], j * 256, s["dz"].at[:, j * 256 : (j + 1) * 256])(turned)
    if direct:
        gate_sum.begin()

    def backward(quads, first, polls):
        @pl.loop(0, SEQ * chunks)
        def _(n):
            @pl.when(n % chunks == 0)
            def _():
                s["state"][:, quads[0] * 256 : (quads[-1] + 1) * 256] = jnp.zeros((STATE, len(quads) * 256), f32)

            scan_backward(n // chunks, chunks - 1 - n % chunks, quads, first, seg_ref, sm, hd, s)
            for index, poll in polls:

                @pl.when(n == index)
                def _():
                    poll()

    polls = ()
    if direct:
        polls = (
            (0, out_sum.first),
            (1, gate_sum.first),
            (3, out_sum.second),
            (5, out_sum.third),
            (6, gate_sum.second),
            (7, out_sum.fourth),
        )
    backward(range(4), True, polls)
    if direct:
        meet(at, shards, scan_done)

    @pl.loop(0, SEQ)
    def _(q):
        conv_backward(q, range(8), sm, s)

    if direct:
        gate_sum.third()
    for j in range(4):
        in_weight_gradient(s["dwu"], j * 256, s["u"].at[:, j * 256 : (j + 1) * 256])(turned)
    if direct:
        met(shards, scan_done)
        early_sum.begin()
        polls = (
            (0, out_sum.sixth),
            (1, early_sum.first),
            (3, gate_sum.fourth),
            (6, early_sum.second),
            (7, gate_sum.sixth),
        )
    backward(range(4, QUADS), False, polls)

    @pl.loop(0, SEQ)
    def _(q):
        conv_backward(q, range(8, CONV_CH // 128), sm, s)

    for j in range(4, CONV_CH // 256):
        in_weight_gradient(s["dwu"], j * 256, s["u"].at[:, j * 256 : (j + 1) * 256])(turned)
    in_weight_gradient(s["dwu"], CONV_CH, s["ddt"])(turned)
    s["dwu"][:, CONV_CH + 128 :] = jnp.zeros((MODEL, 128), bf16)
    pack_small(s["mine"], s)
    if direct:
        late_sum.begin()
        small_sum.begin()
        early_sum.third()
        small_sum.step(0)

    @pl.loop(0, TOKENS // 256)
    def _(i):
        token_gradient(i, win, gtok_ref, s)
        if direct:

            @pl.when(i == 0)
            def _():
                late_sum.first()

            @pl.when(i == 1)
            def _():
                small_sum.step(1)

            @pl.when(i == 3)
            def _():
                small_sum.step(2)

    if direct:
        early_sum.fourth()

    @pl.loop(0, TOKENS // 64)
    def _(i):
        input_gradient(i, x_ref, cot_ref, sm, gtok_ref, s)

    pack_gain(s["gain"], s)
    if direct:
        gain_sum.begin()
        late_sum.second()
        gain_sum.step(0)
        early_sum.sixth()
        gain_sum.step(1)
        late_sum.third()
        gain_sum.step(2)
        out_sum.seventh()
        gate_sum.seventh()
        late_sum.fourth()
        early_sum.seventh()
        late_sum.sixth()
        unpack_small(small_sum.finish(), gain_sum.finish(), gsm_ref)
        late_sum.seventh()
    else:
        unpack_small(s["mine"][0], s["gain"][0], gsm_ref)
        copies = [
            pltpu.make_async_copy(s["dwz"], gin_ref.at[:, :INNER], sems[0].at[0]),
            pltpu.make_async_copy(s["dwu"], gin_ref.at[:, INNER:], sems[0].at[1]),
            pltpu.make_async_copy(s["dwo"], gout_ref, sems[0].at[2]),
        ]
        for copy in copies:
            copy.start()
        for copy in copies:
            copy.wait()


def reaches(mesh):
    return mesh.shape["rep"] == 8 and mesh.shape["shard"] == 4


def layer(mesh, x, cot, seg, win, wout, sm):
    direct, shards = reaches(mesh), mesh.shape["shard"]
    vmem = pl.BlockSpec(memory_space=pltpu.VMEM)
    hbm = pl.BlockSpec(memory_space=pl.ANY)
    dma = pltpu.SemaphoreType.DMA
    if direct:
        sems = [dma((3, 5, shards)), dma((3, 5, shards)), dma((shards,)), dma((shards,))]
        sems += [dma((4, 10)), dma((4, 10)), dma((4,)), dma((2, 6)), dma((2, 6))]
        sems += [pltpu.SemaphoreType.REGULAR] * 2
        options = dict(collective_id=0, has_side_effects=True)
        weights = vmem
    else:
        sems, options, weights = [dma((3,))], {}, hbm
    return pl.pallas_call(
        partial(layer_kernel, direct, shards),
        out_shape=(
            jax.ShapeDtypeStruct((TOKENS, MODEL), bf16),
            jax.ShapeDtypeStruct((TOKENS, MODEL), f32),
            jax.ShapeDtypeStruct((MODEL // shards if direct else MODEL, PADDED), bf16),
            jax.ShapeDtypeStruct((INNER // shards if direct else INNER, MODEL), bf16),
            jax.ShapeDtypeStruct((16, CONV_CH), f32),
        ),
        in_specs=[vmem] * 3 + [weights, hbm, weights],
        out_specs=[hbm, vmem, hbm, hbm, vmem],
        scratch_shapes=[pltpu.VMEM(shape, kind) for shape, kind in SCRATCH.values()] + [dma] + sems,
        compiler_params=pltpu.CompilerParams(vmem_limit_bytes=67043328, **options),
        name="layer",
    )(x, cot, seg, win, wout, sm)


def placed(v, row, width):
    return jnp.pad(v.astype(f32), ((row, 16 - row - v.shape[0]), (0, width - v.shape[1])))


def on_device(mesh, tokens, segment_ids, norm_gain, in_weight, conv_weight, conv_bias, dt_bias, a_log, d_skip, gate_gain, out_weight, cotangent):
    small, heads = (conv_bias, gate_gain, norm_gain), (dt_bias, a_log, d_skip)
    if reaches(mesh):
        win, wout, taps, width = in_weight, out_weight, conv_weight, 512
    else:
        win, wout, taps, *small = lax.all_gather(
            (in_weight, out_weight, conv_weight) + small, "shard", axis=0, tiled=True
        )
        win, width = jnp.pad(win, ((0, 0), (0, PADDED - PROJ))), CONV_CH
    sm = placed(taps.T, 0, width)
    for row, v in enumerate((*small, jnp.zeros((1,), f32), *heads)):
        sm = sm + placed(v[None], CONV + row, width)
    mixed, gtok, gin, gout, gsm = layer(
        mesh,
        tokens.reshape(TOKENS, MODEL), cotangent.reshape(TOKENS, MODEL), segment_ids, win, wout, sm
    )
    if not reaches(mesh):
        gin = lax.psum(lax.psum_scatter(gin, "shard", scatter_dimension=0, tiled=True), "rep")
        gout = lax.psum(lax.psum_scatter(gout, "shard", scatter_dimension=0, tiled=True), "rep")
        gsm = lax.psum(gsm, ("rep", "shard"))
    me = lax.axis_index("shard")

    def owned(v, like):
        return lax.dynamic_slice_in_dim(v, me * like.shape[0], like.shape[0])

    return (
        mixed.reshape(SEQ, LEN, MODEL),
        gtok.reshape(SEQ, LEN, MODEL),
        owned(gsm[6, :MODEL], norm_gain),
        gin[:, :PROJ].astype(f32),
        owned(gsm[:CONV].T, conv_weight),
        owned(gsm[4], conv_bias),
        gsm[8, :HEADS],
        gsm[9, :HEADS],
        gsm[7, :HEADS],
        owned(gsm[5, :INNER], gate_gain),
        gout.astype(f32),
    )


def solution(mesh):
    batch = P(("rep", "shard"), None, None)
    return jax.shard_map(
        partial(on_device, mesh),
        mesh=mesh,
        in_specs=(
            batch,
            P(("rep", "shard"), None),
            P("shard"),
            P("shard", None),
            P("shard", None),
            P("shard"),
            P(),
            P(),
            P(),
            P("shard"),
            P("shard", None),
            batch,
        ),
        out_specs=(
            batch,
            batch,
            P("shard"),
            P("shard", None),
            P("shard", None),
            P("shard"),
            P(),
            P(),
            P(),
            P("shard"),
            P("shard", None),
        ),
        check_vma=False,
    )
```

```python
from functools import partial
from types import SimpleNamespace

import jax
import jax.numpy as jnp
from jax import lax
from jax.experimental import pallas as pl
from jax.experimental.pallas import tpu as pltpu
from jax.sharding import PartitionSpec as P

HEADS = 24
HEADDIM = 64
STATE = 128
CONV = 4
INNER = 1536
CONV_CH = 1792
MODEL = 768
PROJ = 3352
PADDED = 3584
DT = INNER + CONV_CH
EPS = 1e-05
MESH = pl.DeviceIdType.MESH

LEN = 512
CHUNK = 128
SEQ = 2
TOKENS = SEQ * LEN
QUADS = INNER // 256

f32 = jnp.float32
bf16 = jnp.bfloat16


def nn(a, b):
    return lax.dot_general(a, b, (((1,), (0,)), ((), ())), preferred_element_type=f32)


def nt(a, b):
    return lax.dot_general(a, b, (((1,), (1,)), ((), ())), preferred_element_type=f32)


def tn(a, b):
    return lax.dot_general(a, b, (((0,), (0,)), ((), ())), preferred_element_type=f32)


def exact(a, b):
    return lax.dot_general(
        a, b, (((1,), (0,)), ((), ())), preferred_element_type=f32, precision=lax.Precision.HIGHEST
    )


def sigmoid(v):
    return 0.5 * jnp.tanh(0.5 * v) + 0.5


def partial_sum(a):
    return a.reshape(a.shape[0] // 8, 8, a.shape[1]).sum(axis=0)


def lanes_of(shape):
    return lax.broadcasted_iota(jnp.int32, shape, 1)


def rows_of(shape):
    return lax.broadcasted_iota(jnp.int32, shape, 0)


def packed(a):
    a = jnp.where(lanes_of(a.shape) < HEADS, a, 0.0)
    high = a.astype(bf16).astype(f32)
    rest = a - high
    middle = rest.astype(bf16).astype(f32)
    low = rest - middle
    return (high + pltpu.roll(middle, 32, 1) + pltpu.roll(low, 64, 1)).astype(bf16)


def two_parts(a):
    high = a.astype(bf16)
    return high, (a - high.astype(f32)).astype(bf16)


def scanned(s, rows, cols):
    return s.dy[rows, cols].astype(f32) + s.dz[rows, cols].astype(f32)


def place():
    rep, shard = lax.axis_index("rep"), lax.axis_index("shard")
    core = rep % 2
    px, py = (rep // 2) % 2, rep // 4
    a = px * (1 - core) + py * core
    b = py * (1 - core) + px * core
    return SimpleNamespace(
        rep=rep,
        shard=shard,
        core=core,
        a=a,
        b=b,
        one=rep + (1 - 2 * a) * (2 + 2 * core),
        far=rep + (1 - 2 * a) * (2 + 2 * core) + (1 - 2 * b) * (4 - 2 * core),
        two=rep + (1 - 2 * b) * (4 - 2 * core),
        mate=rep + 1 - 2 * core,
    )


def greet(at, shards):
    barrier = pltpu.get_barrier_semaphore()
    for who in (at.one, at.two, at.far, at.mate):
        pl.semaphore_signal(barrier, inc=1, device_id=(who, at.shard), device_id_type=MESH)
    for d in range(1, shards):
        pl.semaphore_signal(
            barrier, inc=1, device_id=(at.rep, (at.shard + d) % shards), device_id_type=MESH
        )
    pl.semaphore_wait(barrier, 3 + shards)


def remote(src, dst, send, recv, rep, shard):
    return pltpu.make_async_remote_copy(
        src_ref=src, dst_ref=dst, send_sem=send, recv_sem=recv, device_id=(rep, shard), device_id_type=MESH
    )


class Gather:
    def __init__(self, at, ref, shards, rows, start, half, sems, part):
        self.at, self.ref, self.shards, self.rows, self.start, self.half = at, ref, shards, rows, start, half
        self.send, self.recv = (lambda kind, d: sems[0].at[part, kind, d]), (lambda kind, d: sems[1].at[part, kind, d])

    def columns(self):
        return pl.ds(pl.multiple_of(self.start + self.at.core * self.half, 128), self.half)

    def piece(self, shard, a, b):
        tall = self.rows // 4
        return self.ref.at[pl.ds(pl.multiple_of(shard * self.rows + (2 * b + a) * tall, 16), tall), self.columns()]

    def strip(self, shard):
        return self.ref.at[pl.ds(pl.multiple_of(shard * self.rows, 16), self.rows), self.columns()]

    def source(self, d):
        return (self.at.shard + self.shards - d) % self.shards

    def copy(self, kind, d):
        at = self.at
        if kind == 0:
            own = self.piece(at.shard, at.a, at.b)
            return remote(own, own, self.send(0, d), self.recv(0, d), at.rep, (at.shard + d) % self.shards)
        if kind == 4:
            what, who = self.strip(self.source(d)), at.mate
        elif kind == 3:
            what, who = self.piece(self.source(d), at.a, 1 - at.b), at.one
        else:
            what, who = self.piece(self.source(d), at.a, at.b), at.one if kind == 1 else at.two
        return remote(what, what, self.send(kind, d), self.recv(kind, d), who, at.shard)

    def each(self):
        return range(1, self.shards)

    def begin(self):
        for d in self.each():
            self.copy(0, d).start()

    def spread(self):
        for d in self.each():
            self.copy(0, d).wait_recv()
            self.copy(2, d).start()
            self.copy(1, d).start()

    def relay(self):
        for d in self.each():
            self.copy(2, d).wait_recv()
            self.copy(3, d).start()

    def share(self):
        for d in self.each():
            self.copy(1, d).wait_recv()
            self.copy(3, d).wait_recv()
            self.copy(4, d).start()

    def finish(self):
        for d in self.each():
            self.copy(4, d).wait_recv()
            for kind in range(5):
                self.copy(kind, d).wait_send()


def meet(at, shards, sem):
    for who in (at.one, at.two, at.far, at.mate):
        pl.semaphore_signal(sem, inc=1, device_id=(who, at.shard), device_id_type=MESH)
    for d in range(1, shards):
        pl.semaphore_signal(sem, inc=1, device_id=(at.rep, (at.shard + d) % shards), device_id_type=MESH)


def met(shards, sem):
    pl.semaphore_wait(sem, 3 + shards)


class Reduce:
    def __init__(self, at, grad, rows, half, slots, out, column, sems, part, local):
        self.at, self.grad, self.rows, self.half, self.slots = at, grad, rows, half, slots
        self.out, self.column = out, column
        self.tall, self.own_rows = rows // 16, rows // 4
        self.send, self.recv = (lambda i: sems[0].at[part, i]), (lambda i: sems[1].at[part, i])
        self.local = local
        self.keep = pl.ds(pl.multiple_of(at.core * half, 128), half)
        self.give = pl.ds(pl.multiple_of((1 - at.core) * half, 128), half)

    def slot(self, level, start, count):
        ref, row, column = self.slots[level]
        return ref.at[pl.ds(row + start, count), pl.ds(column, self.half)]

    def at_block(self, shard, a, b):
        return pl.multiple_of(shard * self.own_rows + (2 * b + a) * self.tall, 16)

    def block(self, shard, a, b):
        return self.grad.at[pl.ds(self.at_block(shard, a, b), self.tall), self.keep]

    def to(self, src, dst, index, who):
        rep, shard = who
        return remote(src, dst, self.send(index), self.recv(index), rep, shard)

    def partner(self, name):
        return name, self.at.shard

    def add(self, start, level, place_in_slot):
        rows = pl.ds(start, self.tall)
        got = self.slot(level, place_in_slot, self.tall)[...]
        self.grad[rows, self.keep] = (self.grad[rows, self.keep].astype(f32) + got.astype(f32)).astype(bf16)

    def halves(self):
        whole = self.slot(0, 0, self.rows)
        return self.to(self.grad.at[:, self.give], whole, 0, self.partner(self.at.mate))

    def begin(self):
        self.halves().start()

    def first(self):
        at = self.at
        self.halves().wait_recv()

        @pl.loop(0, 16)
        def _(i):
            start = pl.multiple_of(i * self.tall, 16)
            self.add(start, 0, start)

        for shard in range(4):
            for b in range(2):
                self.to(
                    self.block(shard, 1 - at.a, b),
                    self.slot(1, (2 * shard + b) * self.tall, self.tall),
                    1,
                    self.partner(self.at.one),
                ).start()

    def all_of(self, level, index, name):
        whole = self.slot(level, 0, self.rows >> level)
        return self.to(whole, whole, index, self.partner(name))

    def second(self):
        at = self.at
        self.all_of(1, 1, self.at.one).wait_recv()
        for shard in range(4):
            for b in range(2):
                self.add(self.at_block(shard, at.a, b), 1, (2 * shard + b) * self.tall)
        for shard in range(4):
            self.to(
                self.block(shard, at.a, 1 - at.b),
                self.slot(2, shard * self.tall, self.tall),
                2,
                self.partner(self.at.two),
            ).start()

    def across(self, d):
        at = self.at
        shard = (at.shard + d) % 4
        return self.to(
            self.block(shard, at.a, at.b), self.slot(3, (d - 1) * self.tall, self.tall), 2 + d, (at.rep, shard)
        )

    def third(self):
        at = self.at
        self.all_of(2, 2, self.at.two).wait_recv()
        for shard in range(4):
            self.add(self.at_block(shard, at.a, at.b), 2, shard * self.tall)
        for d in range(1, 4):
            self.across(d).start()

    def landed(self, a, b):
        rows = pl.ds(pl.multiple_of((2 * b + a) * self.tall, 16), self.tall)
        return self.out.at[rows, pl.ds(pl.multiple_of(self.column + self.at.core * self.half, 128), self.half)]

    def spread(self, index):
        at = self.at
        own = self.block(at.shard, at.a, at.b)
        return self.to(own, self.landed(at.a, at.b), index, self.partner((at.one, at.two, at.far)[index - 6]))

    def home(self):
        at = self.at
        own = self.block(at.shard, at.a, at.b)
        return pltpu.make_async_copy(own, self.landed(at.a, at.b), self.local)

    def fourth(self):
        at = self.at
        for d in range(1, 4):
            self.across(d).wait_recv()
        rows = pl.ds(self.at_block(at.shard, at.a, at.b), self.tall)
        total = self.grad[rows, self.keep].astype(f32)
        for d in range(1, 4):
            total = total + self.slot(3, (d - 1) * self.tall, self.tall)[...].astype(f32)
        self.grad[rows, self.keep] = total.astype(bf16)
        for index in (8, 7, 6):
            self.spread(index).start()
        self.home().start()

    def strip(self):
        columns = pl.ds(pl.multiple_of(self.column + self.at.core * self.half, 128), self.half)
        return self.to(self.out.at[:, columns], self.out.at[:, columns], 9, self.partner(self.at.mate))

    def sixth(self):
        self.home().wait()
        for index in (6, 7, 8):
            self.spread(index).wait_recv()
        self.strip().start()

    def seventh(self):
        self.strip().wait_recv()
        self.halves().wait_send()
        self.all_of(1, 1, self.at.one).wait_send()
        self.all_of(2, 2, self.at.two).wait_send()
        for d in range(1, 4):
            self.across(d).wait_send()
        for index in (6, 7, 8):
            self.spread(index).wait_send()
        self.strip().wait_send()


def unpack_small(total, gain, out):
    for j in range(CONV_CH // 256):
        out[0:8, j * 256 : (j + 1) * 256] = total[j * 8 : (j + 1) * 8, :]
    for j in range(MODEL // 128):
        out[6:7, j * 128 : (j + 1) * 128] = gain[j : j + 1, :]
    for k in range(3):
        out[7 + k : 8 + k, 0:128] = total[8 * (k // 2) + 6 : 8 * (k // 2) + 7, (k % 2) * 128 : (k % 2 + 1) * 128]


class Total:
    def __init__(self, at, mine, slot, sems, part):
        self.at, self.mine, self.slot = at, mine, slot
        self.send, self.recv = (lambda i: sems[0].at[part, i]), (lambda i: sems[1].at[part, i])

    def copy(self, index):
        at = self.at
        if index < 3:
            who = (at.mate, at.one, at.two)[index], at.shard
        else:
            who = at.rep, (at.shard + index - 2) % 4
        return remote(self.mine.at[min(index, 3)], self.slot(index), self.send(index), self.recv(index), *who)

    def begin(self):
        self.copy(0).start()

    def step(self, index):
        self.copy(index).wait_recv()
        self.mine[index + 1] = self.mine[index] + self.slot(index)[...]
        for following in (index + 1,) if index < 2 else (3, 4, 5):
            self.copy(following).start()

    def finish(self):
        total = self.mine[3]
        for index in (3, 4, 5):
            self.copy(index).wait_recv()
            total = total + self.slot(index)[...]
        for index in range(6):
            self.copy(index).wait_send()
        return total


def spread_lanes(block, width, offset):
    total = jnp.zeros((8, CONV_CH), f32)
    for z in range(4):
        part = jnp.where(lanes_of((8, 512)) < width, block[z], 0.0)
        part = jnp.concatenate([part, jnp.zeros((8, CONV_CH - 512), f32)], axis=1)
        total = total + (part if z == 0 else pltpu.roll(part, z * offset, 1))
    return total


def setup(seg_ref, s):
    r, c = rows_of((128, 256)), lanes_of((128, 256))
    for j in range(HEADS * 128 // 256):
        s.one128[:, j * 256 : (j + 1) * 256] = (
            ((r & 31) == ((c + j * 256) >> 7)) & (r < 96)
        ).astype(f32).astype(bf16)
    for j in range(QUADS):
        s.one64[:, j * 256 : (j + 1) * 256] = (
            ((r & 31) == ((c + j * 256) >> 6)) & (r < 96)
        ).astype(f32).astype(bf16)
    r, c = rows_of((256, 128)), lanes_of((256, 128))
    for j in range(QUADS):
        s.sum64[j * 256 : (j + 1) * 256, :] = (((r + j * 256) >> 6) == c).astype(f32).astype(bf16)
    s.acc[...] = jnp.zeros(s.acc.shape, f32)
    s.pre[TOKENS:, :] = jnp.zeros((16, CONV_CH), bf16)
    s.up[:, 0:8, :] = jnp.zeros((2, 8, 256), f32)
    for q in range(SEQ):
        s.segc[q, 0:8, :] = jnp.full((8, 128), -1.0, f32)
        for i in range(LEN // 128):
            seg = seg_ref[q : q + 1, i * 128 : (i + 1) * 128].astype(f32)
            s.segc[q, 8 + i * 128 : 8 + (i + 1) * 128, :] = jnp.broadcast_to(seg, (128, 128)).T


def norm_input(q, x_ref, sm, s):
    @pl.loop(0, LEN // 64)
    def _(i):
        rows = pl.ds(pl.multiple_of(q * LEN + i * 64, 64), 64)
        x = x_ref[rows, :].astype(f32)
        r = lax.rsqrt(jnp.mean(x * x, axis=1, keepdims=True) + EPS)
        s.nrm[rows, :] = (x * r * sm[6:7, :MODEL]).astype(bf16)


def project(q, win, sm, hd, s):
    row0 = pl.multiple_of(q * LEN, LEN)
    seg = s.segc[q, 8 : 8 + LEN, :]
    place = rows_of((LEN, 128))
    for o in range(1, CONV):
        s.back[o - 1] = ((seg == pltpu.roll(seg, o, 0)) & (place >= o)).astype(f32)
    rows = pl.ds(row0, LEN)
    raw = nn(s.nrm[rows, :], win[:, DT : DT + 128]) + hd[0:1, :]
    s.dtx[rows, :] = raw
    for j in range(CONV_CH // 256):
        slot = j % 2
        s.up[slot, 8:, :] = nn(s.nrm[rows, :], win[:, INNER + j * 256 : INNER + (j + 1) * 256])
        for i in range(LEN // 128):
            for half in range(2):
                c0 = j * 256 + half * 128
                here = pl.ds(row0 + i * 128, 128)
                block = s.up[slot, i * 128 : i * 128 + 136, half * 128 : (half + 1) * 128]
                u = block[8:]
                tap = lambda k: sm[k : k + 1, c0 : c0 + 128]
                pre = sm[4:5, c0 : c0 + 128] + tap(3) * u
                for o in range(1, CONV):
                    same = s.back[o - 1, i * 128 : (i + 1) * 128, :]
                    pre = pre + tap(3 - o) * (pltpu.roll(block, o, 0)[8:] * same)
                s.u[here, c0 : c0 + 128] = u.astype(bf16)
                s.pre[here, c0 : c0 + 128] = pre.astype(bf16)
                s.xbc[here, c0 : c0 + 128] = (pre * sigmoid(pre)).astype(bf16)


def chunk_terms(q, c, seg_ref, hd, s):
    row0 = pl.multiple_of(q * LEN + c * CHUNK, CHUNK)
    rows = pl.ds(row0, CHUNK)
    raw = s.dtx[rows, :]
    dt = jnp.maximum(raw, 0.0) + jnp.log1p(jnp.exp(-jnp.abs(raw)))
    rate = -jnp.exp(hd[1:2, :]) * dt
    lower = (rows_of((CHUNK, CHUNK)) >= lanes_of((CHUNK, CHUNK))).astype(f32)
    cum = exact(lower, rate)
    source = cum - jnp.log(jnp.maximum(dt, 1e-37))
    start = 8 + c * CHUNK
    segc = s.segc[q, pl.ds(pl.multiple_of(start, 8), CHUNK), :]
    segr = segc.T
    before = s.segc[q, pl.ds(pl.multiple_of(start - 8, 8), 8), :][7:8]
    last = segc[CHUNK - 1 : CHUNK]
    carry = (segc == before).astype(f32)
    tail = (segc == last).astype(f32)
    end = cum[CHUNK - 1 : CHUNK, :]
    keep = jnp.exp(end) * (before == last).astype(f32)
    grow = jnp.exp(cum) * carry
    shrink = jnp.exp(end - source) * tail
    return rows, raw, dt, rate, cum, source, segc, segr, grow, shrink, keep


def scan_forward(q, c, seg_ref, sm, hd, s):
    rows, raw, dt, rate, cum, source, segc, segr, grow, shrink, keep = chunk_terms(q, c, seg_ref, hd, s)
    t, k = rows_of((CHUNK, CHUNK)), lanes_of((CHUNK, CHUNK))
    bound = jnp.where((segc == segr) & (t >= k), 3e38, -1e30)
    s.rowv[...] = source.T
    target = packed(cum)
    grow_p, shrink_p = packed(grow), packed(shrink)
    keep_p = packed(jnp.broadcast_to(keep, (8, 128)))
    bv = s.xbc[rows, INNER : INNER + STATE]
    cv = s.xbc[rows, INNER + STATE :]
    gram = nt(cv, bv)
    bt = bv.T
    at = q * (LEN // CHUNK) + c
    left = lanes_of((CHUNK, 128)) < HEADDIM
    for j in range(QUADS):
        cols = slice(j * 256, (j + 1) * 256)
        grow_e = nn(grow_p, s.one64[:, cols])
        shrink_e = nn(shrink_p, s.one64[:, cols])
        keep_e = nn(keep_p, s.one64[:, cols])[0:1, :]
        state = s.state[:, cols]
        low_state = state.astype(bf16)
        s.states[at, :, cols] = low_state
        y_state = nn(cv, low_state)
        xv = s.xbc[rows, cols]
        xw = (xv.astype(f32) * shrink_e).astype(bf16)
        s.state[:, cols] = state * keep_e + nn(bt, xw)
        parts = []
        for pair in range(2):
            spread = nn(target, s.one128[:, j * 512 + pair * 256 : j * 512 + (pair + 1) * 256])
            weights = []
            for half in range(2):
                head = 4 * j + 2 * pair + half
                d = spread[:, half * 128 : (half + 1) * 128] - s.rowv[head : head + 1, :]
                weights.append((gram * jnp.exp(jnp.minimum(d, bound))).astype(bf16))
            x2 = xv[:, pair * 128 : (pair + 1) * 128]
            zero = jnp.zeros_like(x2)
            stack = jnp.concatenate([jnp.where(left, x2, zero), jnp.where(left, zero, x2)], axis=0)
            parts.append(nn(jnp.concatenate(weights, axis=1), stack))
        s.dy[rows, cols], s.dz[rows, cols] = two_parts(jnp.concatenate(parts, axis=1) + y_state * grow_e)


def gate(i, x_ref, cot_ref, win, wout, sm, mixed_ref, s):
    tall, block = 256, 64
    row0 = i * tall
    rows = pl.ds(pl.multiple_of(row0, tall), tall)
    for j in range(QUADS):
        cols = slice(j * 256, (j + 1) * 256)
        s.z[:, cols] = nn(s.nrm[rows, :], win[:, cols])
        s.dg[:, cols] = nt(cot_ref[rows, :], wout[cols, :])

    @pl.loop(0, tall // block)
    def _(b):
        own = pl.ds(pl.multiple_of(b * block, block), block)
        where = pl.ds(pl.multiple_of(row0 + b * block, block), block)
        square = jnp.zeros((block, 128), f32)
        along = jnp.zeros((block, 128), f32)
        for j in range(INNER // 128):
            cols = slice(j * 128, (j + 1) * 128)
            z = s.z[own, cols]
            y = scanned(s, where, cols) + sm[7:8, cols] * s.xbc[where, cols].astype(f32)
            v = y * (z * sigmoid(z))
            square = square + v * v
            along = along + s.dg[own, cols] * sm[5:6, cols] * v
        r = lax.rsqrt(jnp.sum(square, axis=1, keepdims=True) * (1.0 / INNER) + EPS)
        k = r * r * r * (jnp.sum(along, axis=1, keepdims=True) * (1.0 / INNER))
        for j in range(INNER // 128):
            cols = slice(j * 128, (j + 1) * 128)
            z = s.z[own, cols]
            dg = s.dg[own, cols]
            ys = scanned(s, where, cols)
            xv = s.xbc[where, cols].astype(f32)
            y = ys + sm[7:8, cols] * xv
            sg = sigmoid(z)
            zs = z * sg
            v = y * zs
            vr = v * r
            gain = sm[5:6, cols]
            s.gated[where, cols] = (vr * gain).astype(bf16)
            s.acc[5, :, cols] += partial_sum(dg * vr)
            dv = r * (dg * gain) - v * k
            dy = dv * zs
            low_dy = dy.astype(bf16)
            s.dy[where, cols] = low_dy
            s.dz[where, cols] = (dv * y * (sg + zs * (1.0 - sg))).astype(bf16)
            s.acc[7, :, cols] += partial_sum(dy * xv)
            s.dg[own, cols] = low_dy.astype(f32) * ys

    high, low = two_parts(s.dg[...])
    s.rowdot[rows, :] = nn(high, s.sum64[...]) + nn(low, s.sum64[...])
    branch = nn(s.gated[rows, :], wout[...])
    s.mixed[...] = (x_ref[rows, :].astype(f32) + branch).astype(bf16)
    out = pltpu.make_async_copy(s.mixed, mixed_ref.at[rows, :], s.mixed_sem)
    out.start()
    out.wait()


def set_aside(s, at, kind):
    row, column = (at // 4) * 128, ((at % 4) * 3 + kind) * 128
    return s.dg.at[pl.ds(pl.multiple_of(row, 128), 128), pl.ds(pl.multiple_of(column, 128), 128)]


def sums_aside(s, at):
    return s.z.at[128:256, pl.ds(pl.multiple_of(at * 128, 128), 128)]


def scan_backward(q, c, quads, first, seg_ref, sm, hd, s):
    rows, raw, dt, rate, cum, source, segc, segr, grow, shrink, keep = chunk_terms(q, c, seg_ref, hd, s)
    k, t = rows_of((CHUNK, CHUNK)), lanes_of((CHUNK, CHUNK))
    allowed = (segc == segr) & (t >= k)
    bound = jnp.where(allowed, 3e38, -1e30)
    s.rowv[...] = cum.T
    origin = packed(source)
    grow_p, shrink_p = packed(grow), packed(shrink)
    keep_p = packed(jnp.broadcast_to(keep, (8, 128)))
    bv = s.xbc[rows, INNER : INNER + STATE]
    cv = s.xbc[rows, INNER + STATE :]
    gram = nt(bv, cv)
    ct = cv.T
    at = q * (LEN // CHUNK) + c
    left = lanes_of((CHUNK, 128)) < HEADDIM
    dgram = jnp.zeros((CHUNK, CHUNK), f32) if first else set_aside(s, at, 0)[...]
    for j in quads:
        cols = slice(j * 256, (j + 1) * 256)
        grow_e = nn(grow_p, s.one64[:, cols])
        s.dys[:, cols] = (s.dy[rows, cols].astype(f32) * grow_e).astype(bf16)
        shrink_e = nn(shrink_p, s.one64[:, cols])
        s.xw[:, cols] = (s.xbc[rows, cols].astype(f32) * shrink_e).astype(bf16)
        low_dstate = s.state[:, cols].astype(bf16)
        s.lowd[:, cols] = low_dstate
        part = nn(bv, low_dstate) * shrink_e
        s.part[:CHUNK, cols] = part
        keep_e = nn(keep_p, s.one64[:, cols])[0:1, :]
        kept = s.state[:, cols] * keep_e
        s.tail[:, cols] = partial_sum(s.xbc[rows, cols].astype(f32) * part) + partial_sum(
            kept * s.states[at, :, cols].astype(f32)
        )
        s.state[:, cols] = kept + nn(ct, s.dys[:, cols])
    for j in range(2 * quads[0], 2 * quads[-1] + 2):
        cols = slice(j * 128, (j + 1) * 128)
        xv = s.xbc[rows, cols]
        dy = s.dy[rows, cols]
        spread = nn(origin, s.one128[:, j * 256 : (j + 1) * 256])
        zero = jnp.zeros_like(dy)
        stack = jnp.concatenate([jnp.where(left, dy, zero), jnp.where(left, zero, dy)], axis=0)
        dweights = nt(xv, stack)
        weights = []
        for half in range(2):
            head = 2 * j + half
            d = s.rowv[head : head + 1, :] - spread[:, half * 128 : (half + 1) * 128]
            e = jnp.exp(jnp.minimum(d, bound))
            weights.append((gram * e).astype(bf16))
            dgram = dgram + dweights[:, half * 128 : (half + 1) * 128] * e
        dx = nn(jnp.concatenate(weights, axis=1), stack) + s.part[:CHUNK, cols]
        s.part[:CHUNK, cols] = xv.astype(f32) * dx
        dx = dx + sm[7:8, cols] * dy.astype(f32)
        pre = s.pre[rows, cols].astype(f32)
        sg = sigmoid(pre)
        s.pre[rows, cols] = (dx * (sg * (1.0 + pre * (1.0 - sg)))).astype(bf16)
    some = slice(quads[0] * 256, (quads[-1] + 1) * 256)
    high, low = two_parts(s.part[:CHUNK, some])
    colsum = nn(high, s.sum64[some, :]) + nn(low, s.sum64[some, :])
    high, low = two_parts(s.tail[:, some])
    dlast = nn(high, s.sum64[some, :]) + nn(low, s.sum64[some, :])
    dc = nt(s.dys[:, some], s.states[at, :, some])
    db = nt(s.xw[:, some], s.lowd[:, some])
    if first:
        for index, value in enumerate((dgram, db, dc)):
            set_aside(s, at, index)[...] = value
        sums_aside(s, at)[...] = colsum
        s.kept_last[at] = dlast
        return
    db, dc, colsum = db + set_aside(s, at, 1)[...], dc + set_aside(s, at, 2)[...], colsum + sums_aside(s, at)[...]
    dlast = jnp.sum(dlast + s.kept_last[at], axis=0, keepdims=True)
    low_dgram = dgram.astype(bf16)
    db = db + nn(low_dgram, cv)
    dc = dc + tn(low_dgram, bv)
    for index, d in ((0, db), (1, dc)):
        cols = slice(INNER + index * STATE, INNER + (index + 1) * STATE)
        pre = s.pre[rows, cols].astype(f32)
        sg = sigmoid(pre)
        s.pre[rows, cols] = (d * (sg * (1.0 + pre * (1.0 - sg)))).astype(bf16)
    dcum = s.rowdot[rows, :] - colsum
    drate = exact(allowed.astype(f32), dcum) + dlast * (segc == segc[CHUNK - 1 : CHUNK]).astype(f32)
    sg = sigmoid(raw)
    ratio = jnp.where(dt > 1e-30, sg / jnp.maximum(dt, 1e-30), 1.0)
    draw = colsum * ratio - drate * jnp.exp(hd[1:2, :]) * sg
    draw = jnp.where(lanes_of((CHUNK, 128)) < HEADS, draw, 0.0)
    s.ddt[rows, :] = draw.astype(bf16)
    s.acc[8, :, 0:128] += partial_sum(draw)
    s.acc[9, :, 0:128] += partial_sum(drate * rate)


def conv_backward(q, tiles, sm, s):
    row0 = pl.multiple_of(q * LEN, LEN)
    rows = pl.ds(row0, LEN)
    seg = s.segc[q, 8 : 8 + LEN, :]
    place = rows_of((LEN, 128))
    for o in range(1, CONV):
        s.back[o - 1] = ((seg == pltpu.roll(seg, LEN - o, 0)) & (place < LEN - o)).astype(f32)
    for j in tiles:
        cols = slice(j * 128, (j + 1) * 128)
        sums = [jnp.zeros((8, 128), f32)] * 5
        for i in range(LEN // 128):
            here = pl.ds(row0 + i * 128, 128)
            block = s.pre[pl.ds(row0 + i * 128, 144), cols].astype(f32)
            ds = block[:128]
            u = s.u[here, cols].astype(f32)
            du = sm[3:4, cols] * ds
            sums[4] = sums[4] + partial_sum(ds)
            sums[3] = sums[3] + partial_sum(ds * u)
            for o in range(1, CONV):
                moved = pltpu.roll(block, 144 - o, 0)[:128] * s.back[o - 1, i * 128 : (i + 1) * 128, :]
                du = du + sm[3 - o : 4 - o, cols] * moved
                sums[3 - o] = sums[3 - o] + partial_sum(moved * u)
            s.u[here, cols] = du.astype(bf16)
        for k in range(5):
            s.acc[k, :, cols] += sums[k]


def input_gradient(i, x_ref, cot_ref, sm, gtok_ref, s):
    rows = pl.ds(pl.multiple_of(i * 64, 64), 64)
    x = x_ref[rows, :].astype(f32)
    dn = gtok_ref[rows, :]
    r = lax.rsqrt(jnp.mean(x * x, axis=1, keepdims=True) + EPS)
    s.acc[6, :, 0:MODEL] += partial_sum(dn * (x * r))
    h = dn * sm[6:7, :MODEL]
    k = r * r * r * jnp.mean(h * x, axis=1, keepdims=True)
    gtok_ref[rows, :] = r * h - k * x + cot_ref[rows, :].astype(f32)


SCRATCH = dict(
    win=((MODEL, PADDED), bf16),
    wout=((INNER, MODEL), bf16),
    parts=((4, 8, 512), f32),
    sm=((16, CONV_CH), f32),
    hd=((8, 128), f32),
    mixed=((256, MODEL), bf16),
    nrm=((TOKENS, MODEL), bf16),
    u=((TOKENS, CONV_CH), bf16),
    pre=((TOKENS + 16, CONV_CH), bf16),
    xbc=((TOKENS, CONV_CH), bf16),
    dtx=((TOKENS, 128), f32),
    gated=((TOKENS, INNER), bf16),
    dy=((TOKENS, INNER), bf16),
    dz=((TOKENS, INNER), bf16),
    ddt=((TOKENS, 128), bf16),
    z=((256, INNER), f32),
    dg=((256, INNER), f32),
    rowdot=((TOKENS, 128), f32),
    dys=((CHUNK, INNER), bf16),
    xw=((CHUNK, INNER), bf16),
    lowd=((CHUNK, INNER), bf16),
    dwz=((MODEL, INNER), bf16),
    dwu=((MODEL, 2048), bf16),
    dwo=((INNER, MODEL), bf16),
    zr=((1488, MODEL), bf16),
    mine=((4, 56, 256), f32),
    gain=((4, 8, 128), f32),
    gain_slots=((6, 8, 128), f32),
    up=((2, 8 + LEN, 256), f32),
    state=((STATE, INNER), f32),
    states=((SEQ * LEN // CHUNK, STATE, INNER), bf16),
    rowv=((128, 128), f32),
    tail=((8, INNER), f32),
    kept_last=((SEQ * LEN // CHUNK, 8, 128), f32),
    segc=((SEQ, 8 + LEN, 128), f32),
    back=((CONV - 1, LEN, 128), f32),
    one128=((128, HEADS * 128), bf16),
    one64=((128, INNER), bf16),
    sum64=((INNER, 128), bf16),
    acc=((10, 8, CONV_CH), f32),
)


def gather_weights(shards, x_ref, seg_ref, win_own, wout_own, sm_own, hd, s, send_sems, recv_sems, small_send, small_recv):
    win, wout, sm = s.win, s.wout, s.sm
    at = place()
    shard = at.shard
    rows = pl.ds(pl.multiple_of(shard * (MODEL // shards), 16), MODEL // shards)
    win[rows, DT:] = jnp.zeros((MODEL // shards, PADDED - DT), bf16)
    win[rows, :PROJ] = win_own[...]
    own = wout.at[pl.ds(pl.multiple_of(shard * (INNER // shards), 16), INNER // shards), :]
    fetch = pltpu.make_async_copy(wout_own, own, s.mixed_sem)
    fetch.start()
    s.parts[shard] = sm_own[0:8, :]
    fetch.wait()
    hd[0:2, :] = sm_own[8:10, :128]
    greet(at, shards)
    sems = (send_sems, recv_sems)
    conv_part = Gather(at, win, shards, MODEL // shards, INNER, (PADDED - INNER) // 2, sems, 0)
    gate_part = Gather(at, win, shards, MODEL // shards, 0, INNER // 2, sems, 1)
    out_part = Gather(at, wout, shards, INNER // shards, 0, MODEL // 2, sems, 2)

    def small(d):
        return remote(
            s.parts.at[shard],
            s.parts.at[shard],
            small_send.at[d],
            small_recv.at[d],
            at.rep,
            (shard + d) % shards,
        )

    for d in range(1, shards):
        small(d).start()
    conv_part.begin()
    setup(seg_ref, s)
    for d in range(1, shards):
        small(d).wait_recv()
        small(d).wait_send()
    row = rows_of((8, CONV_CH))
    taps = spread_lanes(s.parts, 448, 448)
    gain = spread_lanes(s.parts, 384, 384)
    first = spread_lanes(s.parts, 192, 192)
    sm[0:8, :] = jnp.where(row < 5, taps, jnp.where(row == 5, gain, first))
    skip = packed(jnp.broadcast_to(sm_own[10:11, :128], (8, 128)))
    sm[7:8, :INNER] = nn(skip, s.one64[...])[0:1, :]
    conv_part.spread()
    norm_input(0, x_ref, sm, s)
    conv_part.relay()
    norm_input(1, x_ref, sm, s)
    conv_part.share()
    gate_part.begin()
    out_part.begin()
    conv_part.finish()
    return at, gate_part, out_part


def copy_weights(seg_ref, win_all, wout_all, sm_all, hd, s, sems):
    copies = [
        pltpu.make_async_copy(src, dst, sems.at[i])
        for i, (src, dst) in enumerate(((win_all, s.win), (wout_all, s.wout), (sm_all, s.sm)))
    ]
    for copy in copies:
        copy.start()
    setup(seg_ref, s)
    for copy in copies:
        copy.wait()
    hd[0:2, :] = s.sm[8:10, :128]
    skip = packed(jnp.broadcast_to(s.sm[10:11, :128], (8, 128)))
    s.sm[7:8, :INNER] = nn(skip, s.one64[...])[0:1, :]


def transposed(src, dst):
    for i in range(TOKENS // 128):
        for j in range(MODEL // 128):
            dst[j * 128 : (j + 1) * 128, i * 128 : (i + 1) * 128] = src[
                i * 128 : (i + 1) * 128, j * 128 : (j + 1) * 128
            ].T


def out_weight_gradient(cot_ref, s):
    for j in range(QUADS):
        cols = slice(j * 256, (j + 1) * 256)
        s.dwo[cols, :] = tn(s.gated[:, cols], cot_ref[...]).astype(bf16)


def in_weight_gradient(ref, column, tile):
    def fill(turned):
        for i in range(3):
            rows = slice(i * 256, (i + 1) * 256)
            ref[rows, column : column + tile.shape[1]] = nn(turned[rows, :TOKENS], tile[...]).astype(bf16)

    return fill


def token_gradient(i, win, gtok_ref, s):
    rows = pl.ds(pl.multiple_of(i * 256, 256), 256)
    for j in range(3):
        cols = slice(j * 256, (j + 1) * 256)
        gtok_ref[rows, cols] = (
            nt(s.dz[rows, :], win[cols, :INNER])
            + nt(s.u[rows, :], win[cols, INNER:DT])
            + nt(s.ddt[rows, :], win[cols, DT : DT + 128])
        )


def pack_small(mine, s):
    high, low = two_parts(s.acc[7, :, :INNER])
    skip = nn(high, s.sum64[...]) + nn(low, s.sum64[...])
    s.acc[7, :, 0:128] = skip
    heads = [jnp.sum(s.acc[k, :, 0:128], axis=0, keepdims=True) for k in (7, 8, 9)] + [jnp.zeros((1, 128), f32)]
    for j in range(CONV_CH // 256):
        sums = [jnp.sum(s.acc[k, :, j * 256 : (j + 1) * 256], axis=0, keepdims=True) for k in range(6)]
        tail = jnp.concatenate(heads[2 * j : 2 * j + 2], axis=1) if j < 2 else jnp.zeros((1, 256), f32)
        mine[0, j * 8 : (j + 1) * 8, :] = jnp.concatenate(sums + [tail, jnp.zeros((1, 256), f32)], axis=0)


def pack_gain(mine, s):
    sums = [jnp.sum(s.acc[6, :, j * 128 : (j + 1) * 128], axis=0, keepdims=True) for j in range(MODEL // 128)]
    mine[0] = jnp.concatenate(sums + [jnp.zeros((2, 128), f32)], axis=0)


def layer_kernel(
    direct, shards, x_ref, cot_ref, seg_ref, win_own, wout_own, sm_own, mixed_ref, gtok_ref, gin_ref, gout_ref, gsm_ref, *refs
):
    s = SimpleNamespace(**dict(zip(SCRATCH, refs)))
    s.mixed_sem, *sems = refs[len(SCRATCH) :]
    s.part = s.z
    win, wout, sm, hd = s.win, s.wout, s.sm, s.hd
    if direct:
        *sems, sends, recvs, locals_, total_send, total_recv, forward_done, scan_done = sems
        at, gate_part, out_part = gather_weights(shards, x_ref, seg_ref, win_own, wout_own, sm_own, hd, s, *sems)
        pair = (sends, recvs)
        zr, xbc, dy = s.zr, s.xbc, s.dy
        gate_sum = Reduce(
            at, s.dwz, MODEL, INNER // 2, [(zr, 0, 0), (zr, 768, 0), (zr, 1152, 0), (zr, 1344, 0)], gin_ref, 0, pair, 0, locals_.at[0]
        )
        out_sum = Reduce(
            at, s.dwo, INNER, MODEL // 2, [(wout, 0, 0), (wout, 0, 384), (wout, 768, 384), (wout, 1152, 384)], gout_ref, 0, pair, 1, locals_.at[1]
        )
        early_sum, late_sum = (
            Reduce(
                at,
                s.dwu.at[:, i * 1024 : (i + 1) * 1024],
                MODEL,
                512,
                [(xbc, 0, i * 512), (dy, 0, i * 512), (dy, 384, i * 512), (dy, 576, i * 512)],
                gin_ref,
                INNER + i * 1024,
                pair,
                2 + i,
                locals_.at[2 + i],
            )
            for i in range(2)
        )
        totals = (total_send, total_recv)
        small_sum = Total(
            at, s.mine, lambda i: s.up.at[i // 3, pl.ds(8 + (i % 3) * 56, 56), :], totals, 0
        )
        gain_sum = Total(at, s.gain, lambda i: s.gain_slots.at[i], totals, 1)
    else:
        copy_weights(seg_ref, win_own, wout_own, sm_own, hd, s, *sems)
        for q in range(SEQ):
            norm_input(q, x_ref, sm, s)
    chunks = LEN // CHUNK

    @pl.loop(0, SEQ)
    def _(q):
        project(q, win, sm, hd, s)
        s.state[...] = jnp.zeros((STATE, INNER), f32)
        if direct:

            @pl.when(q == 0)
            def _():
                gate_part.spread()
                out_part.spread()

        @pl.loop(0, chunks)
        def _(c):
            scan_forward(q, c, seg_ref, sm, hd, s)
            if direct:
                polls = ((2, gate_part.relay), (3, out_part.relay))
                for index, poll in polls:

                    @pl.when((q == 0) & (c == index))
                    def _():
                        poll()

                @pl.when((q == 1) & (c == 0))
                def _():
                    gate_part.share()

                @pl.when((q == 1) & (c == 1))
                def _():
                    out_part.share()

    if direct:
        gate_part.finish()
        out_part.finish()

    @pl.loop(0, TOKENS // 256)
    def _(i):
        gate(i, x_ref, cot_ref, win, wout, sm, mixed_ref, s)

    if direct:
        meet(at, shards, forward_done)
    out_weight_gradient(cot_ref, s)
    if direct:
        met(shards, forward_done)
        out_sum.begin()
    turned = s.gated
    transposed(s.nrm, turned)
    for j in range(QUADS):
        in_weight_gradient(s.dwz, j * 256, s.dz.at[:, j * 256 : (j + 1) * 256])(turned)
    if direct:
        gate_sum.begin()

    def backward(quads, first, polls):
        @pl.loop(0, SEQ * chunks)
        def _(n):
            @pl.when(n % chunks == 0)
            def _():
                s.state[:, quads[0] * 256 : (quads[-1] + 1) * 256] = jnp.zeros((STATE, len(quads) * 256), f32)

            scan_backward(n // chunks, chunks - 1 - n % chunks, quads, first, seg_ref, sm, hd, s)
            for index, poll in polls:

                @pl.when(n == index)
                def _():
                    poll()

    polls = ()
    if direct:
        polls = (
            (0, out_sum.first),
            (1, gate_sum.first),
            (3, out_sum.second),
            (5, out_sum.third),
            (6, gate_sum.second),
            (7, out_sum.fourth),
        )
    backward(range(4), True, polls)
    if direct:
        meet(at, shards, scan_done)

    @pl.loop(0, SEQ)
    def _(q):
        conv_backward(q, range(8), sm, s)

    if direct:
        gate_sum.third()
    for j in range(4):
        in_weight_gradient(s.dwu, j * 256, s.u.at[:, j * 256 : (j + 1) * 256])(turned)
    if direct:
        met(shards, scan_done)
        early_sum.begin()
        polls = (
            (0, out_sum.sixth),
            (1, early_sum.first),
            (3, gate_sum.fourth),
            (6, early_sum.second),
            (7, gate_sum.sixth),
        )
    backward(range(4, QUADS), False, polls)

    @pl.loop(0, SEQ)
    def _(q):
        conv_backward(q, range(8, CONV_CH // 128), sm, s)

    for j in range(4, CONV_CH // 256):
        in_weight_gradient(s.dwu, j * 256, s.u.at[:, j * 256 : (j + 1) * 256])(turned)
    in_weight_gradient(s.dwu, CONV_CH, s.ddt)(turned)
    s.dwu[:, CONV_CH + 128 :] = jnp.zeros((MODEL, 128), bf16)
    pack_small(s.mine, s)
    if direct:
        late_sum.begin()
        small_sum.begin()
        early_sum.third()
        small_sum.step(0)

    @pl.loop(0, TOKENS // 256)
    def _(i):
        token_gradient(i, win, gtok_ref, s)
        if direct:

            @pl.when(i == 0)
            def _():
                late_sum.first()

            @pl.when(i == 1)
            def _():
                small_sum.step(1)

            @pl.when(i == 3)
            def _():
                small_sum.step(2)

    if direct:
        early_sum.fourth()

    @pl.loop(0, TOKENS // 64)
    def _(i):
        input_gradient(i, x_ref, cot_ref, sm, gtok_ref, s)

    pack_gain(s.gain, s)
    if direct:
        gain_sum.begin()
        late_sum.second()
        gain_sum.step(0)
        early_sum.sixth()
        gain_sum.step(1)
        late_sum.third()
        gain_sum.step(2)
        out_sum.seventh()
        gate_sum.seventh()
        late_sum.fourth()
        early_sum.seventh()
        late_sum.sixth()
        unpack_small(small_sum.finish(), gain_sum.finish(), gsm_ref)
        late_sum.seventh()
    else:
        unpack_small(s.mine[0], s.gain[0], gsm_ref)
        copies = [
            pltpu.make_async_copy(s.dwz, gin_ref.at[:, :INNER], sems[0].at[0]),
            pltpu.make_async_copy(s.dwu, gin_ref.at[:, INNER:], sems[0].at[1]),
            pltpu.make_async_copy(s.dwo, gout_ref, sems[0].at[2]),
        ]
        for copy in copies:
            copy.start()
        for copy in copies:
            copy.wait()


def reaches(mesh):
    return mesh.shape["rep"] == 8 and mesh.shape["shard"] == 4


def layer(mesh, x, cot, seg, win, wout, sm):
    direct, shards = reaches(mesh), mesh.shape["shard"]
    vmem = pl.BlockSpec(memory_space=pltpu.VMEM)
    hbm = pl.BlockSpec(memory_space=pl.ANY)
    dma = pltpu.SemaphoreType.DMA
    if direct:
        sems = [dma((3, 5, shards)), dma((3, 5, shards)), dma((shards,)), dma((shards,))]
        sems += [dma((4, 10)), dma((4, 10)), dma((4,)), dma((2, 6)), dma((2, 6))]
        sems += [pltpu.SemaphoreType.REGULAR] * 2
        options = dict(collective_id=0, has_side_effects=True)
        weights = vmem
    else:
        sems, options, weights = [dma((3,))], {}, hbm
    return pl.pallas_call(
        partial(layer_kernel, direct, shards),
        out_shape=(
            jax.ShapeDtypeStruct((TOKENS, MODEL), bf16),
            jax.ShapeDtypeStruct((TOKENS, MODEL), f32),
            jax.ShapeDtypeStruct((MODEL // shards if direct else MODEL, PADDED), bf16),
            jax.ShapeDtypeStruct((INNER // shards if direct else INNER, MODEL), bf16),
            jax.ShapeDtypeStruct((16, CONV_CH), f32),
        ),
        in_specs=[vmem] * 3 + [weights, hbm, weights],
        out_specs=[hbm, vmem, hbm, hbm, vmem],
        scratch_shapes=[pltpu.VMEM(shape, kind) for shape, kind in SCRATCH.values()] + [dma] + sems,
        compiler_params=pltpu.CompilerParams(vmem_limit_bytes=67043328, **options),
        name="layer",
    )(x, cot, seg, win, wout, sm)


def placed(v, row, width):
    return jnp.pad(v.astype(f32), ((row, 16 - row - v.shape[0]), (0, width - v.shape[1])))


def on_device(mesh, tokens, segment_ids, norm_gain, in_weight, conv_weight, conv_bias, dt_bias, a_log, d_skip, gate_gain, out_weight, cotangent):
    small, heads = (conv_bias, gate_gain, norm_gain), (dt_bias, a_log, d_skip)
    if reaches(mesh):
        win, wout, taps, width = in_weight, out_weight, conv_weight, 512
    else:
        win, wout, taps, *small = lax.all_gather(
            (in_weight, out_weight, conv_weight) + small, "shard", axis=0, tiled=True
        )
        win, width = jnp.pad(win, ((0, 0), (0, PADDED - PROJ))), CONV_CH
    sm = placed(taps.T, 0, width)
    for row, v in enumerate((*small, jnp.zeros((1,), f32), *heads)):
        sm = sm + placed(v[None], CONV + row, width)
    mixed, gtok, gin, gout, gsm = layer(
        mesh,
        tokens.reshape(TOKENS, MODEL), cotangent.reshape(TOKENS, MODEL), segment_ids, win, wout, sm
    )
    if not reaches(mesh):
        gin = lax.psum(lax.psum_scatter(gin, "shard", scatter_dimension=0, tiled=True), "rep")
        gout = lax.psum(lax.psum_scatter(gout, "shard", scatter_dimension=0, tiled=True), "rep")
        gsm = lax.psum(gsm, ("rep", "shard"))
    me = lax.axis_index("shard")

    def owned(v, like):
        return lax.dynamic_slice_in_dim(v, me * like.shape[0], like.shape[0])

    return (
        mixed.reshape(SEQ, LEN, MODEL),
        gtok.reshape(SEQ, LEN, MODEL),
        owned(gsm[6, :MODEL], norm_gain),
        gin[:, :PROJ].astype(f32),
        owned(gsm[:CONV].T, conv_weight),
        owned(gsm[4], conv_bias),
        gsm[8, :HEADS],
        gsm[9, :HEADS],
        gsm[7, :HEADS],
        owned(gsm[5, :INNER], gate_gain),
        gout.astype(f32),
    )


def solution(mesh):
    batch = P(("rep", "shard"), None, None)
    return jax.shard_map(
        partial(on_device, mesh),
        mesh=mesh,
        in_specs=(
            batch,
            P(("rep", "shard"), None),
            P("shard"),
            P("shard", None),
            P("shard", None),
            P("shard"),
            P(),
            P(),
            P(),
            P("shard"),
            P("shard", None),
            batch,
        ),
        out_specs=(
            batch,
            batch,
            P("shard"),
            P("shard", None),
            P("shard", None),
            P("shard"),
            P(),
            P(),
            P(),
            P("shard"),
            P("shard", None),
        ),
        check_vma=False,
    )
```

```python
from functools import partial
from types import SimpleNamespace

import jax
import jax.numpy as jnp
from jax import lax
from jax.experimental import pallas as pl
from jax.experimental.pallas import tpu as pltpu
from jax.sharding import PartitionSpec as P

HEADS = 24
HEADDIM = 64
STATE = 128
CONV = 4
INNER = 1536
CONV_CH = 1792
MODEL = 768
PROJ = 3352
PADDED = 3584
DT = INNER + CONV_CH
EPS = 1e-05
MESH = pl.DeviceIdType.MESH

LEN = 512
CHUNK = 128
SEQ = 2
TOKENS = SEQ * LEN
QUADS = INNER // 256

f32 = jnp.float32
bf16 = jnp.bfloat16


def nn(a, b):
    return lax.dot_general(a, b, (((1,), (0,)), ((), ())), preferred_element_type=f32)


def nt(a, b):
    return lax.dot_general(a, b, (((1,), (1,)), ((), ())), preferred_element_type=f32)


def tn(a, b):
    return lax.dot_general(a, b, (((0,), (0,)), ((), ())), preferred_element_type=f32)


def exact(a, b):
    return lax.dot_general(
        a, b, (((1,), (0,)), ((), ())), preferred_element_type=f32, precision=lax.Precision.HIGHEST
    )


def sigmoid(v):
    return 0.5 * jnp.tanh(0.5 * v) + 0.5


def partial_sum(a):
    return a.reshape(a.shape[0] // 8, 8, a.shape[1]).sum(axis=0)


def lanes_of(shape):
    return lax.broadcasted_iota(jnp.int32, shape, 1)


def rows_of(shape):
    return lax.broadcasted_iota(jnp.int32, shape, 0)


def packed(a):
    a = jnp.where(lanes_of(a.shape) < HEADS, a, 0.0)
    high = a.astype(bf16).astype(f32)
    rest = a - high
    middle = rest.astype(bf16).astype(f32)
    low = rest - middle
    return (high + pltpu.roll(middle, 32, 1) + pltpu.roll(low, 64, 1)).astype(bf16)


def two_parts(a):
    high = a.astype(bf16)
    return high, (a - high.astype(f32)).astype(bf16)


def scanned(s, rows, cols):
    return s.dy[rows, cols].astype(f32) + s.dz[rows, cols].astype(f32)


def place():
    rep, shard = lax.axis_index("rep"), lax.axis_index("shard")
    core = rep % 2
    px, py = (rep // 2) % 2, rep // 4
    a = px * (1 - core) + py * core
    b = py * (1 - core) + px * core
    return SimpleNamespace(
        rep=rep,
        shard=shard,
        core=core,
        a=a,
        b=b,
        one=rep + (1 - 2 * a) * (2 + 2 * core),
        far=rep + (1 - 2 * a) * (2 + 2 * core) + (1 - 2 * b) * (4 - 2 * core),
        two=rep + (1 - 2 * b) * (4 - 2 * core),
        mate=rep + 1 - 2 * core,
    )


def greet(at, shards):
    barrier = pltpu.get_barrier_semaphore()
    for who in (at.one, at.two, at.far, at.mate):
        pl.semaphore_signal(barrier, inc=1, device_id=(who, at.shard), device_id_type=MESH)
    for d in range(1, shards):
        pl.semaphore_signal(
            barrier, inc=1, device_id=(at.rep, (at.shard + d) % shards), device_id_type=MESH
        )
    pl.semaphore_wait(barrier, 3 + shards)


def remote(src, dst, send, recv, rep, shard):
    return pltpu.make_async_remote_copy(
        src_ref=src, dst_ref=dst, send_sem=send, recv_sem=recv, device_id=(rep, shard), device_id_type=MESH
    )


class Gather:
    def __init__(self, at, ref, shards, rows, start, half, sems, part):
        self.at, self.ref, self.shards, self.rows, self.start, self.half = at, ref, shards, rows, start, half
        self.send, self.recv = (lambda kind, d: sems[0].at[part, kind, d]), (lambda kind, d: sems[1].at[part, kind, d])

    def columns(self):
        return pl.ds(pl.multiple_of(self.start + self.at.core * self.half, 128), self.half)

    def piece(self, shard, a, b):
        tall = self.rows // 4
        return self.ref.at[pl.ds(pl.multiple_of(shard * self.rows + (2 * b + a) * tall, 16), tall), self.columns()]

    def strip(self, shard):
        return self.ref.at[pl.ds(pl.multiple_of(shard * self.rows, 16), self.rows), self.columns()]

    def source(self, d):
        return (self.at.shard + self.shards - d) % self.shards

    def copy(self, kind, d):
        at = self.at
        if kind == 0:
            own = self.piece(at.shard, at.a, at.b)
            return remote(own, own, self.send(0, d), self.recv(0, d), at.rep, (at.shard + d) % self.shards)
        if kind == 4:
            what, who = self.strip(self.source(d)), at.mate
        elif kind == 3:
            what, who = self.piece(self.source(d), at.a, 1 - at.b), at.one
        else:
            what, who = self.piece(self.source(d), at.a, at.b), at.one if kind == 1 else at.two
        return remote(what, what, self.send(kind, d), self.recv(kind, d), who, at.shard)

    def each(self):
        return range(1, self.shards)

    def begin(self):
        for d in self.each():
            self.copy(0, d).start()

    def spread(self):
        for d in self.each():
            self.copy(0, d).wait_recv()
            self.copy(2, d).start()
            self.copy(1, d).start()

    def relay(self):
        for d in self.each():
            self.copy(2, d).wait_recv()
            self.copy(3, d).start()

    def share(self):
        for d in self.each():
            self.copy(1, d).wait_recv()
            self.copy(3, d).wait_recv()
            self.copy(4, d).start()

    def finish(self):
        for d in self.each():
            self.copy(4, d).wait_recv()
            for kind in range(5):
                self.copy(kind, d).wait_send()


def meet(at, shards, sem):
    for who in (at.one, at.two, at.far, at.mate):
        pl.semaphore_signal(sem, inc=1, device_id=(who, at.shard), device_id_type=MESH)
    for d in range(1, shards):
        pl.semaphore_signal(sem, inc=1, device_id=(at.rep, (at.shard + d) % shards), device_id_type=MESH)


def met(shards, sem):
    pl.semaphore_wait(sem, 3 + shards)


class Reduce:
    def __init__(self, at, grad, rows, half, slots, out, column, sems, part, local):
        self.at, self.grad, self.rows, self.half, self.slots = at, grad, rows, half, slots
        self.out, self.column = out, column
        self.tall, self.own_rows = rows // 16, rows // 4
        self.send, self.recv = (lambda i: sems[0].at[part, i]), (lambda i: sems[1].at[part, i])
        self.local = local
        self.keep = pl.ds(pl.multiple_of(at.core * half, 128), half)
        self.give = pl.ds(pl.multiple_of((1 - at.core) * half, 128), half)

    def slot(self, level, start, count):
        ref, row, column = self.slots[level]
        return ref.at[pl.ds(row + start, count), pl.ds(column, self.half)]

    def at_block(self, shard, a, b):
        return pl.multiple_of(shard * self.own_rows + (2 * b + a) * self.tall, 16)

    def block(self, shard, a, b):
        return self.grad.at[pl.ds(self.at_block(shard, a, b), self.tall), self.keep]

    def to(self, src, dst, index, who):
        rep, shard = who
        return remote(src, dst, self.send(index), self.recv(index), rep, shard)

    def partner(self, name):
        return name, self.at.shard

    def add(self, start, level, place_in_slot):
        rows = pl.ds(start, self.tall)
        got = self.slot(level, place_in_slot, self.tall)[...]
        self.grad[rows, self.keep] = (self.grad[rows, self.keep].astype(f32) + got.astype(f32)).astype(bf16)

    def halves(self):
        whole = self.slot(0, 0, self.rows)
        return self.to(self.grad.at[:, self.give], whole, 0, self.partner(self.at.mate))

    def begin(self):
        self.halves().start()

    def first(self):
        at = self.at
        self.halves().wait_recv()

        @pl.loop(0, 16)
        def _(i):
            start = pl.multiple_of(i * self.tall, 16)
            self.add(start, 0, start)

        for shard in range(4):
            for b in range(2):
                self.to(
                    self.block(shard, 1 - at.a, b),
                    self.slot(1, (2 * shard + b) * self.tall, self.tall),
                    1,
                    self.partner(self.at.one),
                ).start()

    def all_of(self, level, index, name):
        whole = self.slot(level, 0, self.rows >> level)
        return self.to(whole, whole, index, self.partner(name))

    def second(self):
        at = self.at
        self.all_of(1, 1, self.at.one).wait_recv()
        for shard in range(4):
            for b in range(2):
                self.add(self.at_block(shard, at.a, b), 1, (2 * shard + b) * self.tall)
        for shard in range(4):
            self.to(
                self.block(shard, at.a, 1 - at.b),
                self.slot(2, shard * self.tall, self.tall),
                2,
                self.partner(self.at.two),
            ).start()

    def across(self, d):
        at = self.at
        shard = (at.shard + d) % 4
        return self.to(
            self.block(shard, at.a, at.b), self.slot(3, (d - 1) * self.tall, self.tall), 2 + d, (at.rep, shard)
        )

    def third(self):
        at = self.at
        self.all_of(2, 2, self.at.two).wait_recv()
        for shard in range(4):
            self.add(self.at_block(shard, at.a, at.b), 2, shard * self.tall)
        for d in range(1, 4):
            self.across(d).start()

    def landed(self, a, b):
        rows = pl.ds(pl.multiple_of((2 * b + a) * self.tall, 16), self.tall)
        return self.out.at[rows, pl.ds(pl.multiple_of(self.column + self.at.core * self.half, 128), self.half)]

    def spread(self, index):
        at = self.at
        own = self.block(at.shard, at.a, at.b)
        return self.to(own, self.landed(at.a, at.b), index, self.partner((at.one, at.two, at.far)[index - 6]))

    def home(self):
        at = self.at
        own = self.block(at.shard, at.a, at.b)
        return pltpu.make_async_copy(own, self.landed(at.a, at.b), self.local)

    def fourth(self):
        at = self.at
        for d in range(1, 4):
            self.across(d).wait_recv()
        rows = pl.ds(self.at_block(at.shard, at.a, at.b), self.tall)
        total = self.grad[rows, self.keep].astype(f32)
        for d in range(1, 4):
            total = total + self.slot(3, (d - 1) * self.tall, self.tall)[...].astype(f32)
        self.grad[rows, self.keep] = total.astype(bf16)
        for index in (8, 7, 6):
            self.spread(index).start()
        self.home().start()

    def strip(self):
        columns = pl.ds(pl.multiple_of(self.column + self.at.core * self.half, 128), self.half)
        return self.to(self.out.at[:, columns], self.out.at[:, columns], 9, self.partner(self.at.mate))

    def sixth(self):
        self.home().wait()
        for index in (6, 7, 8):
            self.spread(index).wait_recv()
        self.strip().start()

    def seventh(self):
        self.strip().wait_recv()
        self.halves().wait_send()
        self.all_of(1, 1, self.at.one).wait_send()
        self.all_of(2, 2, self.at.two).wait_send()
        for d in range(1, 4):
            self.across(d).wait_send()
        for index in (6, 7, 8):
            self.spread(index).wait_send()
        self.strip().wait_send()


def unpack_small(total, gain, out):
    for j in range(CONV_CH // 256):
        out[0:8, j * 256 : (j + 1) * 256] = total[j * 8 : (j + 1) * 8, :]
    for j in range(MODEL // 128):
        out[6:7, j * 128 : (j + 1) * 128] = gain[j : j + 1, :]
    for k in range(3):
        out[7 + k : 8 + k, 0:128] = total[8 * (k // 2) + 6 : 8 * (k // 2) + 7, (k % 2) * 128 : (k % 2 + 1) * 128]


class Total:
    def __init__(self, at, mine, slot, sems, part):
        self.at, self.mine, self.slot = at, mine, slot
        self.send, self.recv = (lambda i: sems[0].at[part, i]), (lambda i: sems[1].at[part, i])

    def copy(self, index):
        at = self.at
        if index < 3:
            who = (at.mate, at.one, at.two)[index], at.shard
        else:
            who = at.rep, (at.shard + index - 2) % 4
        return remote(self.mine.at[min(index, 3)], self.slot(index), self.send(index), self.recv(index), *who)

    def begin(self):
        self.copy(0).start()

    def step(self, index):
        self.copy(index).wait_recv()
        self.mine[index + 1] = self.mine[index] + self.slot(index)[...]
        for following in (index + 1,) if index < 2 else (3, 4, 5):
            self.copy(following).start()

    def finish(self):
        total = self.mine[3]
        for index in (3, 4, 5):
            self.copy(index).wait_recv()
            total = total + self.slot(index)[...]
        for index in range(6):
            self.copy(index).wait_send()
        return total


def spread_lanes(block, width, offset):
    total = jnp.zeros((8, CONV_CH), f32)
    for z in range(4):
        part = jnp.where(lanes_of((8, 512)) < width, block[z], 0.0)
        part = jnp.concatenate([part, jnp.zeros((8, CONV_CH - 512), f32)], axis=1)
        total = total + (part if z == 0 else pltpu.roll(part, z * offset, 1))
    return total


def setup(seg_ref, s):
    r, c = rows_of((128, 256)), lanes_of((128, 256))
    for j in range(HEADS * 128 // 256):
        s.one128[:, j * 256 : (j + 1) * 256] = (
            ((r & 31) == ((c + j * 256) >> 7)) & (r < 96)
        ).astype(f32).astype(bf16)
    for j in range(QUADS):
        s.one64[:, j * 256 : (j + 1) * 256] = (
            ((r & 31) == ((c + j * 256) >> 6)) & (r < 96)
        ).astype(f32).astype(bf16)
    r, c = rows_of((256, 128)), lanes_of((256, 128))
    for j in range(QUADS):
        s.sum64[j * 256 : (j + 1) * 256, :] = (((r + j * 256) >> 6) == c).astype(f32).astype(bf16)
    s.acc[...] = jnp.zeros(s.acc.shape, f32)
    s.pre[TOKENS:, :] = jnp.zeros((16, CONV_CH), bf16)
    s.up[:, 0:8, :] = jnp.zeros((2, 8, 256), f32)
    for q in range(SEQ):
        s.segc[q, 0:8, :] = jnp.full((8, 128), -1.0, f32)
        for i in range(LEN // 128):
            seg = seg_ref[q : q + 1, i * 128 : (i + 1) * 128].astype(f32)
            s.segc[q, 8 + i * 128 : 8 + (i + 1) * 128, :] = jnp.broadcast_to(seg, (128, 128)).T


def norm_input(q, x_ref, sm, s):
    @pl.loop(0, LEN // 64)
    def _(i):
        rows = pl.ds(pl.multiple_of(q * LEN + i * 64, 64), 64)
        x = x_ref[rows, :].astype(f32)
        r = lax.rsqrt(jnp.mean(x * x, axis=1, keepdims=True) + EPS)
        s.nrm[rows, :] = (x * r * sm[6:7, :MODEL]).astype(bf16)


def project(q, win, sm, hd, s):
    row0 = pl.multiple_of(q * LEN, LEN)
    seg = s.segc[q, 8 : 8 + LEN, :]
    place = rows_of((LEN, 128))
    for o in range(1, CONV):
        s.back[o - 1] = ((seg == pltpu.roll(seg, o, 0)) & (place >= o)).astype(f32)
    rows = pl.ds(row0, LEN)
    raw = nn(s.nrm[rows, :], win[:, DT : DT + 128]) + hd[0:1, :]
    s.dtx[rows, :] = raw
    for j in range(CONV_CH // 256):
        slot = j % 2
        s.up[slot, 8:, :] = nn(s.nrm[rows, :], win[:, INNER + j * 256 : INNER + (j + 1) * 256])
        for i in range(LEN // 128):
            for half in range(2):
                c0 = j * 256 + half * 128
                here = pl.ds(row0 + i * 128, 128)
                block = s.up[slot, i * 128 : i * 128 + 136, half * 128 : (half + 1) * 128]
                u = block[8:]
                tap = lambda k: sm[k : k + 1, c0 : c0 + 128]
                pre = sm[4:5, c0 : c0 + 128] + tap(3) * u
                for o in range(1, CONV):
                    same = s.back[o - 1, i * 128 : (i + 1) * 128, :]
                    pre = pre + tap(3 - o) * (pltpu.roll(block, o, 0)[8:] * same)
                s.u[here, c0 : c0 + 128] = u.astype(bf16)
                s.pre[here, c0 : c0 + 128] = pre.astype(bf16)
                s.xbc[here, c0 : c0 + 128] = (pre * sigmoid(pre)).astype(bf16)


def chunk_terms(q, c, seg_ref, hd, s):
    row0 = pl.multiple_of(q * LEN + c * CHUNK, CHUNK)
    rows = pl.ds(row0, CHUNK)
    raw = s.dtx[rows, :]
    dt = jnp.maximum(raw, 0.0) + jnp.log1p(jnp.exp(-jnp.abs(raw)))
    rate = -jnp.exp(hd[1:2, :]) * dt
    lower = (rows_of((CHUNK, CHUNK)) >= lanes_of((CHUNK, CHUNK))).astype(f32)
    cum = exact(lower, rate)
    source = cum - jnp.log(jnp.maximum(dt, 1e-37))
    start = 8 + c * CHUNK
    segc = s.segc[q, pl.ds(pl.multiple_of(start, 8), CHUNK), :]
    segr = segc.T
    before = s.segc[q, pl.ds(pl.multiple_of(start - 8, 8), 8), :][7:8]
    last = segc[CHUNK - 1 : CHUNK]
    carry = (segc == before).astype(f32)
    tail = (segc == last).astype(f32)
    end = cum[CHUNK - 1 : CHUNK, :]
    keep = jnp.exp(end) * (before == last).astype(f32)
    grow = jnp.exp(cum) * carry
    shrink = jnp.exp(end - source) * tail
    return rows, raw, dt, rate, cum, source, segc, segr, grow, shrink, keep


def scan_forward(q, c, seg_ref, sm, hd, s):
    rows, raw, dt, rate, cum, source, segc, segr, grow, shrink, keep = chunk_terms(q, c, seg_ref, hd, s)
    t, k = rows_of((CHUNK, CHUNK)), lanes_of((CHUNK, CHUNK))
    bound = jnp.where((segc == segr) & (t >= k), 3e38, -1e30)
    s.rowv[...] = source.T
    target = packed(cum)
    grow_p, shrink_p = packed(grow), packed(shrink)
    keep_p = packed(jnp.broadcast_to(keep, (8, 128)))
    bv = s.xbc[rows, INNER : INNER + STATE]
    cv = s.xbc[rows, INNER + STATE :]
    gram = nt(cv, bv)
    bt = bv.T
    at = q * (LEN // CHUNK) + c
    left = lanes_of((CHUNK, 128)) < HEADDIM
    for j in range(QUADS):
        cols = slice(j * 256, (j + 1) * 256)
        grow_e = nn(grow_p, s.one64[:, cols])
        shrink_e = nn(shrink_p, s.one64[:, cols])
        keep_e = nn(keep_p, s.one64[:, cols])[0:1, :]
        state = s.state[:, cols]
        low_state = state.astype(bf16)
        s.states[at, :, cols] = low_state
        y_state = nn(cv, low_state)
        xv = s.xbc[rows, cols]
        xw = (xv.astype(f32) * shrink_e).astype(bf16)
        s.state[:, cols] = state * keep_e + nn(bt, xw)
        parts = []
        for pair in range(2):
            spread = nn(target, s.one128[:, j * 512 + pair * 256 : j * 512 + (pair + 1) * 256])
            weights = []
            for half in range(2):
                head = 4 * j + 2 * pair + half
                d = spread[:, half * 128 : (half + 1) * 128] - s.rowv[head : head + 1, :]
                weights.append((gram * jnp.exp(jnp.minimum(d, bound))).astype(bf16))
            x2 = xv[:, pair * 128 : (pair + 1) * 128]
            zero = jnp.zeros_like(x2)
            stack = jnp.concatenate([jnp.where(left, x2, zero), jnp.where(left, zero, x2)], axis=0)
            parts.append(nn(jnp.concatenate(weights, axis=1), stack))
        s.dy[rows, cols], s.dz[rows, cols] = two_parts(jnp.concatenate(parts, axis=1) + y_state * grow_e)


def gate(i, x_ref, cot_ref, win, wout, sm, mixed_ref, s):
    tall, block = 256, 64
    row0 = i * tall
    rows = pl.ds(pl.multiple_of(row0, tall), tall)
    for j in range(QUADS):
        cols = slice(j * 256, (j + 1) * 256)
        s.z[:, cols] = nn(s.nrm[rows, :], win[:, cols])
        s.dg[:, cols] = nt(cot_ref[rows, :], wout[cols, :])

    @pl.loop(0, tall // block)
    def _(b):
        own = pl.ds(pl.multiple_of(b * block, block), block)
        where = pl.ds(pl.multiple_of(row0 + b * block, block), block)
        square = jnp.zeros((block, 128), f32)
        along = jnp.zeros((block, 128), f32)
        for j in range(INNER // 128):
            cols = slice(j * 128, (j + 1) * 128)
            z = s.z[own, cols]
            y = scanned(s, where, cols) + sm[7:8, cols] * s.xbc[where, cols].astype(f32)
            v = y * (z * sigmoid(z))
            square = square + v * v
            along = along + s.dg[own, cols] * sm[5:6, cols] * v
        r = lax.rsqrt(jnp.sum(square, axis=1, keepdims=True) * (1.0 / INNER) + EPS)
        k = r * r * r * (jnp.sum(along, axis=1, keepdims=True) * (1.0 / INNER))
        for j in range(INNER // 128):
            cols = slice(j * 128, (j + 1) * 128)
            z = s.z[own, cols]
            dg = s.dg[own, cols]
            ys = scanned(s, where, cols)
            xv = s.xbc[where, cols].astype(f32)
            y = ys + sm[7:8, cols] * xv
            sg = sigmoid(z)
            zs = z * sg
            v = y * zs
            vr = v * r
            gain = sm[5:6, cols]
            s.gated[where, cols] = (vr * gain).astype(bf16)
            s.acc[5, :, cols] += partial_sum(dg * vr)
            dv = r * (dg * gain) - v * k
            dy = dv * zs
            low_dy = dy.astype(bf16)
            s.dy[where, cols] = low_dy
            s.dz[where, cols] = (dv * y * (sg + zs * (1.0 - sg))).astype(bf16)
            s.acc[7, :, cols] += partial_sum(dy * xv)
            s.dg[own, cols] = low_dy.astype(f32) * ys

    high, low = two_parts(s.dg[...])
    s.rowdot[rows, :] = nn(high, s.sum64[...]) + nn(low, s.sum64[...])
    branch = nn(s.gated[rows, :], wout[...])
    s.mixed[...] = (x_ref[rows, :].astype(f32) + branch).astype(bf16)
    out = pltpu.make_async_copy(s.mixed, mixed_ref.at[rows, :], s.mixed_sem)
    out.start()
    out.wait()


def set_aside(s, at, kind):
    row, column = (at // 4) * 128, ((at % 4) * 3 + kind) * 128
    return s.dg.at[pl.ds(pl.multiple_of(row, 128), 128), pl.ds(pl.multiple_of(column, 128), 128)]


def sums_aside(s, at):
    return s.z.at[128:256, pl.ds(pl.multiple_of(at * 128, 128), 128)]


def scan_backward(q, c, quads, first, seg_ref, sm, hd, s):
    rows, raw, dt, rate, cum, source, segc, segr, grow, shrink, keep = chunk_terms(q, c, seg_ref, hd, s)
    k, t = rows_of((CHUNK, CHUNK)), lanes_of((CHUNK, CHUNK))
    allowed = (segc == segr) & (t >= k)
    bound = jnp.where(allowed, 3e38, -1e30)
    s.rowv[...] = cum.T
    origin = packed(source)
    grow_p, shrink_p = packed(grow), packed(shrink)
    keep_p = packed(jnp.broadcast_to(keep, (8, 128)))
    bv = s.xbc[rows, INNER : INNER + STATE]
    cv = s.xbc[rows, INNER + STATE :]
    gram = nt(bv, cv)
    ct = cv.T
    at = q * (LEN // CHUNK) + c
    left = lanes_of((CHUNK, 128)) < HEADDIM
    dgram = jnp.zeros((CHUNK, CHUNK), f32) if first else set_aside(s, at, 0)[...]
    for j in quads:
        cols = slice(j * 256, (j + 1) * 256)
        grow_e = nn(grow_p, s.one64[:, cols])
        s.dys[:, cols] = (s.dy[rows, cols].astype(f32) * grow_e).astype(bf16)
        shrink_e = nn(shrink_p, s.one64[:, cols])
        s.xw[:, cols] = (s.xbc[rows, cols].astype(f32) * shrink_e).astype(bf16)
        low_dstate = s.state[:, cols].astype(bf16)
        s.lowd[:, cols] = low_dstate
        part = nn(bv, low_dstate) * shrink_e
        s.part[:CHUNK, cols] = part
        keep_e = nn(keep_p, s.one64[:, cols])[0:1, :]
        kept = s.state[:, cols] * keep_e
        s.tail[:, cols] = partial_sum(s.xbc[rows, cols].astype(f32) * part) + partial_sum(
            kept * s.states[at, :, cols].astype(f32)
        )
        s.state[:, cols] = kept + nn(ct, s.dys[:, cols])
    for j in range(2 * quads[0], 2 * quads[-1] + 2):
        cols = slice(j * 128, (j + 1) * 128)
        xv = s.xbc[rows, cols]
        dy = s.dy[rows, cols]
        spread = nn(origin, s.one128[:, j * 256 : (j + 1) * 256])
        zero = jnp.zeros_like(dy)
        stack = jnp.concatenate([jnp.where(left, dy, zero), jnp.where(left, zero, dy)], axis=0)
        dweights = nt(xv, stack)
        weights = []
        for half in range(2):
            head = 2 * j + half
            d = s.rowv[head : head + 1, :] - spread[:, half * 128 : (half + 1) * 128]
            e = jnp.exp(jnp.minimum(d, bound))
            weights.append((gram * e).astype(bf16))
            dgram = dgram + dweights[:, half * 128 : (half + 1) * 128] * e
        dx = nn(jnp.concatenate(weights, axis=1), stack) + s.part[:CHUNK, cols]
        s.part[:CHUNK, cols] = xv.astype(f32) * dx
        dx = dx + sm[7:8, cols] * dy.astype(f32)
        pre = s.pre[rows, cols].astype(f32)
        sg = sigmoid(pre)
        s.pre[rows, cols] = (dx * (sg * (1.0 + pre * (1.0 - sg)))).astype(bf16)
    some = slice(quads[0] * 256, (quads[-1] + 1) * 256)
    high, low = two_parts(s.part[:CHUNK, some])
    colsum = nn(high, s.sum64[some, :]) + nn(low, s.sum64[some, :])
    high, low = two_parts(s.tail[:, some])
    dlast = nn(high, s.sum64[some, :]) + nn(low, s.sum64[some, :])
    dc = nt(s.dys[:, some], s.states[at, :, some])
    db = nt(s.xw[:, some], s.lowd[:, some])
    if first:
        for index, value in enumerate((dgram, db, dc)):
            set_aside(s, at, index)[...] = value
        sums_aside(s, at)[...] = colsum
        s.kept_last[at] = dlast
        return
    db, dc, colsum = db + set_aside(s, at, 1)[...], dc + set_aside(s, at, 2)[...], colsum + sums_aside(s, at)[...]
    dlast = jnp.sum(dlast + s.kept_last[at], axis=0, keepdims=True)
    low_dgram = dgram.astype(bf16)
    db = db + nn(low_dgram, cv)
    dc = dc + tn(low_dgram, bv)
    for index, d in ((0, db), (1, dc)):
        cols = slice(INNER + index * STATE, INNER + (index + 1) * STATE)
        pre = s.pre[rows, cols].astype(f32)
        sg = sigmoid(pre)
        s.pre[rows, cols] = (d * (sg * (1.0 + pre * (1.0 - sg)))).astype(bf16)
    dcum = s.rowdot[rows, :] - colsum
    drate = exact(allowed.astype(f32), dcum) + dlast * (segc == segc[CHUNK - 1 : CHUNK]).astype(f32)
    sg = sigmoid(raw)
    ratio = jnp.where(dt > 1e-30, sg / jnp.maximum(dt, 1e-30), 1.0)
    draw = colsum * ratio - drate * jnp.exp(hd[1:2, :]) * sg
    draw = jnp.where(lanes_of((CHUNK, 128)) < HEADS, draw, 0.0)
    s.ddt[rows, :] = draw.astype(bf16)
    s.acc[8, :, 0:128] += partial_sum(draw)
    s.acc[9, :, 0:128] += partial_sum(drate * rate)


def conv_backward(q, tiles, sm, s):
    row0 = pl.multiple_of(q * LEN, LEN)
    rows = pl.ds(row0, LEN)
    seg = s.segc[q, 8 : 8 + LEN, :]
    place = rows_of((LEN, 128))
    for o in range(1, CONV):
        s.back[o - 1] = ((seg == pltpu.roll(seg, LEN - o, 0)) & (place < LEN - o)).astype(f32)
    for j in tiles:
        cols = slice(j * 128, (j + 1) * 128)
        sums = [jnp.zeros((8, 128), f32)] * 5
        for i in range(LEN // 128):
            here = pl.ds(row0 + i * 128, 128)
            block = s.pre[pl.ds(row0 + i * 128, 144), cols].astype(f32)
            ds = block[:128]
            u = s.u[here, cols].astype(f32)
            du = sm[3:4, cols] * ds
            sums[4] = sums[4] + partial_sum(ds)
            sums[3] = sums[3] + partial_sum(ds * u)
            for o in range(1, CONV):
                moved = pltpu.roll(block, 144 - o, 0)[:128] * s.back[o - 1, i * 128 : (i + 1) * 128, :]
                du = du + sm[3 - o : 4 - o, cols] * moved
                sums[3 - o] = sums[3 - o] + partial_sum(moved * u)
            s.u[here, cols] = du.astype(bf16)
        for k in range(5):
            s.acc[k, :, cols] += sums[k]


def input_gradient(i, x_ref, cot_ref, sm, gtok_ref, s):
    rows = pl.ds(pl.multiple_of(i * 64, 64), 64)
    x = x_ref[rows, :].astype(f32)
    dn = gtok_ref[rows, :]
    r = lax.rsqrt(jnp.mean(x * x, axis=1, keepdims=True) + EPS)
    s.acc[6, :, 0:MODEL] += partial_sum(dn * (x * r))
    h = dn * sm[6:7, :MODEL]
    k = r * r * r * jnp.mean(h * x, axis=1, keepdims=True)
    gtok_ref[rows, :] = r * h - k * x + cot_ref[rows, :].astype(f32)


SCRATCH = dict(
    win=((MODEL, PADDED), bf16),
    wout=((INNER, MODEL), bf16),
    parts=((4, 8, 512), f32),
    sm=((16, CONV_CH), f32),
    hd=((8, 128), f32),
    mixed=((256, MODEL), bf16),
    nrm=((TOKENS, MODEL), bf16),
    u=((TOKENS, CONV_CH), bf16),
    pre=((TOKENS + 16, CONV_CH), bf16),
    xbc=((TOKENS, CONV_CH), bf16),
    dtx=((TOKENS, 128), f32),
    gated=((TOKENS, INNER), bf16),
    dy=((TOKENS, INNER), bf16),
    dz=((TOKENS, INNER), bf16),
    ddt=((TOKENS, 128), bf16),
    z=((256, INNER), f32),
    dg=((256, INNER), f32),
    rowdot=((TOKENS, 128), f32),
    dys=((CHUNK, INNER), bf16),
    xw=((CHUNK, INNER), bf16),
    lowd=((CHUNK, INNER), bf16),
    dwz=((MODEL, INNER), bf16),
    dwu=((MODEL, 2048), bf16),
    dwo=((INNER, MODEL), bf16),
    zr=((1488, MODEL), bf16),
    mine=((4, 56, 256), f32),
    gain=((4, 8, 128), f32),
    gain_slots=((6, 8, 128), f32),
    up=((2, 8 + LEN, 256), f32),
    state=((STATE, INNER), f32),
    states=((SEQ * LEN // CHUNK, STATE, INNER), bf16),
    rowv=((128, 128), f32),
    tail=((8, INNER), f32),
    kept_last=((SEQ * LEN // CHUNK, 8, 128), f32),
    segc=((SEQ, 8 + LEN, 128), f32),
    back=((CONV - 1, LEN, 128), f32),
    one128=((128, HEADS * 128), bf16),
    one64=((128, INNER), bf16),
    sum64=((INNER, 128), bf16),
    acc=((10, 8, CONV_CH), f32),
)


def gather_weights(shards, x_ref, seg_ref, win_own, wout_own, sm_own, hd, s, send_sems, recv_sems, small_send, small_recv):
    win, wout, sm = s.win, s.wout, s.sm
    at = place()
    shard = at.shard
    rows = pl.ds(pl.multiple_of(shard * (MODEL // shards), 16), MODEL // shards)
    win[rows, DT:] = jnp.zeros((MODEL // shards, PADDED - DT), bf16)
    win[rows, :PROJ] = win_own[...]
    own = wout.at[pl.ds(pl.multiple_of(shard * (INNER // shards), 16), INNER // shards), :]
    fetch = pltpu.make_async_copy(wout_own, own, s.mixed_sem)
    fetch.start()
    s.parts[shard] = sm_own[0:8, :]
    fetch.wait()
    hd[0:2, :] = sm_own[8:10, :128]
    greet(at, shards)
    sems = (send_sems, recv_sems)
    conv_part = Gather(at, win, shards, MODEL // shards, INNER, (PADDED - INNER) // 2, sems, 0)
    gate_part = Gather(at, win, shards, MODEL // shards, 0, INNER // 2, sems, 1)
    out_part = Gather(at, wout, shards, INNER // shards, 0, MODEL // 2, sems, 2)

    def small(d):
        return remote(
            s.parts.at[shard],
            s.parts.at[shard],
            small_send.at[d],
            small_recv.at[d],
            at.rep,
            (shard + d) % shards,
        )

    for d in range(1, shards):
        small(d).start()
    conv_part.begin()
    setup(seg_ref, s)
    for d in range(1, shards):
        small(d).wait_recv()
        small(d).wait_send()
    row = rows_of((8, CONV_CH))
    taps = spread_lanes(s.parts, 448, 448)
    gain = spread_lanes(s.parts, 384, 384)
    first = spread_lanes(s.parts, 192, 192)
    sm[0:8, :] = jnp.where(row < 5, taps, jnp.where(row == 5, gain, first))
    skip = packed(jnp.broadcast_to(sm_own[10:11, :128], (8, 128)))
    sm[7:8, :INNER] = nn(skip, s.one64[...])[0:1, :]
    conv_part.spread()
    norm_input(0, x_ref, sm, s)
    conv_part.relay()
    norm_input(1, x_ref, sm, s)
    conv_part.share()
    gate_part.begin()
    out_part.begin()
    conv_part.finish()
    return at, gate_part, out_part


def copy_weights(seg_ref, win_all, wout_all, sm_all, hd, s, sems):
    copies = [
        pltpu.make_async_copy(src, dst, sems.at[i])
        for i, (src, dst) in enumerate(((win_all, s.win), (wout_all, s.wout), (sm_all, s.sm)))
    ]
    for copy in copies:
        copy.start()
    setup(seg_ref, s)
    for copy in copies:
        copy.wait()
    hd[0:2, :] = s.sm[8:10, :128]
    skip = packed(jnp.broadcast_to(s.sm[10:11, :128], (8, 128)))
    s.sm[7:8, :INNER] = nn(skip, s.one64[...])[0:1, :]


def transposed(src, dst):
    for i in range(TOKENS // 128):
        for j in range(MODEL // 128):
            dst[j * 128 : (j + 1) * 128, i * 128 : (i + 1) * 128] = src[
                i * 128 : (i + 1) * 128, j * 128 : (j + 1) * 128
            ].T


def out_weight_gradient(cot_ref, s):
    for j in range(QUADS):
        cols = slice(j * 256, (j + 1) * 256)
        s.dwo[cols, :] = tn(s.gated[:, cols], cot_ref[...]).astype(bf16)


def in_weight_gradient(ref, column, tile):
    def fill(turned):
        for i in range(3):
            rows = slice(i * 256, (i + 1) * 256)
            ref[rows, column : column + tile.shape[1]] = nn(turned[rows, :TOKENS], tile[...]).astype(bf16)

    return fill


def token_gradient(i, win, gtok_ref, s):
    rows = pl.ds(pl.multiple_of(i * 256, 256), 256)
    for j in range(3):
        cols = slice(j * 256, (j + 1) * 256)
        gtok_ref[rows, cols] = (
            nt(s.dz[rows, :], win[cols, :INNER])
            + nt(s.u[rows, :], win[cols, INNER:DT])
            + nt(s.ddt[rows, :], win[cols, DT : DT + 128])
        )


def pack_small(mine, s):
    high, low = two_parts(s.acc[7, :, :INNER])
    skip = nn(high, s.sum64[...]) + nn(low, s.sum64[...])
    s.acc[7, :, 0:128] = skip
    heads = [jnp.sum(s.acc[k, :, 0:128], axis=0, keepdims=True) for k in (7, 8, 9)] + [jnp.zeros((1, 128), f32)]
    for j in range(CONV_CH // 256):
        sums = [jnp.sum(s.acc[k, :, j * 256 : (j + 1) * 256], axis=0, keepdims=True) for k in range(6)]
        tail = jnp.concatenate(heads[2 * j : 2 * j + 2], axis=1) if j < 2 else jnp.zeros((1, 256), f32)
        mine[0, j * 8 : (j + 1) * 8, :] = jnp.concatenate(sums + [tail, jnp.zeros((1, 256), f32)], axis=0)


def pack_gain(mine, s):
    sums = [jnp.sum(s.acc[6, :, j * 128 : (j + 1) * 128], axis=0, keepdims=True) for j in range(MODEL // 128)]
    mine[0] = jnp.concatenate(sums + [jnp.zeros((2, 128), f32)], axis=0)


def layer_kernel(
    direct, shards, x_ref, cot_ref, seg_ref, win_own, wout_own, sm_own, mixed_ref, gtok_ref, gin_ref, gout_ref, gsm_ref, *refs
):
    s = SimpleNamespace(**dict(zip(SCRATCH, refs)))
    s.mixed_sem, *sems = refs[len(SCRATCH) :]
    s.part = s.z
    win, wout, sm, hd = s.win, s.wout, s.sm, s.hd
    if direct:
        *sems, sends, recvs, locals_, total_send, total_recv, forward_done, scan_done = sems
        at, gate_part, out_part = gather_weights(shards, x_ref, seg_ref, win_own, wout_own, sm_own, hd, s, *sems)
        pair = (sends, recvs)
        zr, xbc, dy = s.zr, s.xbc, s.dy
        gate_sum = Reduce(
            at, s.dwz, MODEL, INNER // 2, [(zr, 0, 0), (zr, 768, 0), (zr, 1152, 0), (zr, 1344, 0)], gin_ref, 0, pair, 0, locals_.at[0]
        )
        out_sum = Reduce(
            at, s.dwo, INNER, MODEL // 2, [(wout, 0, 0), (wout, 0, 384), (wout, 768, 384), (wout, 1152, 384)], gout_ref, 0, pair, 1, locals_.at[1]
        )
        early_sum, late_sum = (
            Reduce(
                at,
                s.dwu.at[:, i * 1024 : (i + 1) * 1024],
                MODEL,
                512,
                [(xbc, 0, i * 512), (dy, 0, i * 512), (dy, 384, i * 512), (dy, 576, i * 512)],
                gin_ref,
                INNER + i * 1024,
                pair,
                2 + i,
                locals_.at[2 + i],
            )
            for i in range(2)
        )
        totals = (total_send, total_recv)
        small_sum = Total(
            at, s.mine, lambda i: s.up.at[i // 3, pl.ds(8 + (i % 3) * 56, 56), :], totals, 0
        )
        gain_sum = Total(at, s.gain, lambda i: s.gain_slots.at[i], totals, 1)
    else:
        copy_weights(seg_ref, win_own, wout_own, sm_own, hd, s, *sems)
        for q in range(SEQ):
            norm_input(q, x_ref, sm, s)
    chunks = LEN // CHUNK

    @pl.loop(0, SEQ)
    def _(q):
        project(q, win, sm, hd, s)
        s.state[...] = jnp.zeros((STATE, INNER), f32)
        if direct:

            @pl.when(q == 0)
            def _():
                gate_part.spread()
                out_part.spread()

        @pl.loop(0, chunks)
        def _(c):
            scan_forward(q, c, seg_ref, sm, hd, s)
            if direct:
                polls = ((2, gate_part.relay), (3, out_part.relay))
                for index, poll in polls:

                    @pl.when((q == 0) & (c == index))
                    def _():
                        poll()

                @pl.when((q == 1) & (c == 0))
                def _():
                    gate_part.share()

                @pl.when((q == 1) & (c == 1))
                def _():
                    out_part.share()

    if direct:
        gate_part.finish()
        out_part.finish()

    @pl.loop(0, TOKENS // 256)
    def _(i):
        gate(i, x_ref, cot_ref, win, wout, sm, mixed_ref, s)

    if direct:
        meet(at, shards, forward_done)
    out_weight_gradient(cot_ref, s)
    if direct:
        met(shards, forward_done)
        out_sum.begin()
    turned = s.gated
    transposed(s.nrm, turned)
    for j in range(QUADS):
        in_weight_gradient(s.dwz, j * 256, s.dz.at[:, j * 256 : (j + 1) * 256])(turned)
    if direct:
        gate_sum.begin()

    def backward(quads, first, polls):
        @pl.loop(0, SEQ * chunks)
        def _(n):
            @pl.when(n % chunks == 0)
            def _():
                s.state[:, quads[0] * 256 : (quads[-1] + 1) * 256] = jnp.zeros((STATE, len(quads) * 256), f32)

            scan_backward(n // chunks, chunks - 1 - n % chunks, quads, first, seg_ref, sm, hd, s)
            for index, poll in polls:

                @pl.when(n == index)
                def _():
                    poll()

    polls = ()
    if direct:
        polls = (
            (0, out_sum.first),
            (1, gate_sum.first),
            (3, out_sum.second),
            (5, out_sum.third),
            (6, gate_sum.second),
            (7, out_sum.fourth),
        )
    backward(range(4), True, polls)
    if direct:
        meet(at, shards, scan_done)

    @pl.loop(0, SEQ)
    def _(q):
        conv_backward(q, range(8), sm, s)

    if direct:
        gate_sum.third()
    for j in range(4):
        in_weight_gradient(s.dwu, j * 256, s.u.at[:, j * 256 : (j + 1) * 256])(turned)
    if direct:
        met(shards, scan_done)
        early_sum.begin()
        polls = (
            (0, out_sum.sixth),
            (1, early_sum.first),
            (3, gate_sum.fourth),
            (6, early_sum.second),
            (7, gate_sum.sixth),
        )
    backward(range(4, QUADS), False, polls)

    @pl.loop(0, SEQ)
    def _(q):
        conv_backward(q, range(8, CONV_CH // 128), sm, s)

    for j in range(4, CONV_CH // 256):
        in_weight_gradient(s.dwu, j * 256, s.u.at[:, j * 256 : (j + 1) * 256])(turned)
    in_weight_gradient(s.dwu, CONV_CH, s.ddt)(turned)
    s.dwu[:, CONV_CH + 128 :] = jnp.zeros((MODEL, 128), bf16)
    pack_small(s.mine, s)
    if direct:
        late_sum.begin()
        small_sum.begin()
        early_sum.third()
        small_sum.step(0)

    @pl.loop(0, TOKENS // 256)
    def _(i):
        token_gradient(i, win, gtok_ref, s)
        if direct:

            @pl.when(i == 0)
            def _():
                late_sum.first()

            @pl.when(i == 1)
            def _():
                small_sum.step(1)

            @pl.when(i == 3)
            def _():
                small_sum.step(2)

    if direct:
        early_sum.fourth()
        late_sum.second()

    @pl.loop(0, TOKENS // 64)
    def _(i):
        input_gradient(i, x_ref, cot_ref, sm, gtok_ref, s)

    pack_gain(s.gain, s)
    if direct:
        gain_sum.begin()
        gain_sum.step(0)
        early_sum.sixth()
        gain_sum.step(1)
        late_sum.third()
        gain_sum.step(2)
        out_sum.seventh()
        gate_sum.seventh()
        late_sum.fourth()
        early_sum.seventh()
        late_sum.sixth()
        unpack_small(small_sum.finish(), gain_sum.finish(), gsm_ref)
        late_sum.seventh()
    else:
        unpack_small(s.mine[0], s.gain[0], gsm_ref)
        copies = [
            pltpu.make_async_copy(s.dwz, gin_ref.at[:, :INNER], sems[0].at[0]),
            pltpu.make_async_copy(s.dwu, gin_ref.at[:, INNER:], sems[0].at[1]),
            pltpu.make_async_copy(s.dwo, gout_ref, sems[0].at[2]),
        ]
        for copy in copies:
            copy.start()
        for copy in copies:
            copy.wait()


def reaches(mesh):
    return mesh.shape["rep"] == 8 and mesh.shape["shard"] == 4


def layer(mesh, x, cot, seg, win, wout, sm):
    direct, shards = reaches(mesh), mesh.shape["shard"]
    vmem = pl.BlockSpec(memory_space=pltpu.VMEM)
    hbm = pl.BlockSpec(memory_space=pl.ANY)
    dma = pltpu.SemaphoreType.DMA
    if direct:
        sems = [dma((3, 5, shards)), dma((3, 5, shards)), dma((shards,)), dma((shards,))]
        sems += [dma((4, 10)), dma((4, 10)), dma((4,)), dma((2, 6)), dma((2, 6))]
        sems += [pltpu.SemaphoreType.REGULAR] * 2
        options = dict(collective_id=0, has_side_effects=True)
        weights = vmem
    else:
        sems, options, weights = [dma((3,))], {}, hbm
    return pl.pallas_call(
        partial(layer_kernel, direct, shards),
        out_shape=(
            jax.ShapeDtypeStruct((TOKENS, MODEL), bf16),
            jax.ShapeDtypeStruct((TOKENS, MODEL), f32),
            jax.ShapeDtypeStruct((MODEL // shards if direct else MODEL, PADDED), bf16),
            jax.ShapeDtypeStruct((INNER // shards if direct else INNER, MODEL), bf16),
            jax.ShapeDtypeStruct((16, CONV_CH), f32),
        ),
        in_specs=[vmem] * 3 + [weights, hbm, weights],
        out_specs=[hbm, vmem, hbm, hbm, vmem],
        scratch_shapes=[pltpu.VMEM(shape, kind) for shape, kind in SCRATCH.values()] + [dma] + sems,
        compiler_params=pltpu.CompilerParams(vmem_limit_bytes=67043328, **options),
        name="layer",
    )(x, cot, seg, win, wout, sm)


def placed(v, row, width):
    return jnp.pad(v.astype(f32), ((row, 16 - row - v.shape[0]), (0, width - v.shape[1])))


def on_device(mesh, tokens, segment_ids, norm_gain, in_weight, conv_weight, conv_bias, dt_bias, a_log, d_skip, gate_gain, out_weight, cotangent):
    small, heads = (conv_bias, gate_gain, norm_gain), (dt_bias, a_log, d_skip)
    if reaches(mesh):
        win, wout, taps, width = in_weight, out_weight, conv_weight, 512
    else:
        win, wout, taps, *small = lax.all_gather(
            (in_weight, out_weight, conv_weight) + small, "shard", axis=0, tiled=True
        )
        win, width = jnp.pad(win, ((0, 0), (0, PADDED - PROJ))), CONV_CH
    sm = placed(taps.T, 0, width)
    for row, v in enumerate((*small, jnp.zeros((1,), f32), *heads)):
        sm = sm + placed(v[None], CONV + row, width)
    mixed, gtok, gin, gout, gsm = layer(
        mesh,
        tokens.reshape(TOKENS, MODEL), cotangent.reshape(TOKENS, MODEL), segment_ids, win, wout, sm
    )
    if not reaches(mesh):
        gin = lax.psum(lax.psum_scatter(gin, "shard", scatter_dimension=0, tiled=True), "rep")
        gout = lax.psum(lax.psum_scatter(gout, "shard", scatter_dimension=0, tiled=True), "rep")
        gsm = lax.psum(gsm, ("rep", "shard"))
    me = lax.axis_index("shard")

    def owned(v, like):
        return lax.dynamic_slice_in_dim(v, me * like.shape[0], like.shape[0])

    return (
        mixed.reshape(SEQ, LEN, MODEL),
        gtok.reshape(SEQ, LEN, MODEL),
        owned(gsm[6, :MODEL], norm_gain),
        gin[:, :PROJ].astype(f32),
        owned(gsm[:CONV].T, conv_weight),
        owned(gsm[4], conv_bias),
        gsm[8, :HEADS],
        gsm[9, :HEADS],
        gsm[7, :HEADS],
        owned(gsm[5, :INNER], gate_gain),
        gout.astype(f32),
    )


def solution(mesh):
    batch = P(("rep", "shard"), None, None)
    return jax.shard_map(
        partial(on_device, mesh),
        mesh=mesh,
        in_specs=(
            batch,
            P(("rep", "shard"), None),
            P("shard"),
            P("shard", None),
            P("shard", None),
            P("shard"),
            P(),
            P(),
            P(),
            P("shard"),
            P("shard", None),
            batch,
        ),
        out_specs=(
            batch,
            batch,
            P("shard"),
            P("shard", None),
            P("shard", None),
            P("shard"),
            P(),
            P(),
            P(),
            P("shard"),
            P("shard", None),
        ),
        check_vma=False,
    )
```
